16 devices in a mesh: dp: 2 (over y, z), sp: 8 (over x, core).
Axes of the slice: x: 4, y: 2, z: 1, core: 2. Of those that a mesh axis runs over, the one named last changes fastest.
The devices are a block of a 4x4x8 slice.
Arguments:
- pair_rep: float32 [384, 192, 128], P(('dp', 'sp')), parts along dimension 0
- w_qkvg_s: bfloat16 [128, 512], replicated
- w_bias_s: bfloat16 [4, 128], replicated
- w_out_s: bfloat16 [128, 128], replicated
- w_qkvg_e: bfloat16 [128, 512], replicated
- w_bias_e: bfloat16 [4, 128], replicated
- w_out_e: bfloat16 [128, 128], replicated
- w_one: bfloat16 [128, 512], replicated
- w_two: bfloat16 [512, 128], replicated
Outputs:
- output: float32 [384, 192, 128], P(('dp', 'sp')), parts along dimension 0
There are 2 independent parts. The reference program is written for one: setup_inputs(seed, part) draws one part's arguments, and reference() takes and returns one part's arrays. A program takes and returns all parts, laid end to end along the dimension named above; an argument that names none is the same for every part.
All inputs are finite; a program needn't handle non-finite values.
Results may differ from the reference program's by a relative error of at most 0.0102778.
Values are sent between devices in bfloat16 or wider.
A program may use at most 768 MiB of HBM per device.

```python
import jax
import jax.numpy as jnp
from jax import lax

N = 192
C_Z = 128
HEADS = 4
HEAD_DIM = C_Z // HEADS
HIDDEN = 4 * C_Z
LN_EPS = 1e-5
OUT_SCALE = (N / 16) ** 0.5


def setup_inputs(seed: int = 0, part: int = 0) -> dict:
    root_key = jax.random.key(seed)
    part_key = jax.random.fold_in(root_key, part)
    shared = jax.random.split(jax.random.fold_in(root_key, 65537), 8)
    in_scale = C_Z ** -0.5
    hid_scale = HIDDEN ** -0.5
    pair_rep = jax.random.normal(part_key, (N, N, C_Z), jnp.float32)
    w_qkvg_s = jax.random.normal(shared[0], (C_Z, 4 * C_Z), jnp.float32) * in_scale
    w_bias_s = jax.random.normal(shared[1], (HEADS, C_Z), jnp.float32) * in_scale
    w_out_s = jax.random.normal(shared[2], (C_Z, C_Z), jnp.float32) * (in_scale * OUT_SCALE)
    w_qkvg_e = jax.random.normal(shared[3], (C_Z, 4 * C_Z), jnp.float32) * in_scale
    w_bias_e = jax.random.normal(shared[4], (HEADS, C_Z), jnp.float32) * in_scale
    w_out_e = jax.random.normal(shared[5], (C_Z, C_Z), jnp.float32) * (in_scale * OUT_SCALE)
    w_one = jax.random.normal(shared[6], (C_Z, HIDDEN), jnp.float32) * in_scale
    w_two = jax.random.normal(shared[7], (HIDDEN, C_Z), jnp.float32) * hid_scale
    return {
        "pair_rep": pair_rep,
        "w_qkvg_s": w_qkvg_s.astype(jnp.bfloat16),
        "w_bias_s": w_bias_s.astype(jnp.bfloat16),
        "w_out_s": w_out_s.astype(jnp.bfloat16),
        "w_qkvg_e": w_qkvg_e.astype(jnp.bfloat16),
        "w_bias_e": w_bias_e.astype(jnp.bfloat16),
        "w_out_e": w_out_e.astype(jnp.bfloat16),
        "w_one": w_one.astype(jnp.bfloat16),
        "w_two": w_two.astype(jnp.bfloat16),
    }


def layer_norm(values):
    vals_f = values.astype(jnp.float32)
    mean_c = jnp.mean(vals_f, axis=-1, keepdims=True)
    centered = vals_f - mean_c
    variance = jnp.mean(centered * centered, axis=-1, keepdims=True)
    return (centered * lax.rsqrt(variance + LN_EPS)).astype(jnp.bfloat16)


def bias_table(pair_in, w_bias):
    def one_row(row_in):
        return jnp.dot(layer_norm(row_in), w_bias.T, preferred_element_type=jnp.float32).astype(jnp.bfloat16)
    return jnp.transpose(lax.map(one_row, pair_in), (2, 0, 1))


def row_update(row_in, bias_full, w_qkvg, w_out):
    seq_len = row_in.shape[0]
    projected = jnp.dot(layer_norm(row_in), w_qkvg, preferred_element_type=jnp.float32)
    split_shape = (seq_len, HEADS, HEAD_DIM)
    queries = projected[:, :C_Z].astype(jnp.bfloat16).reshape(split_shape).astype(jnp.float32)
    key_vecs = projected[:, C_Z:2 * C_Z].astype(jnp.bfloat16).reshape(split_shape).astype(jnp.float32)
    val_vecs = projected[:, 2 * C_Z:3 * C_Z].astype(jnp.bfloat16).reshape(split_shape).astype(jnp.float32)
    gate_vals = jax.nn.sigmoid(projected[:, 3 * C_Z:]).reshape(split_shape)
    scores = jnp.einsum('jhd,khd->hjk', queries, key_vecs) * HEAD_DIM ** -0.5 + bias_full.astype(jnp.float32)
    attn_prob = jax.nn.softmax(scores, axis=-1).astype(jnp.bfloat16).astype(jnp.float32)
    attn_out = jnp.einsum('hjk,khd->jhd', attn_prob, val_vecs)
    gated_out = (attn_out * gate_vals).astype(jnp.bfloat16).reshape(seq_len, C_Z)
    return jnp.dot(gated_out, w_out, preferred_element_type=jnp.float32)


def tri_attention(pair_in, w_qkvg, w_bias, w_out):
    bias_full = bias_table(pair_in, w_bias)

    def one_row(row_in):
        return row_update(row_in, bias_full, w_qkvg, w_out)
    return lax.map(one_row, pair_in)


def reference(pair_rep, w_qkvg_s, w_bias_s, w_out_s, w_qkvg_e, w_bias_e, w_out_e, w_one, w_two):
    pair_one = pair_rep + tri_attention(pair_rep, w_qkvg_s, w_bias_s, w_out_s)
    pair_trans = jnp.swapaxes(pair_one.astype(jnp.bfloat16), 0, 1)
    end_upd = tri_attention(pair_trans, w_qkvg_e, w_bias_e, w_out_e)

    def finish_row(row_pair):
        trans_row, upd_row = row_pair
        pair_two = trans_row.astype(jnp.float32) + upd_row
        hidden = jax.nn.relu(jnp.dot(layer_norm(pair_two), w_one, preferred_element_type=jnp.float32))
        trans_out = jnp.dot(hidden.astype(jnp.bfloat16), w_two, preferred_element_type=jnp.float32)
        return (upd_row + trans_out).astype(jnp.bfloat16)

    delta_trans = lax.map(finish_row, (pair_trans, end_upd))
    return pair_one + jnp.swapaxes(delta_trans, 0, 1).astype(jnp.float32)
```

```python
import functools

import jax
import jax.numpy as jnp
from jax import lax
from jax.experimental import pallas as pl
from jax.experimental.pallas import tpu as pltpu
from jax.sharding import PartitionSpec as P

LN_EPS = 1e-5
MESH = pl.DeviceIdType.MESH
F32 = jnp.float32
BF16 = jnp.bfloat16


def layer_norm(vals):
    mean_c = jnp.mean(vals, axis=-1, keepdims=True)
    centered = vals - mean_c
    variance = jnp.mean(centered * centered, axis=-1, keepdims=True)
    return (centered * lax.rsqrt(variance + LN_EPS)).astype(BF16)


def dot(lhs, rhs, lhs_dim=1, rhs_dim=0):
    return lax.dot_general(lhs, rhs, (((lhs_dim,), (rhs_dim,)), ((), ())), preferred_element_type=F32)


def duplicate_tail(normed):
    return jnp.concatenate([normed, normed[128:]], axis=0)


def low_half(shape):
    return lax.broadcasted_iota(jnp.int32, shape, len(shape) - 1) < 64


def bias_row(normed_dup, w_bias):
    full = dot(w_bias, normed_dup, 1, 1)
    low = low_half((1, 128))
    tiles = []
    for first in (0, 2):
        head_a, head_b = full[first:first + 1], full[first + 1:first + 2]
        tiles += [head_a[:, :128], jnp.where(low, head_a[:, 128:], head_b[:, 128:]), head_b[:, :128]]
    return jnp.concatenate(tiles, axis=1)


def project(normed_dup, w_t, w_key):
    cols = dot(w_t, normed_dup, 1, 1)
    channels = w_key.shape[0]
    q_t = cols[:channels].astype(BF16)
    v_t = cols[channels:2 * channels, :192].astype(BF16)
    g_t = jax.nn.sigmoid(cols[2 * channels:])
    keys = dot(normed_dup[:192], w_key).astype(BF16)
    return q_t, keys, v_t, g_t


def attend(q_t, keys, v_t, g_t, bias_of, w_out, scale):
    zero = jnp.zeros((32, 128), BF16)
    low = low_half((32, 128))

    def head(idx):
        return q_t[32 * idx:32 * idx + 32, :128], q_t[32 * idx:32 * idx + 32, 128:]

    q0, q0b = head(0)
    q1, q1b = head(1)
    q2, q2b = head(2)
    q3, q3b = head(3)

    def lo(val):
        return jnp.where(low, val, jnp.zeros_like(val))

    def hi(val):
        return jnp.where(low, jnp.zeros_like(val), val)

    def stack(rows):
        return jnp.concatenate([jnp.concatenate(row, axis=1) for row in rows], axis=0)

    none = [zero, zero]
    blocks = [
        stack([[q0, lo(q0b)], [zero, hi(q1b)], none, none]),
        stack([none, [q1, zero], [zero, q2], none]),
        stack([none, none, [lo(q2b), zero], [hi(q3b), q3]]),
    ]
    outs = []
    for tile, block in enumerate(blocks):
        scores = dot(keys, block) * scale + bias_of(tile)
        top = jnp.max(scores, axis=0, keepdims=True)
        prob = jnp.exp(scores - top)
        total = jnp.sum(prob, axis=0, keepdims=True)
        mixed = dot(v_t[32 * tile:32 * tile + 64], prob.astype(BF16))
        outs.append(mixed / total)
    main = jnp.concatenate([outs[0][:32, :128], outs[1][:32, :128], outs[1][32:, 128:], outs[2][32:, 128:]], axis=0)
    tail = jnp.concatenate([lo(outs[0][:32, 128:]), hi(outs[0][32:, 128:]), lo(outs[2][:32, :128]), hi(outs[2][32:, :128])], axis=0)
    gated = (jnp.concatenate([main, tail], axis=1) * g_t).astype(BF16)
    res = dot(gated.T, w_out)
    return jnp.concatenate([res[:128], res[128:192] + res[192:]], axis=0)


def kernel(axis, group, z_ref, wp_s, wb_s, wo_s, wp_e, wb_e, wo_e, w1_ref, w2_ref, y_ref,
           wt_s, wt_e, row_bias, send_bias, got_bias, bias_t, q_sc, k_sc, v_sc, g_sc,
           send_h, got_h, send_d, got_d, flat,
           bias_send_sem, bias_recv_sem, h_send_sem, h_recv_sem, d_send_sem, d_recv_sem):
    rows, seq_len, channels = z_ref.shape
    pairs = rows // 2
    scale = 32 ** -0.5
    me = lax.axis_index(axis)
    peers = [lax.rem(me + step, group) for step in range(1, group)]

    barrier = pltpu.get_barrier_semaphore()
    for peer in peers:
        pl.semaphore_signal(barrier, inc=1, device_id={axis: peer}, device_id_type=MESH)

    for wp, wt in ((wp_s, wt_s), (wp_e, wt_e)):
        wt[0:channels] = wp[:, 0:channels].T
        wt[channels:2 * channels] = wp[:, 2 * channels:3 * channels].T
        wt[2 * channels:3 * channels] = wp[:, 3 * channels:].T

    def copy_bias(phase, peer):
        return pltpu.make_async_remote_copy(
            src_ref=send_bias.at[phase], dst_ref=got_bias.at[phase, me],
            send_sem=bias_send_sem.at[phase, peer], recv_sem=bias_recv_sem.at[phase, me],
            device_id={axis: peer}, device_id_type=MESH)

    def wait_bias(phase):
        for peer in peers:
            pltpu.make_async_copy(got_bias.at[phase, peer], got_bias.at[phase, peer], bias_recv_sem.at[phase, peer]).wait()

    def copy_pair(send, got, send_sem, recv_sem, peer, pair):
        return pltpu.make_async_remote_copy(
            src_ref=send.at[peer, pair], dst_ref=got.at[me, pair],
            send_sem=send_sem.at[peer], recv_sem=recv_sem.at[me],
            device_id={axis: peer}, device_id_type=MESH)

    def wait_all(got, recv_sem):
        for peer in peers:
            pltpu.make_async_copy(got.at[peer], got.at[peer], recv_sem.at[peer]).wait()

    def store_pair(send, got, pair, first, second):
        for dest in range(group):
            span = slice(rows * dest, rows * dest + rows)
            send[dest, pair] = jnp.concatenate([first[span], second[span]], axis=0).astype(BF16)
        got[me, pair] = send[me, pair]

    def publish_bias(phase):
        rounded = row_bias[...].astype(BF16)
        send_bias[phase] = rounded
        got_bias[phase, me] = rounded

    def stage_projection(slot, normed_dup, wt, wp):
        q_t, keys, v_t, g_t = project(normed_dup, wt[...], wp[:, channels:2 * channels])
        q_sc[slot] = q_t
        k_sc[slot] = keys
        v_sc[slot] = v_t
        g_sc[slot] = g_t

    def staged_attention(slot, wo):
        return attend(q_sc[slot], k_sc[slot], v_sc[slot], g_sc[slot],
                      lambda tile: bias_t[:, 256 * tile:256 * tile + 256], wo[...], scale)

    @pl.loop(0, rows)
    def _(row):
        normed_dup = duplicate_tail(layer_norm(z_ref[row]))
        row_bias[pl.ds(row, 1), :] = bias_row(normed_dup, wb_s[...])

    publish_bias(0)
    pl.semaphore_wait(barrier, group - 1)
    for peer in peers:
        copy_bias(0, peer).start()

    @pl.loop(0, rows)
    def _(row):
        normed_dup = duplicate_tail(layer_norm(z_ref[row]))
        stage_projection(row, normed_dup, wt_s, wp_s)

    wait_bias(0)
    low = low_half((64, 128))
    by_query = jnp.concatenate([got_bias[0, src].astype(F32) for src in range(group)], axis=0)
    by_query = jnp.concatenate([by_query, by_query[128:]], axis=0)
    for first in (0, 1):
        base = 384 * first
        head_a = by_query[:, base:base + 128].T
        mixed = by_query[:, base + 128:base + 256].T
        head_b = by_query[:, base + 256:base + 384].T
        bias_t[0:128, base:base + 128] = head_a[:, :128]
        bias_t[128:192, base:base + 128] = mixed[:64, :128]
        low_a = low_half((128, 128))
        bias_t[0:128, base + 128:base + 256] = jnp.where(low_a, head_a[:, 128:], head_b[:, 128:])
        bias_t[128:192, base + 128:base + 256] = jnp.where(low, mixed[:64, 128:], mixed[64:, 128:])
        bias_t[0:128, base + 256:base + 384] = head_b[:, :128]
        bias_t[128:192, base + 256:base + 384] = mixed[64:, :128]

    @pl.loop(0, pairs)
    def _(pair):
        resid = []
        for sub in range(2):
            row = 2 * pair + sub
            value = z_ref[row] + staged_attention(row, wo_s)
            y_ref[row] = value
            resid.append(value)
            again = value.astype(BF16).astype(F32)
            row_bias[pl.ds(row, 1), :] = bias_row(duplicate_tail(layer_norm(again)), wb_e[...])
        store_pair(send_h, got_h, pair, resid[0], resid[1])

        @pl.when(pair > 0)
        def _():
            for peer in peers:
                copy_pair(send_h, got_h, h_send_sem, h_recv_sem, peer, pair - 1).start()

    publish_bias(1)
    for peer in peers:
        copy_pair(send_h, got_h, h_send_sem, h_recv_sem, peer, pairs - 1).start()
    for peer in peers:
        copy_bias(1, peer).start()

    wait_all(got_h, h_recv_sem)

    @pl.loop(0, group)
    def _(src):
        @pl.loop(0, pairs)
        def _(pair):
            start = pl.multiple_of((src * pairs + pair) * 2 * rows, 2 * rows)
            flat[pl.ds(start, 2 * rows), :] = got_h[src, pair].astype(F32)

    wait_bias(1)
    for src in range(group):
        bias_t[rows * src:rows * src + rows] = got_bias[1, src].astype(F32)

    @pl.loop(0, pairs)
    def _(pair):
        delta = []
        for sub in range(2):
            col = 2 * pair + sub
            trans = flat[pl.ds(col, seq_len, stride=rows), :]
            stage_projection(sub, duplicate_tail(layer_norm(trans)), wt_e, wp_e)
            upd = staged_attention(sub, wo_e)
            hidden = jnp.maximum(dot(layer_norm(trans + upd), w1_ref[...]), 0.0).astype(BF16)
            delta.append(upd + dot(hidden, w2_ref[...]))
        store_pair(send_d, got_d, pair, delta[0], delta[1])

        @pl.when(pair > 0)
        def _():
            for peer in peers:
                copy_pair(send_d, got_d, d_send_sem, d_recv_sem, peer, pair - 1).start()

    for peer in peers:
        copy_pair(send_d, got_d, d_send_sem, d_recv_sem, peer, pairs - 1).start()

    wait_all(got_d, d_recv_sem)

    @pl.loop(0, group)
    def _(src):
        @pl.loop(0, pairs)
        def _(pair):
            start = pl.multiple_of((src * pairs + pair) * 2 * rows, 2 * rows)
            flat[pl.ds(start, 2 * rows), :] = got_d[src, pair].astype(F32)

    @pl.loop(0, rows)
    def _(row):
        y_ref[row] = y_ref[row] + flat[pl.ds(row, seq_len, stride=rows), :]

    for peer in peers:
        for phase in range(2):
            pltpu.make_async_copy(send_bias.at[phase], send_bias.at[phase], bias_send_sem.at[phase, peer]).wait()
        pltpu.make_async_copy(send_h.at[peer], send_h.at[peer], h_send_sem.at[peer]).wait()
        pltpu.make_async_copy(send_d.at[peer], send_d.at[peer], d_send_sem.at[peer]).wait()


def solution(mesh):
    row_spec = P(('dp', 'sp'), None, None)
    group = mesh.shape['sp']

    def local_fn(pair_loc, w_qkvg_s, w_bias_s, w_out_s, w_qkvg_e, w_bias_e, w_out_e, w_one, w_two):
        rows, seq_len, channels = pair_loc.shape
        heads = w_bias_s.shape[0]
        pairs = rows // 2
        vmem = pl.BlockSpec(memory_space=pltpu.VMEM)
        wide = heads * seq_len
        exchange = pltpu.VMEM((group, pairs, 2 * rows, channels), BF16)
        return pl.pallas_call(
            functools.partial(kernel, 'sp', group),
            out_shape=jax.ShapeDtypeStruct(pair_loc.shape, F32),
            in_specs=[vmem] * 9,
            out_specs=vmem,
            scratch_shapes=[
                pltpu.VMEM((3 * channels, channels), BF16),
                pltpu.VMEM((3 * channels, channels), BF16),
                pltpu.VMEM((rows, wide), F32),
                pltpu.VMEM((2, rows, wide), BF16),
                pltpu.VMEM((2, group, rows, wide), BF16),
                pltpu.VMEM((seq_len, wide), F32),
                pltpu.VMEM((rows, channels, 256), BF16),
                pltpu.VMEM((rows, seq_len, channels), BF16),
                pltpu.VMEM((rows, channels, seq_len), BF16),
                pltpu.VMEM((rows, channels, 256), F32),
                exchange, exchange, exchange, exchange,
                pltpu.VMEM((rows * seq_len, channels), F32),
                pltpu.SemaphoreType.DMA((2, group)),
                pltpu.SemaphoreType.DMA((2, group)),
                pltpu.SemaphoreType.DMA((group,)),
                pltpu.SemaphoreType.DMA((group,)),
                pltpu.SemaphoreType.DMA((group,)),
                pltpu.SemaphoreType.DMA((group,)),
            ],
            compiler_params=pltpu.CompilerParams(collective_id=0, has_side_effects=True, vmem_limit_bytes=60 * 1024 * 1024),
        )(pair_loc, w_qkvg_s, w_bias_s, w_out_s, w_qkvg_e, w_bias_e, w_out_e, w_one, w_two)

    return jax.shard_map(local_fn, mesh=mesh, in_specs=(row_spec, P(), P(), P(), P(), P(), P(), P(), P()), out_specs=row_spec, check_vma=False)
```

```python
import functools

import jax
import jax.numpy as jnp
from jax import lax
from jax.experimental import pallas as pl
from jax.experimental.pallas import tpu as pltpu
from jax.sharding import PartitionSpec as P

LN_EPS = 1e-5
MESH = pl.DeviceIdType.MESH
F32 = jnp.float32
BF16 = jnp.bfloat16


def layer_norm(vals):
    mean_c = jnp.mean(vals, axis=-1, keepdims=True)
    centered = vals - mean_c
    variance = jnp.mean(centered * centered, axis=-1, keepdims=True)
    return (centered * lax.rsqrt(variance + LN_EPS)).astype(BF16)


def dot(lhs, rhs, lhs_dim=1, rhs_dim=0):
    return lax.dot_general(lhs, rhs, (((lhs_dim,), (rhs_dim,)), ((), ())), preferred_element_type=F32)


def duplicate_tail(normed):
    return jnp.concatenate([normed, normed[128:]], axis=0)


def low_half(shape):
    return lax.broadcasted_iota(jnp.int32, shape, len(shape) - 1) < 64


def bias_row(full):
    low = low_half((1, 128))
    tiles = []
    for first in (0, 2):
        head_a, head_b = full[first:first + 1], full[first + 1:first + 2]
        tiles += [head_a[:, :128], jnp.where(low, head_a[:, 128:], head_b[:, 128:]), head_b[:, :128]]
    return jnp.concatenate(tiles, axis=1)


def keep_low(val):
    return jnp.where(low_half(val.shape), val, jnp.zeros_like(val))


def keep_high(val):
    return jnp.where(low_half(val.shape), jnp.zeros_like(val), val)


def stack(rows):
    return jnp.concatenate([jnp.concatenate(row, axis=1) for row in rows], axis=0)


def score_block(q_t, tile):
    zero = jnp.zeros((32, 128), BF16)
    none = [zero, zero]

    def head(idx):
        return q_t[32 * idx:32 * idx + 32, :128], q_t[32 * idx:32 * idx + 32, 128:]

    first, second = head(tile), head(tile + 1)
    if tile == 0:
        return stack([[first[0], keep_low(first[1])], [zero, keep_high(second[1])], none, none])
    if tile == 1:
        return stack([none, [first[0], zero], [zero, second[0]], none])
    return stack([none, none, [keep_low(first[1]), zero], [keep_high(second[1]), second[0]]])


def gather_heads(outs, g_t):
    main = jnp.concatenate([outs[0][:32, :128], outs[1][:32, :128], outs[1][32:, 128:], outs[2][32:, 128:]], axis=0)
    tail = jnp.concatenate([keep_low(outs[0][:32, 128:]), keep_high(outs[0][32:, 128:]),
                            keep_low(outs[2][:32, :128]), keep_high(outs[2][32:, :128])], axis=0)
    return (jnp.concatenate([main, tail], axis=1) * g_t).astype(BF16)


def merge_tail(res):
    return jnp.concatenate([res[:128], res[128:192] + res[192:]], axis=0)


def kernel(axis, group, z_ref, wp_s, wb_s, wo_s, wp_e, wb_e, wo_e, w1_ref, w2_ref, y_ref,
           wt_s, wt_e, row_bias, send_bias, got_bias, bias_t, normed_sc, q_sc, k_sc, v_sc, g_sc, gated_sc,
           send_h, got_h, send_d, got_d, flat,
           bias_send_sem, bias_recv_sem, h_send_sem, h_recv_sem, d_send_sem, d_recv_sem):
    rows, seq_len, channels = z_ref.shape
    pairs = rows // 2
    scale = 32 ** -0.5
    me = lax.axis_index(axis)
    peers = [lax.rem(me + step, group) for step in range(1, group)]

    barrier = pltpu.get_barrier_semaphore()
    for peer in peers:
        pl.semaphore_signal(barrier, inc=1, device_id={axis: peer}, device_id_type=MESH)

    for wp, wt in ((wp_s, wt_s), (wp_e, wt_e)):
        wt[0:channels] = wp[:, 0:channels].T
        wt[channels:2 * channels] = wp[:, 2 * channels:3 * channels].T
        wt[2 * channels:3 * channels] = wp[:, 3 * channels:].T

    def copy_bias(phase, peer):
        return pltpu.make_async_remote_copy(
            src_ref=send_bias.at[phase], dst_ref=got_bias.at[phase, me],
            send_sem=bias_send_sem.at[phase, peer], recv_sem=bias_recv_sem.at[phase, me],
            device_id={axis: peer}, device_id_type=MESH)

    def wait_bias(phase):
        for peer in peers:
            pltpu.make_async_copy(got_bias.at[phase, peer], got_bias.at[phase, peer], bias_recv_sem.at[phase, peer]).wait()

    def send_pair(send, got, send_sem, recv_sem, pair):
        for peer in peers:
            pltpu.make_async_remote_copy(
                src_ref=send.at[peer, pair], dst_ref=got.at[me, pair],
                send_sem=send_sem.at[peer], recv_sem=recv_sem.at[me],
                device_id={axis: peer}, device_id_type=MESH).start()

    def wait_all(got, recv_sem):
        for peer in peers:
            pltpu.make_async_copy(got.at[peer], got.at[peer], recv_sem.at[peer]).wait()

    def store_pair(send, got, pair, first, second):
        for dest in range(group):
            span = slice(rows * dest, rows * dest + rows)
            send[dest, pair] = jnp.concatenate([first[span], second[span]], axis=0).astype(BF16)
        got[me, pair] = send[me, pair]

    def publish_bias(phase):
        rounded = row_bias[...].astype(BF16)
        send_bias[phase] = rounded
        got_bias[phase, me] = rounded

    def project(slot, normed_dup, wt, wp):
        cols = dot(wt[...], normed_dup, 1, 1)
        keys = dot(normed_dup[:seq_len], wp[:, channels:2 * channels])
        return slot, cols, keys

    def stage(projected):
        slot, cols, keys = projected
        q_sc[slot] = cols[:channels].astype(BF16)
        v_sc[slot] = cols[channels:2 * channels, :seq_len].astype(BF16)
        g_sc[slot] = jax.nn.sigmoid(cols[2 * channels:])
        k_sc[slot] = keys.astype(BF16)

    class Attention:
        def __init__(self, slots):
            self.slots = slots
            self.score, self.prob, self.mixed, self.done = {}, {}, {}, {}

        def qk(self, unit):
            slot, tile = self.slots[unit // 3], unit % 3
            self.score[unit] = dot(k_sc[slot], score_block(q_sc[slot], tile))

        def soften(self, unit):
            tile = unit % 3
            scores = self.score.pop(unit) * scale + bias_t[:, 256 * tile:256 * tile + 256]
            top = jnp.max(scores, axis=0, keepdims=True)
            prob = jnp.exp(scores - top)
            self.prob[unit] = prob.astype(BF16), jnp.sum(prob, axis=0, keepdims=True)

        def mix(self, unit):
            slot, tile = self.slots[unit // 3], unit % 3
            prob, total = self.prob.pop(unit)
            self.mixed[unit] = dot(v_sc[slot, 32 * tile:32 * tile + 64], prob), total

        def norm(self, unit):
            mixed, total = self.mixed.pop(unit)
            self.done[unit] = mixed / total

        def gate(self, sub):
            outs = [self.done.pop(3 * sub + tile) for tile in range(3)]
            gated_sc[sub] = gather_heads(outs, g_sc[self.slots[sub]])

    def out_dot(sub, wo):
        return dot(gated_sc[sub].T, wo[...])

    batch = 4

    @pl.loop(0, rows // batch)
    def _(step):
        normed = [layer_norm(z_ref[step * batch + sub]) for sub in range(batch)]
        full = [dot(wb_s[...], duplicate_tail(val), 1, 1) for val in normed]
        for sub in range(batch):
            normed_sc[step * batch + sub] = normed[sub]
        for sub in range(batch):
            row_bias[pl.ds(step * batch + sub, 1), :] = bias_row(full[sub])

    publish_bias(0)
    pl.semaphore_wait(barrier, group - 1)
    for peer in peers:
        copy_bias(0, peer).start()

    @pl.loop(0, pairs)
    def _(step):
        made = [project(2 * step + sub, duplicate_tail(normed_sc[2 * step + sub]), wt_s, wp_s) for sub in range(2)]
        for val in made:
            stage(val)

    wait_bias(0)
    low = low_half((64, 128))
    by_query = jnp.concatenate([got_bias[0, src].astype(F32) for src in range(group)], axis=0)
    by_query = jnp.concatenate([by_query, by_query[128:]], axis=0)
    for first in (0, 1):
        base = 384 * first
        head_a = by_query[:, base:base + 128].T
        mixed = by_query[:, base + 128:base + 256].T
        head_b = by_query[:, base + 256:base + 384].T
        bias_t[0:128, base:base + 128] = head_a[:, :128]
        bias_t[128:192, base:base + 128] = mixed[:64, :128]
        low_a = low_half((128, 128))
        bias_t[0:128, base + 128:base + 256] = jnp.where(low_a, head_a[:, 128:], head_b[:, 128:])
        bias_t[128:192, base + 128:base + 256] = jnp.where(low, mixed[:64, 128:], mixed[64:, 128:])
        bias_t[0:128, base + 256:base + 384] = head_b[:, :128]
        bias_t[128:192, base + 256:base + 384] = mixed[64:, :128]

    def start_resid(pair, sub, res):
        row = 2 * pair + sub
        value = z_ref[row] + merge_tail(res)
        y_ref[row] = value
        return value, duplicate_tail(layer_norm(value.astype(BF16).astype(F32)))

    def start_tail(pair):
        res = [out_dot(sub, wo_s) for sub in range(2)]
        made = [start_resid(pair, sub, res[sub]) for sub in range(2)]
        full = [dot(wb_e[...], made[sub][1], 1, 1) for sub in range(2)]
        store_pair(send_h, got_h, pair, made[0][0], made[1][0])
        for sub in range(2):
            row_bias[pl.ds(2 * pair + sub, 1), :] = bias_row(full[sub])

    @pl.loop(0, pairs)
    def _(pair):
        @pl.when(pair > 1)
        def _():
            send_pair(send_h, got_h, h_send_sem, h_recv_sem, pair - 2)

        last = jnp.maximum(pair - 1, 0)
        att = Attention([2 * pair, 2 * pair + 1])
        att.qk(0)
        res = [out_dot(sub, wo_s) for sub in range(2)]
        att.qk(1)
        att.soften(0)
        att.mix(0)
        att.qk(2)
        made = [start_resid(last, 0, res[0])]
        att.soften(1)
        att.norm(0)
        att.mix(1)
        att.qk(3)
        made.append(start_resid(last, 1, res[1]))
        full = [dot(wb_e[...], made[0][1], 1, 1)]
        att.soften(2)
        att.norm(1)
        att.mix(2)
        att.qk(4)
        full.append(dot(wb_e[...], made[1][1], 1, 1))
        store_pair(send_h, got_h, last, made[0][0], made[1][0])
        att.soften(3)
        att.norm(2)
        att.mix(3)
        att.gate(0)
        att.qk(5)
        row_bias[pl.ds(2 * last, 1), :] = bias_row(full[0])
        att.soften(4)
        att.norm(3)
        att.mix(4)
        att.soften(5)
        att.norm(4)
        att.mix(5)
        row_bias[pl.ds(2 * last + 1, 1), :] = bias_row(full[1])
        att.norm(5)
        att.gate(1)

    send_pair(send_h, got_h, h_send_sem, h_recv_sem, pairs - 2)
    start_tail(pairs - 1)
    publish_bias(1)
    send_pair(send_h, got_h, h_send_sem, h_recv_sem, pairs - 1)
    for peer in peers:
        copy_bias(1, peer).start()

    wait_all(got_h, h_recv_sem)

    def spread(got):
        @pl.loop(0, group)
        def _(src):
            @pl.loop(0, pairs)
            def _(pair):
                start = pl.multiple_of((src * pairs + pair) * 2 * rows, 2 * rows)
                flat[pl.ds(start, 2 * rows), :] = got[src, pair].astype(F32)

    spread(got_h)

    def column(col):
        return flat[pl.ds(col, seq_len, stride=rows), :]

    for sub in range(2):
        stage(project(sub, duplicate_tail(layer_norm(column(sub))), wt_e, wp_e))

    wait_bias(1)
    for src in range(group):
        bias_t[rows * src:rows * src + rows] = got_bias[1, src].astype(F32)

    def end_mid(pair, sub, res):
        upd = merge_tail(res)
        return upd, layer_norm(column(2 * pair + sub) + upd)

    def widen(mid):
        return jnp.maximum(dot(mid[1], w1_ref[...]), 0.0).astype(BF16)

    def end_tail(pair):
        res = [out_dot(sub, wo_e) for sub in range(2)]
        mids = [end_mid(pair, sub, res[sub]) for sub in range(2)]
        hidden = [widen(mid) for mid in mids]
        delta = [mids[sub][0] + dot(hidden[sub], w2_ref[...]) for sub in range(2)]
        store_pair(send_d, got_d, pair, delta[0], delta[1])

    @pl.loop(0, pairs)
    def _(pair):
        @pl.when(pair > 1)
        def _():
            send_pair(send_d, got_d, d_send_sem, d_recv_sem, pair - 2)

        last = jnp.maximum(pair - 1, 0)
        ahead = jnp.minimum(pair + 1, pairs - 1)
        here = 2 * lax.rem(pair, 2)
        there = 2 - here
        att = Attention([here, here + 1])
        att.qk(0)
        res = [out_dot(sub, wo_e) for sub in range(2)]
        att.qk(1)
        normed = [duplicate_tail(layer_norm(column(2 * ahead + sub))) for sub in range(2)]
        att.soften(0)
        att.mix(0)
        made = project(there, normed[0], wt_e, wp_e)
        att.qk(2)
        mids = [end_mid(last, 0, res[0])]
        att.soften(1)
        att.norm(0)
        att.mix(1)
        stage(made)
        att.qk(3)
        mids.append(end_mid(last, 1, res[1]))
        hidden = [widen(mids[0])]
        att.soften(2)
        att.norm(1)
        att.mix(2)
        hidden.append(widen(mids[1]))
        att.qk(4)
        delta = [mids[0][0] + dot(hidden[0], w2_ref[...])]
        att.soften(3)
        att.norm(2)
        att.gate(0)
        att.mix(3)
        delta.append(mids[1][0] + dot(hidden[1], w2_ref[...]))
        att.qk(5)
        made = project(there + 1, normed[1], wt_e, wp_e)
        att.soften(4)
        att.norm(3)
        att.mix(4)
        stage(made)
        store_pair(send_d, got_d, last, delta[0], delta[1])
        att.soften(5)
        att.norm(4)
        att.mix(5)
        att.norm(5)
        att.gate(1)

    send_pair(send_d, got_d, d_send_sem, d_recv_sem, pairs - 2)
    end_tail(pairs - 1)
    send_pair(send_d, got_d, d_send_sem, d_recv_sem, pairs - 1)

    wait_all(got_d, d_recv_sem)
    spread(got_d)

    @pl.loop(0, rows)
    def _(row):
        y_ref[row] = y_ref[row] + column(row)

    for peer in peers:
        for phase in range(2):
            pltpu.make_async_copy(send_bias.at[phase], send_bias.at[phase], bias_send_sem.at[phase, peer]).wait()
        pltpu.make_async_copy(send_h.at[peer], send_h.at[peer], h_send_sem.at[peer]).wait()
        pltpu.make_async_copy(send_d.at[peer], send_d.at[peer], d_send_sem.at[peer]).wait()


def solution(mesh):
    row_spec = P(('dp', 'sp'), None, None)
    group = mesh.shape['sp']

    def local_fn(pair_loc, w_qkvg_s, w_bias_s, w_out_s, w_qkvg_e, w_bias_e, w_out_e, w_one, w_two):
        rows, seq_len, channels = pair_loc.shape
        heads = w_bias_s.shape[0]
        pairs = rows // 2
        vmem = pl.BlockSpec(memory_space=pltpu.VMEM)
        wide = heads * seq_len
        exchange = pltpu.VMEM((group, pairs, 2 * rows, channels), BF16)
        return pl.pallas_call(
            functools.partial(kernel, 'sp', group),
            out_shape=jax.ShapeDtypeStruct(pair_loc.shape, F32),
            in_specs=[vmem] * 9,
            out_specs=vmem,
            scratch_shapes=[
                pltpu.VMEM((3 * channels, channels), BF16),
                pltpu.VMEM((3 * channels, channels), BF16),
                pltpu.VMEM((rows, wide), F32),
                pltpu.VMEM((2, rows, wide), BF16),
                pltpu.VMEM((2, group, rows, wide), BF16),
                pltpu.VMEM((seq_len, wide), F32),
                pltpu.VMEM((rows, seq_len, channels), BF16),
                pltpu.VMEM((rows, channels, 256), BF16),
                pltpu.VMEM((rows, seq_len, channels), BF16),
                pltpu.VMEM((rows, channels, seq_len), BF16),
                pltpu.VMEM((rows, channels, 256), F32),
                pltpu.VMEM((2, channels, 256), BF16),
                exchange, exchange, exchange, exchange,
                pltpu.VMEM((rows * seq_len, channels), F32),
                pltpu.SemaphoreType.DMA((2, group)),
                pltpu.SemaphoreType.DMA((2, group)),
                pltpu.SemaphoreType.DMA((group,)),
                pltpu.SemaphoreType.DMA((group,)),
                pltpu.SemaphoreType.DMA((group,)),
                pltpu.SemaphoreType.DMA((group,)),
            ],
            compiler_params=pltpu.CompilerParams(collective_id=0, has_side_effects=True, vmem_limit_bytes=60 * 1024 * 1024),
        )(pair_loc, w_qkvg_s, w_bias_s, w_out_s, w_qkvg_e, w_bias_e, w_out_e, w_one, w_two)

    return jax.shard_map(local_fn, mesh=mesh, in_specs=(row_spec, P(), P(), P(), P(), P(), P(), P(), P()), out_specs=row_spec, check_vma=False)
```

```python
import functools

import jax
import jax.numpy as jnp
from jax import lax
from jax.experimental import pallas as pl
from jax.experimental.pallas import tpu as pltpu
from jax.sharding import PartitionSpec as P

LN_EPS = 1e-5
MESH = pl.DeviceIdType.MESH
F32 = jnp.float32
BF16 = jnp.bfloat16


def layer_norm(vals):
    mean_c = jnp.mean(vals, axis=-1, keepdims=True)
    centered = vals - mean_c
    variance = jnp.mean(centered * centered, axis=-1, keepdims=True)
    return (centered * lax.rsqrt(variance + LN_EPS)).astype(BF16)


def dot(lhs, rhs, lhs_dim=1, rhs_dim=0):
    return lax.dot_general(lhs, rhs, (((lhs_dim,), (rhs_dim,)), ((), ())), preferred_element_type=F32)


def duplicate_tail(normed):
    return jnp.concatenate([normed, normed[128:]], axis=0)


def low_half(shape):
    return lax.broadcasted_iota(jnp.int32, shape, len(shape) - 1) < 64


def bias_row(full):
    low = low_half((1, 128))
    tiles = []
    for first in (0, 2):
        head_a, head_b = full[first:first + 1], full[first + 1:first + 2]
        tiles += [head_a[:, :128], jnp.where(low, head_a[:, 128:], head_b[:, 128:]), head_b[:, :128]]
    return jnp.concatenate(tiles, axis=1)


def keep_low(val):
    return jnp.where(low_half(val.shape), val, jnp.zeros_like(val))


def keep_high(val):
    return jnp.where(low_half(val.shape), jnp.zeros_like(val), val)


def stack(rows):
    return jnp.concatenate([jnp.concatenate(row, axis=1) for row in rows], axis=0)


def score_block(q_t, tile):
    zero = jnp.zeros((32, 128), BF16)
    none = [zero, zero]

    def head(idx):
        return q_t[32 * idx:32 * idx + 32, :128], q_t[32 * idx:32 * idx + 32, 128:]

    first, second = head(tile), head(tile + 1)
    if tile == 0:
        return stack([[first[0], keep_low(first[1])], [zero, keep_high(second[1])], none, none])
    if tile == 1:
        return stack([none, [first[0], zero], [zero, second[0]], none])
    return stack([none, none, [keep_low(first[1]), zero], [keep_high(second[1]), second[0]]])


def gather_heads(outs, g_t):
    main = jnp.concatenate([outs[0][:32, :128], outs[1][:32, :128], outs[1][32:, 128:], outs[2][32:, 128:]], axis=0)
    tail = jnp.concatenate([keep_low(outs[0][:32, 128:]), keep_high(outs[0][32:, 128:]),
                            keep_low(outs[2][:32, :128]), keep_high(outs[2][32:, :128])], axis=0)
    return (jnp.concatenate([main, tail], axis=1) * g_t).astype(BF16)


def merge_tail(res):
    return jnp.concatenate([res[:128], res[128:192] + res[192:]], axis=0)


def kernel(axis, group, early, z_hbm, wp_s_hbm, wb_s_hbm, wo_s_hbm, wp_e_hbm, wb_e_hbm, wo_e_hbm, w1_hbm, w2_hbm, y_ref,
           z_ref, wp_s, wb_s, wo_s, wp_e, wb_e, wo_e, w1_ref, w2_ref,
           wt_s, wt_e, row_bias, send_bias, got_bias, bias_t, normed_sc, q_sc, k_sc, v_sc, g_sc, gated_sc,
           send_first, got_first, send_rest, got_rest, send_d, got_d, flat,
           z_sem, w_sem, bias_send_sem, bias_recv_sem, first_send_sem, first_recv_sem, rest_send_sem, rest_recv_sem,
           d_send_sem, d_recv_sem):
    rows, seq_len, channels = z_hbm.shape
    pairs = rows // 2
    chunk = 8
    chunks = rows // chunk
    late = 2 * pairs // 3
    scale = 32 ** -0.5
    me = lax.axis_index(axis)
    peers = [lax.rem(me + step, group) for step in range(1, group)]

    barrier = pltpu.get_barrier_semaphore()
    for peer in peers:
        pl.semaphore_signal(barrier, inc=1, device_id={axis: peer}, device_id_type=MESH)

    def load_z(idx):
        span = pl.ds(idx * chunk, chunk)
        return pltpu.make_async_copy(z_hbm.at[span], z_ref.at[span], z_sem.at[idx])

    loads = [pltpu.make_async_copy(src, dst, w_sem.at[idx]) for idx, (src, dst) in enumerate(
        ((wb_s_hbm, wb_s), (wp_s_hbm, wp_s), (wp_e_hbm, wp_e), (wo_s_hbm, wo_s), (wb_e_hbm, wb_e),
         (wo_e_hbm, wo_e), (w1_hbm, w1_ref), (w2_hbm, w2_ref)))]
    load_z(0).start()
    loads[0].start()
    loads[1].start()
    for idx in range(1, chunks):
        load_z(idx).start()
    for load in loads[2:]:
        load.start()

    def copy_bias(phase, part, peer):
        return pltpu.make_async_remote_copy(
            src_ref=send_bias.at[phase, part], dst_ref=got_bias.at[phase, me, part],
            send_sem=bias_send_sem.at[phase, peer], recv_sem=bias_recv_sem.at[phase, me],
            device_id={axis: peer}, device_id_type=MESH)

    def send_bias_part(phase, part):
        for peer in peers:
            copy_bias(phase, part, peer).start()

    def publish_bias(phase, part):
        rounded = row_bias[chunk * part:chunk * part + chunk].astype(BF16)
        send_bias[phase, part] = rounded
        got_bias[phase, me, part] = rounded

    def wait_bias(phase):
        for peer in peers:
            pltpu.make_async_copy(got_bias.at[phase, peer], got_bias.at[phase, peer], bias_recv_sem.at[phase, peer]).wait()

    def send_blocks(send, got, send_sem, recv_sem, start, count):
        span = pl.ds(start, count)
        for peer in peers:
            pltpu.make_async_remote_copy(
                src_ref=send.at[peer, span], dst_ref=got.at[me, span],
                send_sem=send_sem.at[peer], recv_sem=recv_sem.at[me],
                device_id={axis: peer}, device_id_type=MESH).start()

    def send_early(start, count):
        send_blocks(send_first, got_first, first_send_sem, first_recv_sem, start, count)

    def send_later(start, count):
        send_blocks(send_rest, got_rest, rest_send_sem, rest_recv_sem, start, count)

    def send_delta(pair):
        send_blocks(send_d, got_d, d_send_sem, d_recv_sem.at[pair // late], pair, 1)

    def wait_all(got, recv_sem):
        for peer in peers:
            pltpu.make_async_copy(got.at[peer], got.at[peer], recv_sem.at[peer]).wait()

    def store_block(send, got, pair, first, second, low, high):
        for dest in range(group):
            span = slice(rows * dest + low, rows * dest + high)
            send[dest, pair] = jnp.concatenate([first[span], second[span]], axis=0).astype(BF16)
        got[me, pair] = send[me, pair]

    def project(slot, normed_dup, wt, wp):
        cols = dot(wt[...], normed_dup, 1, 1)
        keys = dot(normed_dup[:seq_len], wp[:, channels:2 * channels])
        return slot, cols, keys

    def stage(projected):
        slot, cols, keys = projected
        q_sc[slot] = cols[:channels].astype(BF16)
        v_sc[slot] = cols[channels:2 * channels, :seq_len].astype(BF16)
        g_sc[slot] = jax.nn.sigmoid(cols[2 * channels:])
        k_sc[slot] = keys.astype(BF16)

    def transpose_weights(wp, wt):
        wt[0:channels] = wp[:, 0:channels].T
        wt[channels:2 * channels] = wp[:, 2 * channels:3 * channels].T
        wt[2 * channels:3 * channels] = wp[:, 3 * channels:].T

    class Attention:
        def __init__(self, slots):
            self.slots = slots
            self.score, self.prob, self.mixed, self.done = {}, {}, {}, {}

        def qk(self, unit):
            slot, tile = self.slots[unit // 3], unit % 3
            self.score[unit] = dot(k_sc[slot], score_block(q_sc[slot], tile))

        def soften(self, unit):
            tile = unit % 3
            scores = self.score.pop(unit) * scale + bias_t[:, 256 * tile:256 * tile + 256]
            top = jnp.max(scores, axis=0, keepdims=True)
            prob = jnp.exp(scores - top)
            self.prob[unit] = prob.astype(BF16), jnp.sum(prob, axis=0, keepdims=True)

        def mix(self, unit):
            slot, tile = self.slots[unit // 3], unit % 3
            prob, total = self.prob.pop(unit)
            self.mixed[unit] = dot(v_sc[slot, 32 * tile:32 * tile + 64], prob), total

        def norm(self, unit):
            mixed, total = self.mixed.pop(unit)
            self.done[unit] = mixed / total

        def gate(self, sub):
            outs = [self.done.pop(3 * sub + tile) for tile in range(3)]
            gated_sc[sub] = gather_heads(outs, g_sc[self.slots[sub]])

    def out_dot(sub, wo):
        return dot(gated_sc[sub].T, wo[...])

    batch = 4
    loads[0].wait()
    for part in range(chunks):
        load_z(part).wait()

        @pl.loop(0, chunk // batch)
        def _(step):
            base = chunk * part + step * batch
            normed = [layer_norm(z_ref[base + sub]) for sub in range(batch)]
            full = [dot(wb_s[...], duplicate_tail(val), 1, 1) for val in normed]
            for sub in range(batch):
                normed_sc[base + sub] = normed[sub]
            for sub in range(batch):
                row_bias[pl.ds(base + sub, 1), :] = bias_row(full[sub])

        publish_bias(0, part)
        if part == 0:
            loads[1].wait()
            transpose_weights(wp_s, wt_s)
            pl.semaphore_wait(barrier, group - 1)
        if part == 1:
            loads[2].wait()
            transpose_weights(wp_e, wt_e)
        if part == 2:
            stage(project(0, duplicate_tail(normed_sc[0]), wt_s, wp_s))
        send_bias_part(0, part)

    for load in loads[3:]:
        load.wait()

    @pl.loop(0, pairs)
    def _(step):
        made = [project(2 * step + sub, duplicate_tail(normed_sc[2 * step + sub]), wt_s, wp_s) for sub in range(2)]
        for val in made:
            stage(val)

    def bias_of(phase, src):
        return jnp.concatenate([got_bias[phase, src, part].astype(F32) for part in range(chunks)], axis=0)

    wait_bias(0)
    low = low_half((64, 128))
    by_query = jnp.concatenate([bias_of(0, src) for src in range(group)], axis=0)
    by_query = jnp.concatenate([by_query, by_query[128:]], axis=0)
    for first in (0, 1):
        base = 384 * first
        head_a = by_query[:, base:base + 128].T
        mixed = by_query[:, base + 128:base + 256].T
        head_b = by_query[:, base + 256:base + 384].T
        bias_t[0:128, base:base + 128] = head_a[:, :128]
        bias_t[128:192, base:base + 128] = mixed[:64, :128]
        low_a = low_half((128, 128))
        bias_t[0:128, base + 128:base + 256] = jnp.where(low_a, head_a[:, 128:], head_b[:, 128:])
        bias_t[128:192, base + 128:base + 256] = jnp.where(low, mixed[:64, 128:], mixed[64:, 128:])
        bias_t[0:128, base + 256:base + 384] = head_b[:, :128]
        bias_t[128:192, base + 256:base + 384] = mixed[64:, :128]

    def start_resid(pair, sub, res):
        row = 2 * pair + sub
        value = z_ref[row] + merge_tail(res)
        y_ref[row] = value
        return value, duplicate_tail(layer_norm(value.astype(BF16).astype(F32)))

    def store_h(pair, first, second):
        store_block(send_first, got_first, pair, first, second, 0, early)
        store_block(send_rest, got_rest, pair, first, second, early, rows)

    def start_tail(pair):
        res = [out_dot(sub, wo_s) for sub in range(2)]
        made = [start_resid(pair, sub, res[sub]) for sub in range(2)]
        full = [dot(wb_e[...], made[sub][1], 1, 1) for sub in range(2)]
        store_h(pair, made[0][0], made[1][0])
        for sub in range(2):
            row_bias[pl.ds(2 * pair + sub, 1), :] = bias_row(full[sub])

    @pl.loop(0, pairs)
    def _(pair):
        @pl.when(jnp.logical_and(pair > 2, lax.rem(pair, 2) == 1))
        def _():
            send_early(pair - 3, 2)

        @pl.when(jnp.logical_and(pair > 4, lax.rem(pair, 2) == 1))
        def _():
            send_later(pair - 5, 2)

        for part in range(chunks - 1):
            @pl.when(pair == (part + 1) * (chunk // 2) + 1)
            def _():
                publish_bias(1, part)

            @pl.when(pair == (part + 1) * (chunk // 2) + 2)
            def _():
                send_bias_part(1, part)

        last = jnp.maximum(pair - 1, 0)
        att = Attention([2 * pair, 2 * pair + 1])
        att.qk(0)
        res = [out_dot(sub, wo_s) for sub in range(2)]
        att.qk(1)
        att.soften(0)
        att.mix(0)
        att.qk(2)
        made = [start_resid(last, 0, res[0])]
        att.soften(1)
        att.norm(0)
        att.mix(1)
        att.qk(3)
        made.append(start_resid(last, 1, res[1]))
        full = [dot(wb_e[...], made[0][1], 1, 1)]
        att.soften(2)
        att.norm(1)
        att.mix(2)
        att.qk(4)
        full.append(dot(wb_e[...], made[1][1], 1, 1))
        store_h(last, made[0][0], made[1][0])
        att.soften(3)
        att.norm(2)
        att.mix(3)
        att.gate(0)
        att.qk(5)
        row_bias[pl.ds(2 * last, 1), :] = bias_row(full[0])
        att.soften(4)
        att.norm(3)
        att.mix(4)
        att.soften(5)
        att.norm(4)
        att.mix(5)
        row_bias[pl.ds(2 * last + 1, 1), :] = bias_row(full[1])
        att.norm(5)
        att.gate(1)

    start_tail(pairs - 1)
    publish_bias(1, chunks - 1)
    send_early(pairs - 2, 2)
    send_bias_part(1, chunks - 1)
    send_later(pairs - 4, 4)

    def spread(got, low, high):
        width = high - low

        @pl.loop(0, group)
        def _(src):
            @pl.loop(0, pairs)
            def _(pair):
                block = got[src, pair].astype(F32)
                for sub in range(2):
                    start = pl.multiple_of(((src * pairs + pair) * 2 + sub) * rows + low, 8)
                    flat[pl.ds(start, width), :] = block[width * sub:width * sub + width]

    def column(col):
        return flat[pl.ds(col, seq_len, stride=rows), :]

    wait_all(got_first, first_recv_sem)
    spread(got_first, 0, early)

    for sub in range(2):
        stage(project(sub, duplicate_tail(layer_norm(column(sub))), wt_e, wp_e))

    wait_bias(1)
    for src in range(group):
        bias_t[rows * src:rows * src + rows] = bias_of(1, src)

    def end_mid(pair, sub, res):
        upd = merge_tail(res)
        return upd, layer_norm(column(2 * pair + sub) + upd)

    def widen(mid):
        return jnp.maximum(dot(mid[1], w1_ref[...]), 0.0).astype(BF16)

    def end_tail(pair):
        res = [out_dot(sub, wo_e) for sub in range(2)]
        mids = [end_mid(pair, sub, res[sub]) for sub in range(2)]
        hidden = [widen(mid) for mid in mids]
        delta = [mids[sub][0] + dot(hidden[sub], w2_ref[...]) for sub in range(2)]
        store_block(send_d, got_d, pair, delta[0], delta[1], 0, rows)

    @pl.loop(0, pairs)
    def _(pair):
        @pl.when(pair == early // 2 - 1)
        def _():
            wait_all(got_rest, rest_recv_sem)
            spread(got_rest, early, rows)

        @pl.when(pair > 1)
        def _():
            send_delta(pair - 2)

        last = jnp.maximum(pair - 1, 0)
        ahead = jnp.minimum(pair + 1, pairs - 1)
        here = 2 * lax.rem(pair, 2)
        there = 2 - here
        att = Attention([here, here + 1])
        att.qk(0)
        res = [out_dot(sub, wo_e) for sub in range(2)]
        att.qk(1)
        normed = [duplicate_tail(layer_norm(column(2 * ahead + sub))) for sub in range(2)]
        att.soften(0)
        att.mix(0)
        made = project(there, normed[0], wt_e, wp_e)
        att.qk(2)
        mids = [end_mid(last, 0, res[0])]
        att.soften(1)
        att.norm(0)
        att.mix(1)
        stage(made)
        att.qk(3)
        mids.append(end_mid(last, 1, res[1]))
        hidden = [widen(mids[0])]
        att.soften(2)
        att.norm(1)
        att.mix(2)
        hidden.append(widen(mids[1]))
        att.qk(4)
        delta = [mids[0][0] + dot(hidden[0], w2_ref[...])]
        att.soften(3)
        att.norm(2)
        att.gate(0)
        att.mix(3)
        delta.append(mids[1][0] + dot(hidden[1], w2_ref[...]))
        att.qk(5)
        made = project(there + 1, normed[1], wt_e, wp_e)
        att.soften(4)
        att.norm(3)
        att.mix(4)
        stage(made)
        store_block(send_d, got_d, last, delta[0], delta[1], 0, rows)
        att.soften(5)
        att.norm(4)
        att.mix(5)
        att.norm(5)
        att.gate(1)

    send_delta(pairs - 2)
    end_tail(pairs - 1)
    send_delta(pairs - 1)

    def finish(part, first, count):
        span = pl.ds(first, count)
        for peer in peers:
            pltpu.make_async_copy(got_d.at[peer, span], got_d.at[peer, span], d_recv_sem.at[part, peer]).wait()

        @pl.loop(0, group)
        def _(src):
            @pl.loop(first, first + count)
            def _(pair):
                start = pl.multiple_of((src * pairs + pair) * 2 * rows, 2 * rows)
                flat[pl.ds(start, 2 * rows), :] = got_d[src, pair].astype(F32)

        @pl.loop(0, rows)
        def _(row):
            for src in range(group):
                low_col = rows * src + 2 * first
                y_ref[row, low_col:low_col + 2 * count] += flat[pl.ds(low_col * rows + row, 2 * count, stride=rows), :]

    finish(0, 0, late)
    finish(1, late, pairs - late)

    def drain(ref, sem):
        pltpu.make_async_copy(ref, ref, sem).wait()

    for peer in peers:
        for phase in range(2):
            drain(send_bias.at[phase], bias_send_sem.at[phase, peer])
        drain(send_first.at[peer], first_send_sem.at[peer])
        drain(send_rest.at[peer], rest_send_sem.at[peer])
        drain(send_d.at[peer], d_send_sem.at[peer])


def solution(mesh):
    row_spec = P(('dp', 'sp'), None, None)
    group = mesh.shape['sp']

    def local_fn(pair_loc, *weights):
        rows, seq_len, channels = pair_loc.shape
        heads = weights[1].shape[0]
        pairs = rows // 2
        wide = heads * seq_len
        early = 8
        chunk = 8
        hbm = pl.BlockSpec(memory_space=pltpu.HBM)

        def exchange(width):
            return pltpu.VMEM((group, pairs, 2 * width, channels), BF16)

        return pl.pallas_call(
            functools.partial(kernel, 'sp', group, early),
            out_shape=jax.ShapeDtypeStruct(pair_loc.shape, F32),
            in_specs=[hbm] * 9,
            out_specs=pl.BlockSpec(memory_space=pltpu.VMEM),
            scratch_shapes=[pltpu.VMEM(pair_loc.shape, F32)] + [pltpu.VMEM(val.shape, BF16) for val in weights] + [
                pltpu.VMEM((3 * channels, channels), BF16),
                pltpu.VMEM((3 * channels, channels), BF16),
                pltpu.VMEM((rows, wide), F32),
                pltpu.VMEM((2, rows // chunk, chunk, wide), BF16),
                pltpu.VMEM((2, group, rows // chunk, chunk, wide), BF16),
                pltpu.VMEM((seq_len, wide), F32),
                pltpu.VMEM((rows, seq_len, channels), BF16),
                pltpu.VMEM((rows, channels, 256), BF16),
                pltpu.VMEM((rows, seq_len, channels), BF16),
                pltpu.VMEM((rows, channels, seq_len), BF16),
                pltpu.VMEM((rows, channels, 256), F32),
                pltpu.VMEM((2, channels, 256), BF16),
                exchange(early), exchange(early), exchange(rows - early), exchange(rows - early), exchange(rows), exchange(rows),
                pltpu.VMEM((rows * seq_len, channels), F32),
                pltpu.SemaphoreType.DMA((rows // chunk,)),
                pltpu.SemaphoreType.DMA((8,)),
                pltpu.SemaphoreType.DMA((2, group)),
                pltpu.SemaphoreType.DMA((2, group)),
                pltpu.SemaphoreType.DMA((group,)),
                pltpu.SemaphoreType.DMA((group,)),
                pltpu.SemaphoreType.DMA((group,)),
                pltpu.SemaphoreType.DMA((group,)),
                pltpu.SemaphoreType.DMA((group,)),
                pltpu.SemaphoreType.DMA((2, group)),
            ],
            compiler_params=pltpu.CompilerParams(collective_id=0, has_side_effects=True, vmem_limit_bytes=34 * 1024 * 1024),
        )(*[pltpu.with_memory_space_constraint(val, pltpu.HBM) for val in (pair_loc, *weights)])

    return jax.shard_map(local_fn, mesh=mesh, in_specs=(row_spec, P(), P(), P(), P(), P(), P(), P(), P()), out_specs=row_spec, check_vma=False)
```

```python
import functools

import jax
import jax.numpy as jnp
from jax import lax
from jax.experimental import pallas as pl
from jax.experimental.pallas import tpu as pltpu
from jax.sharding import PartitionSpec as P

LN_EPS = 1e-5
Q_SHRINK = 0.125
SHRINK = 32 ** -0.5 / Q_SHRINK
LOG2_E = 1.4426950408889634
MESH = pl.DeviceIdType.MESH
F32 = jnp.float32
BF16 = jnp.bfloat16


def layer_norm(vals):
    mean_c = jnp.mean(vals, axis=-1, keepdims=True)
    centered = vals - mean_c
    variance = jnp.mean(centered * centered, axis=-1, keepdims=True)
    return (centered * lax.rsqrt(variance + LN_EPS)).astype(BF16)


def dot(lhs, rhs, lhs_dim=1, rhs_dim=0):
    return lax.dot_general(lhs, rhs, (((lhs_dim,), (rhs_dim,)), ((), ())), preferred_element_type=F32)


def duplicate_tail(normed):
    return jnp.concatenate([normed, normed[128:]], axis=0)


def low_half(shape):
    return lax.broadcasted_iota(jnp.int32, shape, len(shape) - 1) < 64


def bias_row(full):
    low = low_half((1, 128))
    tiles = []
    for first in (0, 2):
        head_a, head_b = full[first:first + 1], full[first + 1:first + 2]
        tiles += [head_a[:, :128], jnp.where(low, head_a[:, 128:], head_b[:, 128:]), head_b[:, :128]]
    return jnp.concatenate(tiles, axis=1)


def keep_low(val):
    return jnp.where(low_half(val.shape), val, jnp.zeros_like(val))


def keep_high(val):
    return jnp.where(low_half(val.shape), jnp.zeros_like(val), val)


def stack(rows):
    return jnp.concatenate([jnp.concatenate(row, axis=1) for row in rows], axis=0)


def score_block(q_t, tile):
    zero = jnp.zeros((32, 128), BF16)
    none = [zero, zero]

    def head(idx):
        return q_t[32 * idx:32 * idx + 32, :128], q_t[32 * idx:32 * idx + 32, 128:]

    first, second = head(tile), head(tile + 1)
    if tile == 0:
        return stack([[first[0], keep_low(first[1])], [zero, keep_high(second[1])], none, none])
    if tile == 1:
        return stack([none, [first[0], zero], [zero, second[0]], none])
    return stack([none, none, [keep_low(first[1]), zero], [keep_high(second[1]), second[0]]])


def gather_heads(outs, g_t):
    main = jnp.concatenate([outs[0][:32, :128], outs[1][:32, :128], outs[1][32:, 128:], outs[2][32:, 128:]], axis=0)
    tail = jnp.concatenate([keep_low(outs[0][:32, 128:]), keep_high(outs[0][32:, 128:]),
                            keep_low(outs[2][:32, :128]), keep_high(outs[2][32:, :128])], axis=0)
    return (jnp.concatenate([main, tail], axis=1) * g_t).astype(BF16)


def merge_tail(res):
    return jnp.concatenate([res[:128], res[128:192] + res[192:]], axis=0)


def kernel(axis, group, early, z_hbm, wp_s_hbm, wb_s_hbm, wo_s_hbm, wp_e_hbm, wb_e_hbm, wo_e_hbm, w1_hbm, w2_hbm, y_ref,
           z_ref, wp_s, wb_s, wo_s, wp_e, wb_e, wo_e, w1_ref, w2_ref,
           wt_s, wt_e, row_bias, send_bias, got_bias, bias_t, normed_sc, q_sc, k_sc, v_sc, g_sc, gated_sc, part_sc, top_sc,
           send_first, got_first, send_rest, got_rest, send_d, got_d, flat,
           z_sem, w_sem, bias_send_sem, bias_recv_sem, pass_send_sem, first_send_sem, first_recv_sem, rest_send_sem, rest_recv_sem,
           d_send_sem, d_recv_sem):
    rows, seq_len, channels = z_hbm.shape
    pairs = rows // 2
    chunk = 8
    chunks = rows // chunk
    late = pairs - 3
    later = rows // early - 1
    held = pairs - 7
    me = lax.axis_index(axis)
    half = group // 2
    order = sorted(range(1, group), key=lambda step: abs(step - half))
    peers = [lax.rem(me + step, group) for step in order]
    partner = me + 1 - 2 * lax.rem(me, 2)
    alike = [lax.rem(me + step, group) for step in order if step % 2 == 0]
    others = [lax.rem(partner + step, group) for step in order if step % 2 == 0]

    barrier = pltpu.get_barrier_semaphore()
    for peer in peers:
        pl.semaphore_signal(barrier, inc=1, device_id={axis: peer}, device_id_type=MESH)

    def load_z(idx):
        span = pl.ds(idx * chunk, chunk)
        return pltpu.make_async_copy(z_hbm.at[span], z_ref.at[span], z_sem.at[idx])

    loads = [pltpu.make_async_copy(src, dst, w_sem.at[idx]) for idx, (src, dst) in enumerate(
        ((wb_s_hbm, wb_s), (wp_s_hbm, wp_s), (wp_e_hbm, wp_e), (wo_s_hbm, wo_s), (wb_e_hbm, wb_e),
         (wo_e_hbm, wo_e), (w1_hbm, w1_ref), (w2_hbm, w2_ref)))]
    load_z(0).start()
    loads[0].start()
    loads[1].start()
    for idx in range(1, chunks):
        load_z(idx).start()
    for load in loads[2:]:
        load.start()

    def send_bias_part(phase, part, count=1):
        span = pl.ds(part, count)
        for peer in peers if phase == 0 else alike + [partner]:
            pltpu.make_async_remote_copy(
                src_ref=send_bias.at[phase, span], dst_ref=got_bias.at[phase, me, span],
                send_sem=bias_send_sem.at[phase, peer], recv_sem=bias_recv_sem.at[phase, me],
                device_id={axis: peer}, device_id_type=MESH).start()

    def wait_for_bias(phase, src):
        pltpu.make_async_copy(got_bias.at[phase, src], got_bias.at[phase, src], bias_recv_sem.at[phase, src]).wait()

    def forward_bias(phase):
        for src in alike:
            wait_for_bias(phase, src)
            pltpu.make_async_remote_copy(
                src_ref=got_bias.at[phase, src], dst_ref=got_bias.at[phase, src],
                send_sem=pass_send_sem.at[src], recv_sem=bias_recv_sem.at[phase, src],
                device_id={axis: partner}, device_id_type=MESH).start()

    def publish_bias(phase, part):
        rounded = row_bias[chunk * part:chunk * part + chunk].astype(BF16)
        send_bias[phase, part] = rounded
        got_bias[phase, me, part] = rounded

    def wait_bias(phase):
        for src in peers if phase == 0 else [partner] + others:
            wait_for_bias(phase, src)

    def send_blocks(send, got, send_sem, recv_sem, start, count):
        span = pl.ds(start, count)
        for peer in peers:
            pltpu.make_async_remote_copy(
                src_ref=send.at[peer, span], dst_ref=got.at[me, span],
                send_sem=send_sem.at[peer], recv_sem=recv_sem.at[me],
                device_id={axis: peer}, device_id_type=MESH).start()

    def send_early(start, count):
        send_blocks(send_first, got_first, first_send_sem, first_recv_sem.at[int(isinstance(start, int) and start == pairs - 1)], start, count)

    def send_later(start, count):
        span = pl.ds(start, count)
        for peer in peers:
            pltpu.make_async_remote_copy(
                src_ref=send_rest.at[peer, :, span], dst_ref=got_rest.at[me, :, span],
                send_sem=rest_send_sem.at[0, peer], recv_sem=rest_recv_sem.at[0, me],
                device_id={axis: peer}, device_id_type=MESH).start()

    def send_last(idx, start, count):
        span = pl.ds(start, count)
        for peer in peers:
            pltpu.make_async_remote_copy(
                src_ref=send_rest.at[peer, idx, span], dst_ref=got_rest.at[me, idx, span],
                send_sem=rest_send_sem.at[1 + idx, peer], recv_sem=rest_recv_sem.at[1 + idx, me],
                device_id={axis: peer}, device_id_type=MESH).start()

    def send_delta(start, count):
        send_blocks(send_d, got_d, d_send_sem, d_recv_sem.at[start // late], start, count)

    def store_block(send, got, pair, first, second, low, high):
        for dest in range(group):
            span = slice(rows * dest + low, rows * dest + high)
            send[dest, pair] = jnp.concatenate([first[span], second[span]], axis=0).astype(BF16)
        got[me, pair] = send[me, pair]

    def project(slot, normed_dup, wt, wp):
        cols = dot(wt[...], normed_dup, 1, 1)
        keys = dot(normed_dup[:seq_len], wp[:, channels:2 * channels])
        return slot, cols, keys

    def stage(projected):
        slot, cols, keys = projected
        q_sc[slot] = cols[:channels].astype(BF16)
        v_sc[slot] = cols[channels:2 * channels, :seq_len].astype(BF16)
        g_sc[slot] = jax.nn.sigmoid(cols[2 * channels:])
        k_sc[slot] = keys.astype(BF16)

    def transpose_weights(wp, wt):
        wt[0:channels] = wp[:, 0:channels].T * jnp.asarray(Q_SHRINK, BF16)
        wt[channels:2 * channels] = wp[:, 2 * channels:3 * channels].T
        wt[2 * channels:3 * channels] = wp[:, 3 * channels:].T

    class Attention:
        def __init__(self, slots):
            self.slots = slots
            self.score, self.prob, self.mixed, self.done = {}, {}, {}, {}

        def qk(self, unit):
            slot, tile = self.slots[unit // 3], unit % 3
            self.score[unit] = dot(k_sc[slot], score_block(q_sc[slot], tile))

        def biased(self, unit, half):
            at = 256 * (unit % 3) + 128 * half
            return self.score[unit][:, 128 * half:128 * half + 128] + bias_t[:, at:at + 128]

        def hand_on(self, unit):
            for half in range(2):
                part = self.biased(unit, half)
                part_sc[unit % 3, half] = part
                top_sc[unit % 3, half] = jnp.max(part, axis=0, keepdims=True)

        def soften(self, unit):
            probs, totals = [], []
            for half in range(2):
                if unit in self.score:
                    part = self.biased(unit, half)
                    top = jnp.max(part, axis=0, keepdims=True)
                else:
                    part, top = part_sc[unit, half], top_sc[unit, half]
                prob = jnp.exp2((part - top) * (SHRINK * LOG2_E))
                totals.append(jnp.sum(prob, axis=0, keepdims=True))
                probs.append(prob.astype(BF16))
            self.prob[unit] = jnp.concatenate(probs, axis=1), jnp.concatenate(totals, axis=1)

        def mix(self, unit):
            slot, tile = self.slots[unit // 3], unit % 3
            prob, total = self.prob.pop(unit)
            self.mixed[unit] = dot(v_sc[slot, 32 * tile:32 * tile + 64], prob), total

        def norm(self, unit):
            mixed, total = self.mixed.pop(unit)
            self.done[unit] = mixed / total

        def gate(self, sub):
            outs = [self.done.pop(3 * sub + tile) for tile in range(3)]
            gated_sc[sub] = gather_heads(outs, g_sc[self.slots[sub]])

    def out_dot(sub, wo):
        return dot(gated_sc[sub].T, wo[...])

    loads[0].wait()
    for part in range(chunks):
        load_z(part).wait()
        base = chunk * part
        normed = [layer_norm(z_ref[base + sub]) for sub in range(chunk)]
        full = [dot(wb_s[...], duplicate_tail(val), 1, 1) for val in normed]
        for sub in range(chunk):
            normed_sc[base + sub] = normed[sub]
        for sub in range(chunk):
            row_bias[base + sub:base + sub + 1, :] = bias_row(full[sub])
        publish_bias(0, part)
        if part == chunks - 2:
            loads[1].wait()
            transpose_weights(wp_s, wt_s)
            pl.semaphore_wait(barrier, group - 1)
            send_bias_part(0, 0, chunks - 1)
        if part == chunks - 1:
            loads[2].wait()
            transpose_weights(wp_e, wt_e)
            send_bias_part(0, chunks - 1)

    for load in loads[3:]:
        load.wait()

    @pl.loop(0, pairs)
    def _(step):
        made = [project(2 * step + sub, duplicate_tail(normed_sc[2 * step + sub]), wt_s, wp_s) for sub in range(2)]
        for val in made:
            stage(val)

    def bias_of(phase, src):
        return jnp.concatenate([got_bias[phase, src, part].astype(F32) for part in range(chunks)], axis=0)

    wait_bias(0)
    low = low_half((64, 128))
    by_query = jnp.concatenate([bias_of(0, src) for src in range(group)], axis=0) * (1 / SHRINK)
    by_query = jnp.concatenate([by_query, by_query[128:]], axis=0)
    for first in (0, 1):
        base = 384 * first
        head_a = by_query[:, base:base + 128].T
        mixed = by_query[:, base + 128:base + 256].T
        head_b = by_query[:, base + 256:base + 384].T
        bias_t[0:128, base:base + 128] = head_a[:, :128]
        bias_t[128:192, base:base + 128] = mixed[:64, :128]
        low_a = low_half((128, 128))
        bias_t[0:128, base + 128:base + 256] = jnp.where(low_a, head_a[:, 128:], head_b[:, 128:])
        bias_t[128:192, base + 128:base + 256] = jnp.where(low, mixed[:64, 128:], mixed[64:, 128:])
        bias_t[0:128, base + 256:base + 384] = head_b[:, :128]
        bias_t[128:192, base + 256:base + 384] = mixed[64:, :128]

    def start_resid(pair, sub, res):
        row = 2 * pair + sub
        value = z_ref[row] + merge_tail(res)
        y_ref[row] = value
        return value

    def store_h(pair, first, second):
        store_block(send_first, got_first, pair, first, second, 0, early)
        for idx in range(later):
            for dest in range(group):
                low = rows * dest + early * (idx + 1)
                span = slice(low, low + early)
                send_rest[dest, idx, pair] = jnp.concatenate([first[span], second[span]], axis=0).astype(BF16)
            got_rest[me, idx, pair] = send_rest[me, idx, pair]

    def end_normed(pair, sub):
        return duplicate_tail(layer_norm(y_ref[2 * pair + sub].astype(BF16).astype(F32)))

    def prime(slot):
        att = Attention([slot])
        for unit in range(2):
            att.qk(unit)
        for unit in range(2):
            att.hand_on(unit)

    prime(0)

    @pl.loop(0, pairs)
    def _(pair):
        even = lax.rem(pair, 2) == 0
        for part in range(chunks - 1):
            @pl.when(pair == chunk // 2 * (part + 1) + 2)
            def _():
                publish_bias(1, part)

        @pl.when(pair == 2)
        def _():
            send_early(0, 1)

        @pl.when(jnp.logical_and(pair > 2, even))
        def _():
            send_early(pair - 3, 2)

        @pl.when(pair == pairs - 1)
        def _():
            send_early(pairs - 3, 1)

        @pl.when(pair == 4)
        def _():
            send_later(0, 1)

        @pl.when(jnp.logical_and(jnp.logical_and(pair > 4, pair < held + 5), even))
        def _():
            send_later(pair - 5, 2)

        for part in range(chunks - 1):
            @pl.when(pair == chunk // 2 * (part + 1) + 2)
            def _():
                send_bias_part(1, part)

        last = jnp.maximum(pair - 1, 0)
        older = jnp.maximum(pair - 2, 0)
        att = Attention([2 * pair, 2 * pair + 1, 2 * jnp.minimum(pair + 1, pairs - 1)])
        att.qk(2)
        att.qk(3)
        normed = [end_normed(older, sub) for sub in range(2)]
        att.soften(0)
        att.mix(0)
        res = [out_dot(sub, wo_s) for sub in range(2)]
        att.soften(1)
        att.mix(1)
        full = [dot(wb_e[...], val, 1, 1) for val in normed]
        att.qk(4)
        made = [start_resid(last, 0, res[0])]
        att.soften(2)
        att.norm(0)
        att.mix(2)
        att.qk(5)
        made.append(start_resid(last, 1, res[1]))
        att.soften(3)
        att.norm(1)
        att.mix(3)
        att.qk(6)
        for sub in range(2):
            row_bias[pl.ds(2 * older + sub, 1), :] = bias_row(full[sub])
        att.soften(4)
        att.norm(2)
        att.gate(0)
        att.mix(4)
        att.qk(7)
        att.soften(5)
        att.norm(3)
        att.mix(5)
        store_h(last, made[0], made[1])
        att.hand_on(6)
        att.norm(4)
        att.hand_on(7)
        att.norm(5)
        att.gate(1)

    send_early(pairs - 2, 1)
    res = [out_dot(sub, wo_s) for sub in range(2)]
    made = [start_resid(pairs - 1, sub, res[sub]) for sub in range(2)]
    store_h(pairs - 1, made[0], made[1])
    ends = [(pair, sub) for pair in (pairs - 2, pairs - 1) for sub in range(2)]
    full = [dot(wb_e[...], end_normed(pair, sub), 1, 1) for pair, sub in ends]
    send_early(pairs - 1, 1)
    for (pair, sub), val in zip(ends, full):
        row_bias[2 * pair + sub:2 * pair + sub + 1, :] = bias_row(val)
    publish_bias(1, chunks - 1)
    send_last(0, held, pairs - held)
    send_bias_part(1, chunks - 1)
    send_last(1, held, pairs - held)

    def wait_blocks(view, recv_sem):
        for peer in peers:
            pltpu.make_async_copy(view(peer), view(peer), recv_sem.at[peer]).wait()

    def spread(view, low, first, count):
        @pl.loop(0, group)
        def _(src):
            for pair in range(first, first + count):
                block = view(src)[pair].astype(F32)
                for sub in range(2):
                    start = pl.multiple_of(((src * pairs + pair) * 2 + sub) * rows + low, 8)
                    flat[pl.ds(start, early), :] = block[early * sub:early * sub + early]

    def spread_rest(idx):
        if idx == 0:
            wait_blocks(lambda src: got_rest.at[src, :, pl.ds(0, held)], rest_recv_sem.at[0])
        wait_blocks(lambda src: got_rest.at[src, idx, pl.ds(held, pairs - held)], rest_recv_sem.at[1 + idx])
        spread(lambda src: got_rest.at[src, idx], early * (idx + 1), 0, pairs)

    def column(col):
        return flat[pl.ds(col, seq_len, stride=rows), :]

    wait_blocks(lambda src: got_first.at[src, pl.ds(0, pairs - 1)], first_recv_sem.at[0])
    spread(lambda src: got_first.at[src], 0, 0, pairs - 1)
    wait_blocks(lambda src: got_first.at[src, pl.ds(pairs - 1, 1)], first_recv_sem.at[1])
    spread(lambda src: got_first.at[src], 0, pairs - 1, 1)
    forward_bias(1)

    for sub in range(2):
        stage(project(sub, duplicate_tail(layer_norm(column(sub))), wt_e, wp_e))

    wait_bias(1)
    for src in range(group):
        bias_t[rows * src:rows * src + rows] = bias_of(1, src) * (1 / SHRINK)

    prime(0)

    def end_mid(pair, sub, res):
        upd = merge_tail(res)
        return upd, layer_norm(column(2 * pair + sub) + upd)

    def widen(mid):
        return jnp.maximum(dot(mid[1], w1_ref[...]), 0.0).astype(BF16)

    def end_tail(pair):
        res = [out_dot(sub, wo_e) for sub in range(2)]
        mids = [end_mid(pair, sub, res[sub]) for sub in range(2)]
        hidden = [widen(mid) for mid in mids]
        delta = [mids[sub][0] + dot(hidden[sub], w2_ref[...]) for sub in range(2)]
        store_block(send_d, got_d, pair, delta[0], delta[1], 0, rows)

    @pl.loop(0, pairs)
    def _(pair):
        for idx in range(later):
            @pl.when(pair == early // 2 * (idx + 1) - 1)
            def _():
                spread_rest(idx)

        @pl.when(pair == 2)
        def _():
            send_delta(0, 1)

        @pl.when(jnp.logical_and(pair > 2, lax.rem(pair, 2) == 0))
        def _():
            send_delta(pair - 3, 2)

        @pl.when(pair == pairs - 1)
        def _():
            send_delta(pairs - 3, 1)

        last = jnp.maximum(pair - 1, 0)
        ahead = jnp.minimum(pair + 1, pairs - 1)
        here = 2 * lax.rem(pair, 2)
        there = 2 - here
        att = Attention([here, here + 1, there])
        att.qk(2)
        att.qk(3)
        normed = [duplicate_tail(layer_norm(column(2 * ahead + sub))) for sub in range(2)]
        att.soften(0)
        att.mix(0)
        res = [out_dot(sub, wo_e) for sub in range(2)]
        att.soften(1)
        att.mix(1)
        made = project(there, normed[0], wt_e, wp_e)
        att.qk(4)
        mids = [end_mid(last, 0, res[0])]
        att.soften(2)
        att.norm(0)
        att.mix(2)
        stage(made)
        att.qk(5)
        mids.append(end_mid(last, 1, res[1]))
        hidden = [widen(mids[0])]
        att.soften(3)
        att.norm(1)
        att.mix(3)
        hidden.append(widen(mids[1]))
        att.qk(6)
        delta = [mids[0][0] + dot(hidden[0], w2_ref[...])]
        att.soften(4)
        att.norm(2)
        att.gate(0)
        att.mix(4)
        made = project(there + 1, normed[1], wt_e, wp_e)
        att.qk(7)
        delta.append(mids[1][0] + dot(hidden[1], w2_ref[...]))
        att.soften(5)
        att.norm(3)
        att.mix(5)
        stage(made)
        store_block(send_d, got_d, last, delta[0], delta[1], 0, rows)
        att.hand_on(6)
        att.norm(4)
        att.hand_on(7)
        att.norm(5)
        att.gate(1)

    send_delta(pairs - 2, 1)
    end_tail(pairs - 1)
    send_delta(pairs - 1, 1)

    def finish(part, first, count):
        span = pl.ds(first, count)
        for peer in peers:
            pltpu.make_async_copy(got_d.at[peer, span], got_d.at[peer, span], d_recv_sem.at[part, peer]).wait()

        @pl.loop(0, group)
        def _(src):
            for pair in range(first, first + count):
                start = pl.multiple_of((src * pairs + pair) * 2 * rows, 2 * rows)
                flat[pl.ds(start, 2 * rows), :] = got_d[src, pair].astype(F32)

        @pl.loop(0, rows)
        def _(row):
            for src in range(group):
                low_col = rows * src + 2 * first
                y_ref[row, low_col:low_col + 2 * count] += flat[pl.ds(low_col * rows + row, 2 * count, stride=rows), :]

    finish(0, 0, late)
    finish(1, late, pairs - late)

    def drain(ref, sem):
        pltpu.make_async_copy(ref, ref, sem).wait()

    for phase in range(2):
        for peer in peers if phase == 0 else alike + [partner]:
            drain(send_bias.at[phase], bias_send_sem.at[phase, peer])
    for src in alike:
        drain(got_bias.at[1, src], pass_send_sem.at[src])
    for peer in peers:
        drain(send_first.at[peer], first_send_sem.at[peer])
        drain(send_rest.at[peer, :, pl.ds(0, held)], rest_send_sem.at[0, peer])
        for idx in range(later):
            drain(send_rest.at[peer, idx, pl.ds(held, pairs - held)], rest_send_sem.at[1 + idx, peer])
        drain(send_d.at[peer], d_send_sem.at[peer])


def solution(mesh):
    row_spec = P(('dp', 'sp'), None, None)
    group = mesh.shape['sp']

    def local_fn(pair_loc, *weights):
        rows, seq_len, channels = pair_loc.shape
        heads = weights[1].shape[0]
        pairs = rows // 2
        wide = heads * seq_len
        early = 8
        chunk = 8
        hbm = pl.BlockSpec(memory_space=pltpu.HBM)

        later = pltpu.VMEM((group, rows // early - 1, pairs, 2 * early, channels), BF16)

        def exchange(width):
            return pltpu.VMEM((group, pairs, 2 * width, channels), BF16)

        return pl.pallas_call(
            functools.partial(kernel, 'sp', group, early),
            out_shape=jax.ShapeDtypeStruct(pair_loc.shape, F32),
            in_specs=[hbm] * 9,
            out_specs=pl.BlockSpec(memory_space=pltpu.VMEM),
            scratch_shapes=[pltpu.VMEM(pair_loc.shape, F32)] + [pltpu.VMEM(val.shape, BF16) for val in weights] + [
                pltpu.VMEM((3 * channels, channels), BF16),
                pltpu.VMEM((3 * channels, channels), BF16),
                pltpu.VMEM((rows, wide), F32),
                pltpu.VMEM((2, rows // chunk, chunk, wide), BF16),
                pltpu.VMEM((2, group, rows // chunk, chunk, wide), BF16),
                pltpu.VMEM((seq_len, wide), F32),
                pltpu.VMEM((rows, seq_len, channels), BF16),
                pltpu.VMEM((rows, channels, 256), BF16),
                pltpu.VMEM((rows, seq_len, channels), BF16),
                pltpu.VMEM((rows, channels, seq_len), BF16),
                pltpu.VMEM((rows, channels, 256), F32),
                pltpu.VMEM((2, channels, 256), BF16),
                pltpu.VMEM((2, 2, seq_len, 128), F32),
                pltpu.VMEM((2, 2, 1, 128), F32),
                exchange(early), exchange(early), later, later, exchange(rows), exchange(rows),
                pltpu.VMEM((rows * seq_len, channels), F32),
                pltpu.SemaphoreType.DMA((rows // chunk,)),
                pltpu.SemaphoreType.DMA((8,)),
                pltpu.SemaphoreType.DMA((2, group)),
                pltpu.SemaphoreType.DMA((2, group)),
                pltpu.SemaphoreType.DMA((group,)),
                pltpu.SemaphoreType.DMA((group,)),
                pltpu.SemaphoreType.DMA((2, group)),
                pltpu.SemaphoreType.DMA((rows // early, group)),
                pltpu.SemaphoreType.DMA((rows // early, group)),
                pltpu.SemaphoreType.DMA((group,)),
                pltpu.SemaphoreType.DMA((2, group)),
            ],
            compiler_params=pltpu.CompilerParams(collective_id=0, has_side_effects=True, vmem_limit_bytes=34 * 1024 * 1024),
        )(*[pltpu.with_memory_space_constraint(val, pltpu.HBM) for val in (pair_loc, *weights)])

    return jax.shard_map(local_fn, mesh=mesh, in_specs=(row_spec, P(), P(), P(), P(), P(), P(), P(), P()), out_specs=row_spec, check_vma=False)
```

```python
import functools

import jax
import jax.numpy as jnp
from jax import lax
from jax.experimental import pallas as pl
from jax.experimental.pallas import tpu as pltpu
from jax.sharding import PartitionSpec as P

LN_EPS = 1e-5
LANES = 128
DOUBLE = 256
HALF = 64
HEAD = 32
Q_SHRINK = 0.125
SHRINK = 32 ** -0.5 / Q_SHRINK
LOG2_E = 1.4426950408889634
MESH = pl.DeviceIdType.MESH
F32 = jnp.float32
BF16 = jnp.bfloat16


def layer_norm(vals):
    mean_c = jnp.mean(vals, axis=-1, keepdims=True)
    centered = vals - mean_c
    variance = jnp.mean(centered * centered, axis=-1, keepdims=True)
    return (centered * lax.rsqrt(variance + LN_EPS)).astype(BF16)


def dot(lhs, rhs, lhs_dim=1, rhs_dim=0):
    return lax.dot_general(lhs, rhs, (((lhs_dim,), (rhs_dim,)), ((), ())), preferred_element_type=F32)


def duplicate_tail(normed):
    return jnp.concatenate([normed, normed[LANES:]], axis=0)


def low_half(shape):
    return lax.broadcasted_iota(jnp.int32, shape, len(shape) - 1) < HALF


def bias_row(full):
    low = low_half((1, LANES))
    tiles = []
    for first in (0, 2):
        head_a, head_b = full[first:first + 1], full[first + 1:first + 2]
        tiles += [head_a[:, :LANES], jnp.where(low, head_a[:, LANES:], head_b[:, LANES:]), head_b[:, :LANES]]
    return jnp.concatenate(tiles, axis=1)


def keep_low(val):
    return jnp.where(low_half(val.shape), val, jnp.zeros_like(val))


def keep_high(val):
    return jnp.where(low_half(val.shape), jnp.zeros_like(val), val)


def stack(rows):
    return jnp.concatenate([jnp.concatenate(row, axis=1) for row in rows], axis=0)


def score_block(q_t, tile):
    zero = jnp.zeros((HEAD, LANES), BF16)
    none = [zero, zero]

    def head(idx):
        return q_t[HEAD * idx:HEAD * idx + HEAD, :LANES], q_t[HEAD * idx:HEAD * idx + HEAD, LANES:]

    first, second = head(tile), head(tile + 1)
    if tile == 0:
        return stack([[first[0], keep_low(first[1])], [zero, keep_high(second[1])], none, none])
    if tile == 1:
        return stack([none, [first[0], zero], [zero, second[0]], none])
    return stack([none, none, [keep_low(first[1]), zero], [keep_high(second[1]), second[0]]])


def gather_heads(outs, g_t):
    main = jnp.concatenate([outs[0][:HEAD, :LANES], outs[1][:HEAD, :LANES], outs[1][HEAD:, LANES:], outs[2][HEAD:, LANES:]], axis=0)
    tail = jnp.concatenate([keep_low(outs[0][:HEAD, LANES:]), keep_high(outs[0][HEAD:, LANES:]),
                            keep_low(outs[2][:HEAD, :LANES]), keep_high(outs[2][HEAD:, :LANES])], axis=0)
    return (jnp.concatenate([main, tail], axis=1) * g_t).astype(BF16)


def merge_tail(res):
    return jnp.concatenate([res[:LANES], res[LANES:192] + res[192:]], axis=0)


def kernel(axis, group, early, z_hbm, wp_s_hbm, wb_s_hbm, wo_s_hbm, wp_e_hbm, wb_e_hbm, wo_e_hbm, w1_hbm, w2_hbm, y_ref,
           z_ref, wp_s, wb_s, wo_s, wp_e, wb_e, wo_e, w1_ref, w2_ref,
           wt_s, wt_e, row_bias, send_bias, got_bias, bias_t, normed_sc, q_sc, k_sc, v_sc, g_sc, gated_sc, part_sc, top_sc,
           send_h, got_h, send_d, got_d, flat,
           z_sem, w_sem, bias_send_sem, bias_recv_sem, pass_send_sem, h_send_sem, h_recv_sem, d_send_sem, d_recv_sem):
    rows, seq_len, channels = z_hbm.shape
    pairs = rows // 2
    chunk = 8
    chunks = rows // chunk
    late = pairs - 3
    groups = rows // early
    held = pairs - 7
    me = lax.axis_index(axis)
    half = group // 2
    order = sorted(range(1, group), key=lambda step: abs(step - half))
    peers = [lax.rem(me + step, group) for step in order]
    partner = me + 1 - 2 * lax.rem(me, 2)
    alike = [lax.rem(me + step, group) for step in order if step % 2 == 0]
    others = [lax.rem(partner + step, group) for step in order if step % 2 == 0]

    barrier = pltpu.get_barrier_semaphore()
    for peer in peers:
        pl.semaphore_signal(barrier, inc=1, device_id={axis: peer}, device_id_type=MESH)

    def load_z(idx):
        span = pl.ds(idx * chunk, chunk)
        return pltpu.make_async_copy(z_hbm.at[span], z_ref.at[span], z_sem.at[idx])

    loads = [pltpu.make_async_copy(src, dst, w_sem.at[idx]) for idx, (src, dst) in enumerate(
        ((wb_s_hbm, wb_s), (wp_s_hbm, wp_s), (wp_e_hbm, wp_e), (wo_s_hbm, wo_s), (wb_e_hbm, wb_e),
         (wo_e_hbm, wo_e), (w1_hbm, w1_ref), (w2_hbm, w2_ref)))]
    load_z(0).start()
    loads[0].start()
    loads[1].start()
    for idx in range(1, chunks):
        load_z(idx).start()
    for load in loads[2:]:
        load.start()

    def send_bias_part(phase, part, count, to, sem):
        span = pl.ds(part, count)
        for peer in to:
            pltpu.make_async_remote_copy(
                src_ref=send_bias.at[phase, span], dst_ref=got_bias.at[phase, me, span],
                send_sem=bias_send_sem.at[sem, peer], recv_sem=bias_recv_sem.at[sem, me],
                device_id={axis: peer}, device_id_type=MESH).start()

    def drain(ref, sem):
        pltpu.make_async_copy(ref, ref, sem).wait()

    most, final = pl.ds(0, chunks - 1), pl.ds(chunks - 1, 1)

    def forward_bias():
        for src in alike:
            view = got_bias.at[1, src, most]
            drain(view, bias_recv_sem.at[1, src])
            pltpu.make_async_remote_copy(
                src_ref=view, dst_ref=view,
                send_sem=pass_send_sem.at[src], recv_sem=bias_recv_sem.at[1, src],
                device_id={axis: partner}, device_id_type=MESH).start()

    def publish_bias(phase, part):
        rounded = row_bias[chunk * part:chunk * part + chunk].astype(BF16)
        send_bias[phase, part] = rounded
        got_bias[phase, me, part] = rounded

    def send_blocks(send, got, send_sem, recv_sem, start, count):
        span = pl.ds(start, count)
        for peer in peers:
            pltpu.make_async_remote_copy(
                src_ref=send.at[peer, span], dst_ref=got.at[me, span],
                send_sem=send_sem.at[peer], recv_sem=recv_sem.at[me],
                device_id={axis: peer}, device_id_type=MESH).start()

    def send_h_view(sem, view):
        for peer in peers:
            pltpu.make_async_remote_copy(
                src_ref=view(send_h, peer), dst_ref=view(got_h, me),
                send_sem=h_send_sem.at[sem, peer], recv_sem=h_recv_sem.at[sem, me],
                device_id={axis: peer}, device_id_type=MESH).start()

    def wide_view(start, count):
        return lambda ref, who: ref.at[who, :, pl.ds(start, count)]

    def group_view(idx, start, count):
        return lambda ref, who: ref.at[who, idx, pl.ds(start, count)]

    WIDE, FIRST, LAST = range(3)
    whole_views = [wide_view(0, held), group_view(0, held, pairs - 1 - held), group_view(0, pairs - 1, 1)]
    whole_views += [group_view(idx, held, pairs - held) for idx in range(1, groups)]

    def wait_h(sem):
        for peer in peers:
            view = whole_views[sem](got_h, peer)
            pltpu.make_async_copy(view, view, h_recv_sem.at[sem, peer]).wait()

    def send_first(start, count):
        send_h_view(FIRST, group_view(0, start, count))

    def send_delta(start, count):
        send_blocks(send_d, got_d, d_send_sem, d_recv_sem.at[start // late], start, count)

    def store_block(send, got, pair, first, second, low, high):
        for dest in range(group):
            span = slice(rows * dest + low, rows * dest + high)
            send[dest, pair] = jnp.concatenate([first[span], second[span]], axis=0).astype(BF16)
        got[me, pair] = send[me, pair]

    def project(slot, normed_dup, wt, wp):
        cols = dot(wt[...], normed_dup, 1, 1)
        keys = dot(normed_dup[:seq_len], wp[:, channels:2 * channels])
        return slot, cols, keys

    def stage(projected):
        slot, cols, keys = projected
        q_sc[slot] = cols[:channels].astype(BF16)
        v_sc[slot] = cols[channels:2 * channels, :seq_len].astype(BF16)
        g_sc[slot] = jax.nn.sigmoid(cols[2 * channels:])
        k_sc[slot] = keys.astype(BF16)

    def transpose_weights(wp, wt):
        wt[0:channels] = wp[:, 0:channels].T * jnp.asarray(Q_SHRINK, BF16)
        wt[channels:2 * channels] = wp[:, 2 * channels:3 * channels].T
        wt[2 * channels:3 * channels] = wp[:, 3 * channels:].T

    class Attention:
        def __init__(self, slots):
            self.slots = slots
            self.score, self.prob, self.mixed, self.done = {}, {}, {}, {}

        def qk(self, unit):
            slot, tile = self.slots[unit // 3], unit % 3
            self.score[unit] = dot(k_sc[slot], score_block(q_sc[slot], tile))

        def biased(self, unit, half):
            at = DOUBLE * (unit % 3) + LANES * half
            return self.score[unit][:, LANES * half:LANES * half + LANES] + bias_t[:, at:at + LANES]

        def hand_on(self, unit):
            for half in range(2):
                part = self.biased(unit, half)
                part_sc[unit % 3, half] = part
                top_sc[unit % 3, half] = jnp.max(part, axis=0, keepdims=True)

        def soften(self, unit):
            probs, totals = [], []
            for half in range(2):
                if unit in self.score:
                    part = self.biased(unit, half)
                    top = jnp.max(part, axis=0, keepdims=True)
                else:
                    part, top = part_sc[unit, half], top_sc[unit, half]
                prob = jnp.exp2((part - top) * (SHRINK * LOG2_E))
                totals.append(jnp.sum(prob, axis=0, keepdims=True))
                probs.append(prob.astype(BF16))
            self.prob[unit] = jnp.concatenate(probs, axis=1), jnp.concatenate(totals, axis=1)

        def mix(self, unit):
            slot, tile = self.slots[unit // 3], unit % 3
            prob, total = self.prob.pop(unit)
            self.mixed[unit] = dot(v_sc[slot, HEAD * tile:HEAD * tile + HALF], prob), total

        def norm(self, unit):
            mixed, total = self.mixed.pop(unit)
            self.done[unit] = mixed / total

        def gate(self, sub):
            outs = [self.done.pop(3 * sub + tile) for tile in range(3)]
            gated_sc[sub] = gather_heads(outs, g_sc[self.slots[sub]])

    def out_dot(sub, wo):
        return dot(gated_sc[sub].T, wo[...])

    loads[0].wait()
    for part in range(chunks):
        load_z(part).wait()
        base = chunk * part
        normed = [layer_norm(z_ref[base + sub]) for sub in range(chunk)]
        full = [dot(wb_s[...], duplicate_tail(val), 1, 1) for val in normed]
        for sub in range(chunk):
            normed_sc[base + sub] = normed[sub]
        for sub in range(chunk):
            row_bias[base + sub:base + sub + 1, :] = bias_row(full[sub])
        publish_bias(0, part)
        if part == chunks - 2:
            loads[1].wait()
            transpose_weights(wp_s, wt_s)
            pl.semaphore_wait(barrier, group - 1)
            send_bias_part(0, 0, chunks - 1, peers, 0)

    for load in loads[3:]:
        load.wait()
    send_bias_part(0, chunks - 1, 1, peers, 0)

    @pl.loop(0, pairs)
    def _(step):
        made = [project(2 * step + sub, duplicate_tail(normed_sc[2 * step + sub]), wt_s, wp_s) for sub in range(2)]
        for val in made:
            stage(val)

    def bias_of(phase, src):
        return jnp.concatenate([got_bias[phase, src, part].astype(F32) for part in range(chunks)], axis=0)

    loads[2].wait()
    transpose_weights(wp_e, wt_e)
    for src in peers:
        drain(got_bias.at[0, src], bias_recv_sem.at[0, src])
    low = low_half((HALF, LANES))
    by_query = jnp.concatenate([bias_of(0, src) for src in range(group)], axis=0) * (1 / SHRINK)
    by_query = jnp.concatenate([by_query, by_query[LANES:]], axis=0)
    for first in (0, 1):
        base = 384 * first
        head_a = by_query[:, base:base + LANES].T
        mixed = by_query[:, base + LANES:base + DOUBLE].T
        head_b = by_query[:, base + DOUBLE:base + 384].T
        bias_t[0:LANES, base:base + LANES] = head_a[:, :LANES]
        bias_t[LANES:192, base:base + LANES] = mixed[:HALF, :LANES]
        low_a = low_half((LANES, LANES))
        bias_t[0:LANES, base + LANES:base + DOUBLE] = jnp.where(low_a, head_a[:, LANES:], head_b[:, LANES:])
        bias_t[LANES:192, base + LANES:base + DOUBLE] = jnp.where(low, mixed[:HALF, LANES:], mixed[HALF:, LANES:])
        bias_t[0:LANES, base + DOUBLE:base + 384] = head_b[:, :LANES]
        bias_t[LANES:192, base + DOUBLE:base + 384] = mixed[HALF:, :LANES]

    def start_resid(pair, sub, res):
        row = 2 * pair + sub
        value = z_ref[row] + merge_tail(res)
        y_ref[row] = value
        return value

    def store_h(pair, first, second):
        for idx in range(groups):
            for dest in range(group):
                low = rows * dest + early * idx
                span = slice(low, low + early)
                send_h[dest, idx, pair] = jnp.concatenate([first[span], second[span]], axis=0).astype(BF16)
            got_h[me, idx, pair] = send_h[me, idx, pair]

    def end_normed(pair, sub):
        return duplicate_tail(layer_norm(y_ref[2 * pair + sub].astype(BF16).astype(F32)))

    def prime(slot):
        att = Attention([slot])
        for unit in range(2):
            att.qk(unit)
        for unit in range(2):
            att.hand_on(unit)

    prime(0)

    @pl.loop(0, pairs)
    def _(pair):
        even = lax.rem(pair, 2) == 0
        for part in range(chunks - 1):
            @pl.when(pair == chunk // 2 * (part + 1) + 2)
            def _():
                publish_bias(1, part)

        @pl.when(pair == 2)
        def _():
            send_h_view(WIDE, wide_view(0, 1))

        @pl.when(jnp.logical_and(jnp.logical_and(pair > 2, pair < held + 2), even))
        def _():
            send_h_view(WIDE, wide_view(pair - 3, 2))

        @pl.when(jnp.logical_and(pair > held + 2, even))
        def _():
            send_first(pair - 3, 2)

        @pl.when(pair == pairs - 1)
        def _():
            send_first(pairs - 3, 1)

        for part in range(chunks - 1):
            @pl.when(pair == chunk // 2 * (part + 1) + 2)
            def _():
                send_bias_part(1, part, 1, alike + [partner], 1)

        last = jnp.maximum(pair - 1, 0)
        older = jnp.maximum(pair - 2, 0)
        att = Attention([2 * pair, 2 * pair + 1, 2 * jnp.minimum(pair + 1, pairs - 1)])
        att.qk(2)
        att.qk(3)
        normed = [end_normed(older, sub) for sub in range(2)]
        att.soften(0)
        att.mix(0)
        res = [out_dot(sub, wo_s) for sub in range(2)]
        att.soften(1)
        att.mix(1)
        full = [dot(wb_e[...], val, 1, 1) for val in normed]
        att.qk(4)
        made = [start_resid(last, 0, res[0])]
        att.soften(2)
        att.norm(0)
        att.mix(2)
        att.qk(5)
        made.append(start_resid(last, 1, res[1]))
        att.soften(3)
        att.norm(1)
        att.mix(3)
        att.qk(6)
        for sub in range(2):
            row_bias[pl.ds(2 * older + sub, 1), :] = bias_row(full[sub])
        att.soften(4)
        att.norm(2)
        att.gate(0)
        att.mix(4)
        att.qk(7)
        att.soften(5)
        att.norm(3)
        att.mix(5)
        store_h(last, made[0], made[1])
        att.hand_on(6)
        att.norm(4)
        att.hand_on(7)
        att.norm(5)
        att.gate(1)

    send_first(pairs - 2, 1)
    res = [out_dot(sub, wo_s) for sub in range(2)]
    made = [start_resid(pairs - 1, sub, res[sub]) for sub in range(2)]
    store_h(pairs - 1, made[0], made[1])
    ends = [(pair, sub) for pair in (pairs - 2, pairs - 1) for sub in range(2)]
    full = [dot(wb_e[...], end_normed(pair, sub), 1, 1) for pair, sub in ends]
    send_h_view(LAST, group_view(0, pairs - 1, 1))
    for (pair, sub), val in zip(ends, full):
        row_bias[2 * pair + sub:2 * pair + sub + 1, :] = bias_row(val)
    publish_bias(1, chunks - 1)
    for peer in peers:
        drain(send_bias.at[0], bias_send_sem.at[0, peer])
    send_bias_part(1, chunks - 1, 1, peers, 2)
    for idx in range(1, groups):
        send_h_view(LAST + idx, group_view(idx, held, pairs - held))

    def spread(idx, first, count):
        @pl.loop(0, group)
        def _(src):
            for pair in range(first, first + count):
                block = got_h[src, idx, pair].astype(F32)
                for sub in range(2):
                    start = pl.multiple_of(((src * pairs + pair) * 2 + sub) * rows + early * idx, 8)
                    flat[pl.ds(start, early), :] = block[early * sub:early * sub + early]

    def column(col):
        return flat[pl.ds(col, seq_len, stride=rows), :]

    wait_h(WIDE)
    wait_h(FIRST)
    spread(0, 0, pairs - 1)
    wait_h(LAST)
    spread(0, pairs - 1, 1)
    forward_bias()

    for sub in range(2):
        stage(project(sub, duplicate_tail(layer_norm(column(sub))), wt_e, wp_e))

    for src in [partner] + others:
        drain(got_bias.at[1, src, most], bias_recv_sem.at[1, src])
    for src in peers:
        drain(got_bias.at[1, src, final], bias_recv_sem.at[2, src])
    for src in range(group):
        bias_t[rows * src:rows * src + rows] = bias_of(1, src) * (1 / SHRINK)

    prime(0)

    def end_mid(pair, sub, res):
        upd = merge_tail(res)
        return upd, layer_norm(column(2 * pair + sub) + upd)

    def widen(mid):
        return jnp.maximum(dot(mid[1], w1_ref[...]).astype(BF16), jnp.asarray(0, BF16))

    def end_tail(pair):
        res = [out_dot(sub, wo_e) for sub in range(2)]
        mids = [end_mid(pair, sub, res[sub]) for sub in range(2)]
        hidden = [widen(mid) for mid in mids]
        delta = [mids[sub][0] + dot(hidden[sub], w2_ref[...]) for sub in range(2)]
        store_block(send_d, got_d, pair, delta[0], delta[1], 0, rows)

    @pl.loop(0, pairs)
    def _(pair):
        for idx in range(1, groups):
            @pl.when(pair == early // 2 * idx - 1)
            def _():
                wait_h(LAST + idx)
                spread(idx, 0, pairs)

        @pl.when(pair == 2)
        def _():
            send_delta(0, 1)

        @pl.when(jnp.logical_and(pair > 2, lax.rem(pair, 2) == 0))
        def _():
            send_delta(pair - 3, 2)

        @pl.when(pair == pairs - 1)
        def _():
            send_delta(pairs - 3, 1)

        last = jnp.maximum(pair - 1, 0)
        ahead = jnp.minimum(pair + 1, pairs - 1)
        here = 2 * lax.rem(pair, 2)
        there = 2 - here
        att = Attention([here, here + 1, there])
        att.qk(2)
        att.qk(3)
        normed = [duplicate_tail(layer_norm(column(2 * ahead + sub))) for sub in range(2)]
        att.soften(0)
        att.mix(0)
        res = [out_dot(sub, wo_e) for sub in range(2)]
        att.soften(1)
        att.mix(1)
        made = project(there, normed[0], wt_e, wp_e)
        att.qk(4)
        mids = [end_mid(last, 0, res[0])]
        att.soften(2)
        att.norm(0)
        att.mix(2)
        stage(made)
        att.qk(5)
        mids.append(end_mid(last, 1, res[1]))
        hidden = [widen(mids[0])]
        att.soften(3)
        att.norm(1)
        att.mix(3)
        hidden.append(widen(mids[1]))
        att.qk(6)
        delta = [mids[0][0] + dot(hidden[0], w2_ref[...])]
        att.soften(4)
        att.norm(2)
        att.gate(0)
        att.mix(4)
        made = project(there + 1, normed[1], wt_e, wp_e)
        att.qk(7)
        delta.append(mids[1][0] + dot(hidden[1], w2_ref[...]))
        att.soften(5)
        att.norm(3)
        att.mix(5)
        stage(made)
        store_block(send_d, got_d, last, delta[0], delta[1], 0, rows)
        att.hand_on(6)
        att.norm(4)
        att.hand_on(7)
        att.norm(5)
        att.gate(1)

    send_delta(pairs - 2, 1)
    end_tail(pairs - 1)
    send_delta(pairs - 1, 1)

    def finish(part, first, count):
        span = pl.ds(first, count)
        for peer in peers:
            pltpu.make_async_copy(got_d.at[peer, span], got_d.at[peer, span], d_recv_sem.at[part, peer]).wait()

        @pl.loop(0, group)
        def _(src):
            for pair in range(first, first + count):
                start = pl.multiple_of((src * pairs + pair) * 2 * rows, 2 * rows)
                flat[pl.ds(start, 2 * rows), :] = got_d[src, pair].astype(F32)

        @pl.loop(0, rows)
        def _(row):
            for src in range(group):
                low_col = rows * src + 2 * first
                y_ref[row, low_col:low_col + 2 * count] += flat[pl.ds(low_col * rows + row, 2 * count, stride=rows), :]

    finish(0, 0, late)
    finish(1, late, pairs - late)

    for peer in alike + [partner]:
        drain(send_bias.at[1, most], bias_send_sem.at[1, peer])
    for src in alike:
        drain(got_bias.at[1, src, most], pass_send_sem.at[src])
    for peer in peers:
        drain(send_bias.at[1, final], bias_send_sem.at[2, peer])
        for sem, view in enumerate(whole_views):
            drain(view(send_h, peer), h_send_sem.at[sem, peer])
        drain(send_d.at[peer], d_send_sem.at[peer])


def solution(mesh):
    row_spec = P(('dp', 'sp'), None, None)
    group = mesh.shape['sp']

    def local_fn(pair_loc, *weights):
        rows, seq_len, channels = pair_loc.shape
        heads = weights[1].shape[0]
        pairs = rows // 2
        wide = heads * seq_len
        early = 8
        chunk = 8
        hbm = pl.BlockSpec(memory_space=pltpu.HBM)

        groups = rows // early
        columns = pltpu.VMEM((group, groups, pairs, 2 * early, channels), BF16)
        deltas = pltpu.VMEM((group, pairs, 2 * rows, channels), BF16)

        def sems(*shape):
            return pltpu.SemaphoreType.DMA(shape)

        return pl.pallas_call(
            functools.partial(kernel, 'sp', group, early),
            out_shape=jax.ShapeDtypeStruct(pair_loc.shape, F32),
            in_specs=[hbm] * 9,
            out_specs=pl.BlockSpec(memory_space=pltpu.VMEM),
            scratch_shapes=[pltpu.VMEM(pair_loc.shape, F32)] + [pltpu.VMEM(val.shape, BF16) for val in weights] + [
                pltpu.VMEM((3 * channels, channels), BF16),
                pltpu.VMEM((3 * channels, channels), BF16),
                pltpu.VMEM((rows, wide), F32),
                pltpu.VMEM((2, rows // chunk, chunk, wide), BF16),
                pltpu.VMEM((2, group, rows // chunk, chunk, wide), BF16),
                pltpu.VMEM((seq_len, wide), F32),
                pltpu.VMEM((rows, seq_len, channels), BF16),
                pltpu.VMEM((rows, channels, DOUBLE), BF16),
                pltpu.VMEM((rows, seq_len, channels), BF16),
                pltpu.VMEM((rows, channels, seq_len), BF16),
                pltpu.VMEM((rows, channels, DOUBLE), F32),
                pltpu.VMEM((2, channels, DOUBLE), BF16),
                pltpu.VMEM((2, 2, seq_len, LANES), F32),
                pltpu.VMEM((2, 2, 1, LANES), F32),
                columns, columns, deltas, deltas,
                pltpu.VMEM((rows * seq_len, channels), F32),
                sems(rows // chunk), sems(len(weights)), sems(3, group), sems(3, group), sems(group),
                sems(groups + 2, group), sems(groups + 2, group), sems(group), sems(2, group),
            ],
            compiler_params=pltpu.CompilerParams(collective_id=0, has_side_effects=True, vmem_limit_bytes=34 * 1024 * 1024),
        )(*[pltpu.with_memory_space_constraint(val, pltpu.HBM) for val in (pair_loc, *weights)])

    return jax.shard_map(local_fn, mesh=mesh, in_specs=(row_spec, P(), P(), P(), P(), P(), P(), P(), P()), out_specs=row_spec, check_vma=False)
```

```python
import functools

import jax
import jax.numpy as jnp
from jax import lax
from jax.experimental import pallas as pl
from jax.experimental.pallas import tpu as pltpu
from jax.sharding import PartitionSpec as P

LN_EPS = 1e-5
LANES = 128
DOUBLE = 256
HALF = 64
HEAD = 32
Q_SHRINK = 0.125
SHRINK = 32 ** -0.5 / Q_SHRINK
LOG2_E = 1.4426950408889634
MESH = pl.DeviceIdType.MESH
F32 = jnp.float32
BF16 = jnp.bfloat16


def layer_norm(vals):
    mean_c = jnp.mean(vals, axis=-1, keepdims=True)
    centered = vals - mean_c
    variance = jnp.mean(centered * centered, axis=-1, keepdims=True)
    return (centered * lax.rsqrt(variance + LN_EPS)).astype(BF16)


def dot(lhs, rhs, lhs_dim=1, rhs_dim=0):
    return lax.dot_general(lhs, rhs, (((lhs_dim,), (rhs_dim,)), ((), ())), preferred_element_type=F32)


def duplicate_tail(normed):
    return jnp.concatenate([normed, normed[LANES:]], axis=0)


def low_half(shape):
    return lax.broadcasted_iota(jnp.int32, shape, len(shape) - 1) < HALF


def bias_row(full):
    low = low_half((1, LANES))
    tiles = []
    for first in (0, 2):
        head_a, head_b = full[first:first + 1], full[first + 1:first + 2]
        tiles += [head_a[:, :LANES], jnp.where(low, head_a[:, LANES:], head_b[:, LANES:]), head_b[:, :LANES]]
    return jnp.concatenate(tiles, axis=1)


def keep_low(val):
    return jnp.where(low_half(val.shape), val, jnp.zeros_like(val))


def keep_high(val):
    return jnp.where(low_half(val.shape), jnp.zeros_like(val), val)


def stack(rows):
    return jnp.concatenate([jnp.concatenate(row, axis=1) for row in rows], axis=0)


def score_block(q_t, tile):
    zero = jnp.zeros((HEAD, LANES), BF16)
    none = [zero, zero]

    def head(idx):
        return q_t[HEAD * idx:HEAD * idx + HEAD, :LANES], q_t[HEAD * idx:HEAD * idx + HEAD, LANES:]

    first, second = head(tile), head(tile + 1)
    if tile == 0:
        return stack([[first[0], keep_low(first[1])], [zero, keep_high(second[1])], none, none])
    if tile == 1:
        return stack([none, [first[0], zero], [zero, second[0]], none])
    return stack([none, none, [keep_low(first[1]), zero], [keep_high(second[1]), second[0]]])


def gather_heads(outs, g_t):
    main = jnp.concatenate([outs[0][:HEAD, :LANES], outs[1][:HEAD, :LANES], outs[1][HEAD:, LANES:], outs[2][HEAD:, LANES:]], axis=0)
    tail = jnp.concatenate([keep_low(outs[0][:HEAD, LANES:]), keep_high(outs[0][HEAD:, LANES:]),
                            keep_low(outs[2][:HEAD, :LANES]), keep_high(outs[2][HEAD:, :LANES])], axis=0)
    return (jnp.concatenate([main, tail], axis=1) * g_t).astype(BF16)


def merge_tail(res):
    return jnp.concatenate([res[:LANES], res[LANES:192] + res[192:]], axis=0)


def kernel(axis, group, early, z_hbm, wp_s_hbm, wb_s_hbm, wo_s_hbm, wp_e_hbm, wb_e_hbm, wo_e_hbm, w1_hbm, w2_hbm, y_ref,
           z_ref, wp_s, wb_s, wo_s, wp_e, wb_e, wo_e, w1_ref, w2_ref,
           wt_s, wt_e, row_bias, send_bias, got_bias, bias_t, normed_sc, q_sc, k_sc, v_sc, g_sc, gated_sc, part_sc, top_sc,
           send_h, got_h, send_d, got_d, flat,
           z_sem, w_sem, bias_send_sem, bias_recv_sem, pass_send_sem, h_send_sem, h_recv_sem, d_send_sem, d_recv_sem):
    rows, seq_len, channels = z_hbm.shape
    pairs = rows // 2
    chunk = 8
    chunks = rows // chunk
    late = pairs - 3
    groups = rows // early
    held = pairs - 9
    me = lax.axis_index(axis)
    half = group // 2
    order = sorted(range(1, group), key=lambda step: abs(step - half))
    peers = [lax.rem(me + step, group) for step in order]
    partner = me + 1 - 2 * lax.rem(me, 2)
    alike = [lax.rem(me + step, group) for step in order if step % 2 == 0]
    others = [lax.rem(partner + step, group) for step in order if step % 2 == 0]

    def load_z(idx):
        span = pl.ds(idx * chunk, chunk)
        return pltpu.make_async_copy(z_hbm.at[span], z_ref.at[span], z_sem.at[idx])

    loads = [pltpu.make_async_copy(src, dst, w_sem.at[idx]) for idx, (src, dst) in enumerate(
        ((wb_s_hbm, wb_s), (wp_s_hbm, wp_s), (wp_e_hbm, wp_e), (wo_s_hbm, wo_s), (wb_e_hbm, wb_e),
         (wo_e_hbm, wo_e), (w1_hbm, w1_ref), (w2_hbm, w2_ref)))]
    loads[0].start()
    for idx in range(chunks):
        load_z(idx).start()
    for load in loads[1:]:
        load.start()

    barrier = pltpu.get_barrier_semaphore()
    for peer in peers:
        pl.semaphore_signal(barrier, inc=1, device_id={axis: peer}, device_id_type=MESH)

    def send_bias_part(phase, part, count, to, sem):
        span = pl.ds(part, count)
        for peer in to:
            pltpu.make_async_remote_copy(
                src_ref=send_bias.at[phase, span], dst_ref=got_bias.at[phase, me, span],
                send_sem=bias_send_sem.at[sem, peer], recv_sem=bias_recv_sem.at[sem, me],
                device_id={axis: peer}, device_id_type=MESH).start()

    def drain(ref, sem):
        pltpu.make_async_copy(ref, ref, sem).wait()

    most, final = pl.ds(0, chunks - 1), pl.ds(chunks - 1, 1)

    def forward_bias():
        for src in alike:
            view = got_bias.at[1, src, most]
            drain(view, bias_recv_sem.at[1, src])
            pltpu.make_async_remote_copy(
                src_ref=view, dst_ref=view,
                send_sem=pass_send_sem.at[src], recv_sem=bias_recv_sem.at[1, src],
                device_id={axis: partner}, device_id_type=MESH).start()

    def publish_bias(phase, part):
        rounded = row_bias[chunk * part:chunk * part + chunk].astype(BF16)
        send_bias[phase, part] = rounded
        got_bias[phase, me, part] = rounded

    def send_blocks(send, got, send_sem, recv_sem, start, count):
        span = pl.ds(start, count)
        for peer in peers:
            pltpu.make_async_remote_copy(
                src_ref=send.at[peer, span], dst_ref=got.at[me, span],
                send_sem=send_sem.at[peer], recv_sem=recv_sem.at[me],
                device_id={axis: peer}, device_id_type=MESH).start()

    def send_h_view(sem, view):
        for peer in peers:
            pltpu.make_async_remote_copy(
                src_ref=view(send_h, peer), dst_ref=view(got_h, me),
                send_sem=h_send_sem.at[sem, peer], recv_sem=h_recv_sem.at[sem, me],
                device_id={axis: peer}, device_id_type=MESH).start()

    def wide_view(start, count):
        return lambda ref, who: ref.at[who, :, pl.ds(start, count)]

    def group_view(idx, start, count):
        return lambda ref, who: ref.at[who, idx, pl.ds(start, count)]

    WIDE, FIRST, LAST = range(3)
    whole_views = [wide_view(0, held), group_view(0, held, pairs - 1 - held), group_view(0, pairs - 1, 1)]
    whole_views += [group_view(idx, held, pairs - held) for idx in range(1, groups)]

    def wait_h(sem):
        for peer in peers:
            view = whole_views[sem](got_h, peer)
            pltpu.make_async_copy(view, view, h_recv_sem.at[sem, peer]).wait()

    def send_first(start, count):
        send_h_view(FIRST, group_view(0, start, count))

    def send_delta(start, count):
        send_blocks(send_d, got_d, d_send_sem, d_recv_sem.at[start // late], start, count)

    def store_block(send, got, pair, first, second, low, high):
        for dest in range(group):
            span = slice(rows * dest + low, rows * dest + high)
            send[dest, pair] = jnp.concatenate([first[span], second[span]], axis=0).astype(BF16)
        got[me, pair] = send[me, pair]

    def project(slot, normed_dup, wt, wp):
        cols = dot(wt[...], normed_dup, 1, 1)
        keys = dot(normed_dup[:seq_len], wp[:, channels:2 * channels])
        return slot, cols, keys

    def stage(projected):
        slot, cols, keys = projected
        q_sc[slot] = cols[:channels].astype(BF16)
        v_sc[slot] = cols[channels:2 * channels, :seq_len].astype(BF16)
        g_sc[slot] = jax.nn.sigmoid(cols[2 * channels:])
        k_sc[slot] = keys.astype(BF16)

    def transpose_weights(wp, wt):
        wt[0:channels] = wp[:, 0:channels].T * jnp.asarray(Q_SHRINK, BF16)
        wt[channels:2 * channels] = wp[:, 2 * channels:3 * channels].T
        wt[2 * channels:3 * channels] = wp[:, 3 * channels:].T

    class Attention:
        def __init__(self, slots):
            self.slots = slots
            self.score, self.prob, self.mixed, self.done = {}, {}, {}, {}

        def qk(self, unit):
            slot, tile = self.slots[unit // 3], unit % 3
            self.score[unit] = dot(k_sc[slot], score_block(q_sc[slot], tile))

        def biased(self, unit, half):
            at = DOUBLE * (unit % 3) + LANES * half
            return self.score[unit][:, LANES * half:LANES * half + LANES] + bias_t[:, at:at + LANES]

        def hand_on(self, unit):
            for half in range(2):
                part = self.biased(unit, half)
                part_sc[unit % 3, half] = part
                top_sc[unit % 3, half] = jnp.max(part, axis=0, keepdims=True)

        def soften(self, unit):
            probs, totals = [], []
            for half in range(2):
                if unit in self.score:
                    part = self.biased(unit, half)
                    top = jnp.max(part, axis=0, keepdims=True)
                else:
                    part, top = part_sc[unit, half], top_sc[unit, half]
                prob = jnp.exp2((part - top) * (SHRINK * LOG2_E))
                totals.append(jnp.sum(prob, axis=0, keepdims=True))
                probs.append(prob.astype(BF16))
            self.prob[unit] = jnp.concatenate(probs, axis=1), jnp.concatenate(totals, axis=1)

        def mix(self, unit):
            slot, tile = self.slots[unit // 3], unit % 3
            prob, total = self.prob.pop(unit)
            self.mixed[unit] = dot(v_sc[slot, HEAD * tile:HEAD * tile + HALF], prob), total

        def norm(self, unit):
            mixed, total = self.mixed.pop(unit)
            self.done[unit] = mixed / total

        def gate(self, sub):
            outs = [self.done.pop(3 * sub + tile) for tile in range(3)]
            gated_sc[sub] = gather_heads(outs, g_sc[self.slots[sub]])

    def out_dot(sub, wo):
        return dot(gated_sc[sub].T, wo[...])

    loads[0].wait()
    for part in range(chunks):
        load_z(part).wait()
        base = chunk * part
        normed = [layer_norm(z_ref[base + sub]) for sub in range(chunk)]
        full = [dot(wb_s[...], duplicate_tail(val), 1, 1) for val in normed]
        for sub in range(chunk):
            normed_sc[base + sub] = normed[sub]
        for sub in range(chunk):
            row_bias[base + sub:base + sub + 1, :] = bias_row(full[sub])
        publish_bias(0, part)
        if part == chunks - 2:
            pl.semaphore_wait(barrier, group - 1)
            send_bias_part(0, 0, chunks - 1, peers, 0)

    for load in loads[1:]:
        load.wait()
    send_bias_part(0, chunks - 1, 1, peers, 0)
    transpose_weights(wp_s, wt_s)

    @pl.loop(0, pairs)
    def _(step):
        made = [project(2 * step + sub, duplicate_tail(normed_sc[2 * step + sub]), wt_s, wp_s) for sub in range(2)]
        for val in made:
            stage(val)

    def bias_of(phase, src):
        return jnp.concatenate([got_bias[phase, src, part].astype(F32) for part in range(chunks)], axis=0)

    transpose_weights(wp_e, wt_e)
    for src in peers:
        drain(got_bias.at[0, src], bias_recv_sem.at[0, src])
    low = low_half((HALF, LANES))
    by_query = jnp.concatenate([bias_of(0, src) for src in range(group)], axis=0) * (1 / SHRINK)
    by_query = jnp.concatenate([by_query, by_query[LANES:]], axis=0)
    for first in (0, 1):
        base = 384 * first
        head_a = by_query[:, base:base + LANES].T
        mixed = by_query[:, base + LANES:base + DOUBLE].T
        head_b = by_query[:, base + DOUBLE:base + 384].T
        bias_t[0:LANES, base:base + LANES] = head_a[:, :LANES]
        bias_t[LANES:192, base:base + LANES] = mixed[:HALF, :LANES]
        low_a = low_half((LANES, LANES))
        bias_t[0:LANES, base + LANES:base + DOUBLE] = jnp.where(low_a, head_a[:, LANES:], head_b[:, LANES:])
        bias_t[LANES:192, base + LANES:base + DOUBLE] = jnp.where(low, mixed[:HALF, LANES:], mixed[HALF:, LANES:])
        bias_t[0:LANES, base + DOUBLE:base + 384] = head_b[:, :LANES]
        bias_t[LANES:192, base + DOUBLE:base + 384] = mixed[HALF:, :LANES]

    def start_resid(pair, sub, res):
        row = 2 * pair + sub
        value = z_ref[row] + merge_tail(res)
        y_ref[row] = value
        return value

    def store_h(pair, first, second):
        for idx in range(groups):
            for dest in range(group):
                low = rows * dest + early * idx
                span = slice(low, low + early)
                send_h[dest, idx, pair] = jnp.concatenate([first[span], second[span]], axis=0).astype(BF16)
            got_h[me, idx, pair] = send_h[me, idx, pair]

    def end_normed(pair, sub):
        return duplicate_tail(layer_norm(y_ref[2 * pair + sub].astype(BF16).astype(F32)))

    def prime(slot):
        att = Attention([slot])
        for unit in range(2):
            att.qk(unit)
        for unit in range(2):
            att.hand_on(unit)

    prime(0)

    @pl.loop(0, pairs)
    def _(pair):
        even = lax.rem(pair, 2) == 0
        for part in range(chunks - 1):
            @pl.when(pair == chunk // 2 * (part + 1) + 2)
            def _():
                publish_bias(1, part)

        @pl.when(pair == 2)
        def _():
            send_h_view(WIDE, wide_view(0, 1))

        @pl.when(jnp.logical_and(jnp.logical_and(pair > 2, pair < held + 2), even))
        def _():
            send_h_view(WIDE, wide_view(pair - 3, 2))

        @pl.when(jnp.logical_and(pair > held + 2, even))
        def _():
            send_first(pair - 3, 2)

        @pl.when(pair == pairs - 1)
        def _():
            send_first(pairs - 3, 1)

        for part in range(chunks - 1):
            @pl.when(pair == chunk // 2 * (part + 1) + 2)
            def _():
                send_bias_part(1, part, 1, alike + [partner], 1)

        last = jnp.maximum(pair - 1, 0)
        older = jnp.maximum(pair - 2, 0)
        att = Attention([2 * pair, 2 * pair + 1, 2 * jnp.minimum(pair + 1, pairs - 1)])
        normed0 = end_normed(older, 0)
        att.qk(3)
        normed1 = end_normed(older, 1)
        att.soften(0)
        res1 = out_dot(1, wo_s)
        att.qk(2)
        att.mix(0)
        att.soften(1)
        att.soften(2)
        res0 = out_dot(0, wo_s)
        att.mix(1)
        made0 = start_resid(last, 0, res0)
        full1 = dot(wb_e[...], normed1, 1, 1)
        att.qk(4)
        full0 = dot(wb_e[...], normed0, 1, 1)
        att.norm(1)
        att.soften(3)
        att.mix(2)
        att.norm(0)
        att.qk(5)
        made1 = start_resid(last, 1, res1)
        att.soften(5)
        att.soften(4)
        att.qk(6)
        att.norm(2)
        att.gate(0)
        att.qk(7)
        att.mix(3)
        att.mix(4)
        att.mix(5)
        store_h(last, made0, made1)
        row_bias[pl.ds(2 * older, 1), :] = bias_row(full0)
        att.norm(4)
        att.norm(5)
        att.hand_on(6)
        row_bias[pl.ds(2 * older + 1, 1), :] = bias_row(full1)
        att.norm(3)
        att.hand_on(7)
        att.gate(1)

    send_first(pairs - 2, 1)
    res = [out_dot(sub, wo_s) for sub in range(2)]
    made = [start_resid(pairs - 1, sub, res[sub]) for sub in range(2)]
    store_h(pairs - 1, made[0], made[1])
    ends = [(pair, sub) for pair in (pairs - 2, pairs - 1) for sub in range(2)]
    send_h_view(LAST, group_view(0, pairs - 1, 1))
    full = [dot(wb_e[...], end_normed(pair, sub), 1, 1) for pair, sub in ends]
    for (pair, sub), val in zip(ends, full):
        row_bias[2 * pair + sub:2 * pair + sub + 1, :] = bias_row(val)
    publish_bias(1, chunks - 1)
    for peer in peers:
        drain(send_bias.at[0], bias_send_sem.at[0, peer])
    send_bias_part(1, chunks - 1, 1, peers, 2)
    for idx in range(1, groups):
        send_h_view(LAST + idx, group_view(idx, held, pairs - held))

    def spread(idx, first, count):
        @pl.loop(0, group)
        def _(src):
            for pair in range(first, first + count):
                block = got_h[src, idx, pair].astype(F32)
                for sub in range(2):
                    start = pl.multiple_of(((src * pairs + pair) * 2 + sub) * rows + early * idx, 8)
                    flat[pl.ds(start, early), :] = block[early * sub:early * sub + early]

    def column(col):
        return flat[pl.ds(col, seq_len, stride=rows), :]

    wait_h(WIDE)
    wait_h(FIRST)
    spread(0, 0, pairs - 1)
    wait_h(LAST)
    spread(0, pairs - 1, 1)
    forward_bias()

    for sub in range(2):
        stage(project(sub, duplicate_tail(layer_norm(column(sub))), wt_e, wp_e))

    for src in [partner] + others:
        drain(got_bias.at[1, src, most], bias_recv_sem.at[1, src])
    for src in peers:
        drain(got_bias.at[1, src, final], bias_recv_sem.at[2, src])
    for src in range(group):
        bias_t[rows * src:rows * src + rows] = bias_of(1, src) * (1 / SHRINK)

    prime(0)

    def end_mid(pair, sub, res):
        upd = merge_tail(res)
        return upd, layer_norm(column(2 * pair + sub) + upd)

    def widen(mid):
        return jnp.maximum(dot(mid[1], w1_ref[...]).astype(BF16), jnp.asarray(0, BF16))

    def end_tail(pair):
        res = [out_dot(sub, wo_e) for sub in range(2)]
        mids = [end_mid(pair, sub, res[sub]) for sub in range(2)]
        hidden = [widen(mid) for mid in mids]
        delta = [mids[sub][0] + dot(hidden[sub], w2_ref[...]) for sub in range(2)]
        store_block(send_d, got_d, pair, delta[0], delta[1], 0, rows)

    @pl.loop(0, pairs)
    def _(pair):
        for idx in range(1, groups):
            @pl.when(pair == early // 2 * idx - 1)
            def _():
                wait_h(LAST + idx)
                spread(idx, 0, pairs)

        @pl.when(pair == 2)
        def _():
            send_delta(0, 1)

        @pl.when(jnp.logical_and(pair > 2, lax.rem(pair, 2) == 0))
        def _():
            send_delta(pair - 3, 2)

        @pl.when(pair == pairs - 1)
        def _():
            send_delta(pairs - 3, 1)

        last = jnp.maximum(pair - 1, 0)
        ahead = jnp.minimum(pair + 1, pairs - 1)
        here = 2 * lax.rem(pair, 2)
        there = 2 - here
        att = Attention([here, here + 1, there])
        normed1 = duplicate_tail(layer_norm(column(2 * ahead + 1)))
        att.qk(2)
        att.qk(3)
        att.soften(0)
        res0 = out_dot(0, wo_e)
        res1 = out_dot(1, wo_e)
        att.soften(1)
        normed0 = duplicate_tail(layer_norm(column(2 * ahead)))
        att.mix(1)
        next0 = project(there, normed0, wt_e, wp_e)
        mid0 = end_mid(last, 0, res0)
        att.norm(1)
        att.soften(2)
        att.mix(0)
        att.qk(4)
        att.mix(2)
        stage(next0)
        att.norm(0)
        att.soften(3)
        att.qk(5)
        att.norm(2)
        hidden0 = widen(mid0)
        mid1 = end_mid(last, 1, res1)
        att.soften(4)
        att.qk(6)
        att.mix(3)
        delta0 = mid0[0] + dot(hidden0, w2_ref[...])
        hidden1 = widen(mid1)
        att.gate(0)
        att.qk(7)
        next1 = project(there + 1, normed1, wt_e, wp_e)
        delta1 = mid1[0] + dot(hidden1, w2_ref[...])
        att.hand_on(6)
        att.hand_on(7)
        att.norm(3)
        store_block(send_d, got_d, last, delta0, delta1, 0, rows)
        att.soften(5)
        att.mix(4)
        att.mix(5)
        att.norm(5)
        stage(next1)
        att.norm(4)
        att.gate(1)

    send_delta(pairs - 2, 1)
    end_tail(pairs - 1)
    send_delta(pairs - 1, 1)

    def finish(part, first, count):
        span = pl.ds(first, count)
        for peer in peers:
            pltpu.make_async_copy(got_d.at[peer, span], got_d.at[peer, span], d_recv_sem.at[part, peer]).wait()

        @pl.loop(0, group)
        def _(src):
            for pair in range(first, first + count):
                start = pl.multiple_of((src * pairs + pair) * 2 * rows, 2 * rows)
                flat[pl.ds(start, 2 * rows), :] = got_d[src, pair].astype(F32)

        @pl.loop(0, rows)
        def _(row):
            for src in range(group):
                low_col = rows * src + 2 * first
                y_ref[row, low_col:low_col + 2 * count] += flat[pl.ds(low_col * rows + row, 2 * count, stride=rows), :]

    finish(0, 0, late)
    finish(1, late, pairs - late)

    for peer in alike + [partner]:
        drain(send_bias.at[1, most], bias_send_sem.at[1, peer])
    for src in alike:
        drain(got_bias.at[1, src, most], pass_send_sem.at[src])
    for peer in peers:
        drain(send_bias.at[1, final], bias_send_sem.at[2, peer])
        for sem, view in enumerate(whole_views):
            drain(view(send_h, peer), h_send_sem.at[sem, peer])
        drain(send_d.at[peer], d_send_sem.at[peer])


def solution(mesh):
    row_spec = P(('dp', 'sp'), None, None)
    group = mesh.shape['sp']

    def local_fn(pair_loc, *weights):
        rows, seq_len, channels = pair_loc.shape
        heads = weights[1].shape[0]
        pairs = rows // 2
        wide = heads * seq_len
        early = 8
        chunk = 8
        hbm = pl.BlockSpec(memory_space=pltpu.HBM)

        groups = rows // early
        columns = pltpu.VMEM((group, groups, pairs, 2 * early, channels), BF16)
        deltas = pltpu.VMEM((group, pairs, 2 * rows, channels), BF16)

        def sems(*shape):
            return pltpu.SemaphoreType.DMA(shape)

        return pl.pallas_call(
            functools.partial(kernel, 'sp', group, early),
            out_shape=jax.ShapeDtypeStruct(pair_loc.shape, F32),
            in_specs=[hbm] * 9,
            out_specs=pl.BlockSpec(memory_space=pltpu.VMEM),
            scratch_shapes=[pltpu.VMEM(pair_loc.shape, F32)] + [pltpu.VMEM(val.shape, BF16) for val in weights] + [
                pltpu.VMEM((3 * channels, channels), BF16),
                pltpu.VMEM((3 * channels, channels), BF16),
                pltpu.VMEM((rows, wide), F32),
                pltpu.VMEM((2, rows // chunk, chunk, wide), BF16),
                pltpu.VMEM((2, group, rows // chunk, chunk, wide), BF16),
                pltpu.VMEM((seq_len, wide), F32),
                pltpu.VMEM((rows, seq_len, channels), BF16),
                pltpu.VMEM((rows, channels, DOUBLE), BF16),
                pltpu.VMEM((rows, seq_len, channels), BF16),
                pltpu.VMEM((rows, channels, seq_len), BF16),
                pltpu.VMEM((rows, channels, DOUBLE), F32),
                pltpu.VMEM((2, channels, DOUBLE), BF16),
                pltpu.VMEM((2, 2, seq_len, LANES), F32),
                pltpu.VMEM((2, 2, 1, LANES), F32),
                columns, columns, deltas, deltas,
                pltpu.VMEM((rows * seq_len, channels), F32),
                sems(rows // chunk), sems(len(weights)), sems(3, group), sems(3, group), sems(group),
                sems(groups + 2, group), sems(groups + 2, group), sems(group), sems(2, group),
            ],
            compiler_params=pltpu.CompilerParams(collective_id=0, has_side_effects=True, vmem_limit_bytes=34 * 1024 * 1024),
        )(*[pltpu.with_memory_space_constraint(val, pltpu.HBM) for val in (pair_loc, *weights)])

    return jax.shard_map(local_fn, mesh=mesh, in_specs=(row_spec, P(), P(), P(), P(), P(), P(), P(), P()), out_specs=row_spec, check_vma=False)
```

```python
import functools

import jax
import jax.numpy as jnp
from jax import lax
from jax.experimental import pallas as pl
from jax.experimental.pallas import tpu as pltpu
from jax.sharding import PartitionSpec as P

LN_EPS = 1e-5
LANES = 128
DOUBLE = 256
HALF = 64
HEAD = 32
Q_SHRINK = 0.125
SHRINK = 32 ** -0.5 / Q_SHRINK
LOG2_E = 1.4426950408889634
MESH = pl.DeviceIdType.MESH
F32 = jnp.float32
BF16 = jnp.bfloat16


def layer_norm(vals):
    mean_c = jnp.mean(vals, axis=-1, keepdims=True)
    centered = vals - mean_c
    variance = jnp.mean(centered * centered, axis=-1, keepdims=True)
    return (centered * lax.rsqrt(variance + LN_EPS)).astype(BF16)


def dot(lhs, rhs, lhs_dim=1, rhs_dim=0):
    return lax.dot_general(lhs, rhs, (((lhs_dim,), (rhs_dim,)), ((), ())), preferred_element_type=F32)


def duplicate_tail(normed):
    return jnp.concatenate([normed, normed[LANES:]], axis=0)


def low_half(shape):
    return lax.broadcasted_iota(jnp.int32, shape, len(shape) - 1) < HALF


def bias_row(full):
    low = low_half((1, LANES))
    tiles = []
    for first in (0, 2):
        head_a, head_b = full[first:first + 1], full[first + 1:first + 2]
        tiles += [head_a[:, :LANES], jnp.where(low, head_a[:, LANES:], head_b[:, LANES:]), head_b[:, :LANES]]
    return jnp.concatenate(tiles, axis=1)


def keep_low(val):
    return jnp.where(low_half(val.shape), val, jnp.zeros_like(val))


def keep_high(val):
    return jnp.where(low_half(val.shape), jnp.zeros_like(val), val)


def stack(rows):
    return jnp.concatenate([jnp.concatenate(row, axis=1) for row in rows], axis=0)


def score_block(q_t, tile):
    zero = jnp.zeros((HEAD, LANES), BF16)
    none = [zero, zero]

    def head(idx):
        return q_t[HEAD * idx:HEAD * idx + HEAD, :LANES], q_t[HEAD * idx:HEAD * idx + HEAD, LANES:]

    first, second = head(tile), head(tile + 1)
    if tile == 0:
        return stack([[first[0], keep_low(first[1])], [zero, keep_high(second[1])], none, none])
    if tile == 1:
        return stack([none, [first[0], zero], [zero, second[0]], none])
    return stack([none, none, [keep_low(first[1]), zero], [keep_high(second[1]), second[0]]])


def gather_heads(outs, g_t):
    main = jnp.concatenate([outs[0][:HEAD, :LANES], outs[1][:HEAD, :LANES], outs[1][HEAD:, LANES:], outs[2][HEAD:, LANES:]], axis=0)
    tail = jnp.concatenate([keep_low(outs[0][:HEAD, LANES:]), keep_high(outs[0][HEAD:, LANES:]),
                            keep_low(outs[2][:HEAD, :LANES]), keep_high(outs[2][HEAD:, :LANES])], axis=0)
    return (jnp.concatenate([main, tail], axis=1) * g_t).astype(BF16)


def merge_tail(res):
    return jnp.concatenate([res[:LANES], res[LANES:192] + res[192:]], axis=0)


def kernel(axis, group, early, z_hbm, wp_s_hbm, wb_s_hbm, wo_s_hbm, wp_e_hbm, wb_e_hbm, wo_e_hbm, w1_hbm, w2_hbm, y_ref,
           z_ref, wp_s, wb_s, wo_s, wp_e, wb_e, wo_e, w1_ref, w2_ref,
           wt_s, wt_e, row_bias, send_bias, got_bias, bias_t, normed_sc, q_sc, k_sc, v_sc, g_sc, gated_sc, part_sc, top_sc,
           send_h, got_h, send_d, got_d, flat,
           z_sem, w_sem, bias_send_sem, bias_recv_sem, pass_send_sem, h_send_sem, h_recv_sem, d_send_sem, d_recv_sem):
    rows, seq_len, channels = z_hbm.shape
    pairs = rows // 2
    chunk = 8
    chunks = rows // chunk
    late = pairs - 3
    groups = rows // early
    held = pairs - 9
    me = lax.axis_index(axis)
    half = group // 2
    order = sorted(range(1, group), key=lambda step: abs(step - half))
    peers = [lax.rem(me + step, group) for step in order]
    partner = me + 1 - 2 * lax.rem(me, 2)
    alike = [lax.rem(me + step, group) for step in order if step % 2 == 0]
    others = [lax.rem(partner + step, group) for step in order if step % 2 == 0]

    def load_z(idx):
        span = pl.ds(idx * chunk, chunk)
        return pltpu.make_async_copy(z_hbm.at[span], z_ref.at[span], z_sem.at[idx])

    loads = [pltpu.make_async_copy(src, dst, w_sem.at[idx]) for idx, (src, dst) in enumerate(
        ((wb_s_hbm, wb_s), (wp_s_hbm, wp_s), (wp_e_hbm, wp_e), (wo_s_hbm, wo_s), (wb_e_hbm, wb_e),
         (wo_e_hbm, wo_e), (w1_hbm, w1_ref), (w2_hbm, w2_ref)))]
    loads[0].start()
    for idx in range(chunks):
        load_z(idx).start()
    for load in loads[1:]:
        load.start()

    barrier = pltpu.get_barrier_semaphore()
    for peer in peers:
        pl.semaphore_signal(barrier, inc=1, device_id={axis: peer}, device_id_type=MESH)

    def send_bias_part(phase, part, count, to, sem):
        span = pl.ds(part, count)
        for peer in to:
            pltpu.make_async_remote_copy(
                src_ref=send_bias.at[phase, span], dst_ref=got_bias.at[phase, me, span],
                send_sem=bias_send_sem.at[sem, peer], recv_sem=bias_recv_sem.at[sem, me],
                device_id={axis: peer}, device_id_type=MESH).start()

    def drain(ref, sem):
        pltpu.make_async_copy(ref, ref, sem).wait()

    most, final = pl.ds(0, chunks - 1), pl.ds(chunks - 1, 1)

    def forward_bias():
        for src in alike:
            view = got_bias.at[1, src, most]
            drain(view, bias_recv_sem.at[1, src])
            pltpu.make_async_remote_copy(
                src_ref=view, dst_ref=view,
                send_sem=pass_send_sem.at[src], recv_sem=bias_recv_sem.at[1, src],
                device_id={axis: partner}, device_id_type=MESH).start()

    def publish_bias(phase, part):
        rounded = row_bias[chunk * part:chunk * part + chunk].astype(BF16)
        send_bias[phase, part] = rounded
        got_bias[phase, me, part] = rounded

    def send_blocks(send, got, send_sem, recv_sem, start, count):
        span = pl.ds(start, count)
        for peer in peers:
            pltpu.make_async_remote_copy(
                src_ref=send.at[peer, span], dst_ref=got.at[me, span],
                send_sem=send_sem.at[peer], recv_sem=recv_sem.at[me],
                device_id={axis: peer}, device_id_type=MESH).start()

    def send_h_view(sem, view):
        for peer in peers:
            pltpu.make_async_remote_copy(
                src_ref=view(send_h, peer), dst_ref=view(got_h, me),
                send_sem=h_send_sem.at[sem, peer], recv_sem=h_recv_sem.at[sem, me],
                device_id={axis: peer}, device_id_type=MESH).start()

    def wide_view(start, count):
        return lambda ref, who: ref.at[who, :, pl.ds(start, count)]

    def group_view(idx, start, count):
        return lambda ref, who: ref.at[who, idx, pl.ds(start, count)]

    WIDE, FIRST, LAST = range(3)
    whole_views = [wide_view(0, held), group_view(0, held, pairs - 1 - held), group_view(0, pairs - 1, 1)]
    whole_views += [group_view(idx, held, pairs - held) for idx in range(1, groups)]

    def wait_h(sem):
        for peer in peers:
            view = whole_views[sem](got_h, peer)
            pltpu.make_async_copy(view, view, h_recv_sem.at[sem, peer]).wait()

    def send_first(start, count):
        send_h_view(FIRST, group_view(0, start, count))

    def send_delta(start, count):
        send_blocks(send_d, got_d, d_send_sem, d_recv_sem.at[start // late], start, count)

    def store_block(send, got, pair, first, second, low, high):
        for dest in range(group):
            span = slice(rows * dest + low, rows * dest + high)
            send[dest, pair] = jnp.concatenate([first[span], second[span]], axis=0).astype(BF16)
        got[me, pair] = send[me, pair]

    def project(slot, normed_dup, wt, wp):
        cols = dot(wt[...], normed_dup, 1, 1)
        keys = dot(normed_dup[:seq_len], wp[:, channels:2 * channels])
        return slot, cols, keys

    def stage(projected):
        slot, cols, keys = projected
        q_sc[slot] = cols[:channels].astype(BF16)
        v_sc[slot] = cols[channels:2 * channels, :seq_len].astype(BF16)
        g_sc[slot] = jax.nn.sigmoid(cols[2 * channels:])
        k_sc[slot] = keys.astype(BF16)

    def transpose_weights(wp, wt):
        wt[0:channels] = wp[:, 0:channels].T * jnp.asarray(Q_SHRINK, BF16)
        wt[channels:2 * channels] = wp[:, 2 * channels:3 * channels].T
        wt[2 * channels:3 * channels] = wp[:, 3 * channels:].T

    class Attention:
        def __init__(self, slots):
            self.slots = slots
            self.score, self.prob, self.mixed, self.done = {}, {}, {}, {}

        def qk(self, unit):
            slot, tile = self.slots[unit // 3], unit % 3
            self.score[unit] = dot(k_sc[slot], score_block(q_sc[slot], tile))

        def biased(self, unit, half):
            at = DOUBLE * (unit % 3) + LANES * half
            return self.score[unit][:, LANES * half:LANES * half + LANES] + bias_t[:, at:at + LANES]

        def hand_on(self, unit):
            for half in range(2):
                part = self.biased(unit, half)
                part_sc[unit % 3, half] = part
                top_sc[unit % 3, half] = jnp.max(part, axis=0, keepdims=True)

        def soften(self, unit):
            probs, totals = [], []
            for half in range(2):
                if unit in self.score:
                    part = self.biased(unit, half)
                    top = jnp.max(part, axis=0, keepdims=True)
                else:
                    part, top = part_sc[unit, half], top_sc[unit, half]
                prob = jnp.exp2((part - top) * (SHRINK * LOG2_E))
                totals.append(jnp.sum(prob, axis=0, keepdims=True))
                probs.append(prob.astype(BF16))
            self.prob[unit] = jnp.concatenate(probs, axis=1), jnp.concatenate(totals, axis=1)

        def mix(self, unit):
            slot, tile = self.slots[unit // 3], unit % 3
            prob, total = self.prob.pop(unit)
            self.mixed[unit] = dot(v_sc[slot, HEAD * tile:HEAD * tile + HALF], prob), total

        def norm(self, unit):
            mixed, total = self.mixed.pop(unit)
            self.done[unit] = mixed / total

        def gate(self, sub):
            outs = [self.done.pop(3 * sub + tile) for tile in range(3)]
            gated_sc[sub] = gather_heads(outs, g_sc[self.slots[sub]])

    def out_dot(sub, wo):
        return dot(gated_sc[sub].T, wo[...])

    loads[0].wait()
    for part in range(chunks):
        load_z(part).wait()
        base = chunk * part
        normed = [layer_norm(z_ref[base + sub]) for sub in range(chunk)]
        full = [dot(wb_s[...], duplicate_tail(val), 1, 1) for val in normed]
        for sub in range(chunk):
            normed_sc[base + sub] = normed[sub]
        for sub in range(chunk):
            row_bias[base + sub:base + sub + 1, :] = bias_row(full[sub])
        publish_bias(0, part)
        if part == chunks - 2:
            pl.semaphore_wait(barrier, group - 1)
            send_bias_part(0, 0, chunks - 1, peers, 0)

    for load in loads[1:]:
        load.wait()
    send_bias_part(0, chunks - 1, 1, peers, 0)
    transpose_weights(wp_s, wt_s)

    @pl.loop(0, pairs)
    def _(step):
        made = [project(2 * step + sub, duplicate_tail(normed_sc[2 * step + sub]), wt_s, wp_s) for sub in range(2)]
        for val in made:
            stage(val)

    def bias_of(phase, src):
        return jnp.concatenate([got_bias[phase, src, part].astype(F32) for part in range(chunks)], axis=0)

    def open_scores():
        att = Attention([0])
        for unit in range(2):
            att.qk(unit)
        return att

    transpose_weights(wp_e, wt_e)
    opening = open_scores()
    for src in peers:
        drain(got_bias.at[0, src], bias_recv_sem.at[0, src])
    low = low_half((HALF, LANES))
    by_query = jnp.concatenate([bias_of(0, src) for src in range(group)], axis=0) * (1 / SHRINK)
    by_query = jnp.concatenate([by_query, by_query[LANES:]], axis=0)
    for first in (0, 1):
        base = 384 * first
        head_a = by_query[:, base:base + LANES].T
        mixed = by_query[:, base + LANES:base + DOUBLE].T
        head_b = by_query[:, base + DOUBLE:base + 384].T
        bias_t[0:LANES, base:base + LANES] = head_a[:, :LANES]
        bias_t[LANES:192, base:base + LANES] = mixed[:HALF, :LANES]
        low_a = low_half((LANES, LANES))
        bias_t[0:LANES, base + LANES:base + DOUBLE] = jnp.where(low_a, head_a[:, LANES:], head_b[:, LANES:])
        bias_t[LANES:192, base + LANES:base + DOUBLE] = jnp.where(low, mixed[:HALF, LANES:], mixed[HALF:, LANES:])
        bias_t[0:LANES, base + DOUBLE:base + 384] = head_b[:, :LANES]
        bias_t[LANES:192, base + DOUBLE:base + 384] = mixed[HALF:, :LANES]

    def start_resid(pair, sub, res):
        row = 2 * pair + sub
        value = z_ref[row] + merge_tail(res)
        y_ref[row] = value
        return value

    def store_h(pair, first, second):
        for idx in range(groups):
            for dest in range(group):
                low = rows * dest + early * idx
                span = slice(low, low + early)
                send_h[dest, idx, pair] = jnp.concatenate([first[span], second[span]], axis=0).astype(BF16)
            got_h[me, idx, pair] = send_h[me, idx, pair]

    def end_normed(pair, sub):
        return duplicate_tail(layer_norm(y_ref[2 * pair + sub].astype(BF16).astype(F32)))

    for unit in range(2):
        opening.hand_on(unit)

    @pl.loop(0, pairs)
    def _(pair):
        even = lax.rem(pair, 2) == 0
        @pl.when(pair == pairs - 2)
        def _():
            for part in range(chunks - 1):
                publish_bias(1, part)

        @pl.when(pair == held + 1)
        def _():
            send_h_view(WIDE, wide_view(0, held))

        @pl.when(pair == pairs - 4)
        def _():
            send_first(held, pairs - 5 - held)

        @pl.when(pair == pairs - 2)
        def _():
            send_first(pairs - 5, 2)

        @pl.when(pair == pairs - 1)
        def _():
            send_first(pairs - 3, 1)

        @pl.when(pair == pairs - 2)
        def _():
            send_bias_part(1, 0, chunks - 1, alike + [partner], 1)

        last = jnp.maximum(pair - 1, 0)
        older = jnp.maximum(pair - 2, 0)
        att = Attention([2 * pair, 2 * pair + 1, 2 * jnp.minimum(pair + 1, pairs - 1)])
        normed0 = end_normed(older, 0)
        att.qk(3)
        normed1 = end_normed(older, 1)
        att.soften(0)
        res1 = out_dot(1, wo_s)
        att.qk(2)
        att.mix(0)
        att.soften(1)
        att.soften(2)
        res0 = out_dot(0, wo_s)
        att.mix(1)
        made0 = start_resid(last, 0, res0)
        full1 = dot(wb_e[...], normed1, 1, 1)
        att.qk(4)
        full0 = dot(wb_e[...], normed0, 1, 1)
        att.norm(1)
        att.soften(3)
        att.mix(2)
        att.norm(0)
        att.qk(5)
        made1 = start_resid(last, 1, res1)
        att.soften(5)
        att.soften(4)
        att.qk(6)
        att.norm(2)
        att.gate(0)
        att.qk(7)
        att.mix(3)
        att.mix(4)
        att.mix(5)
        store_h(last, made0, made1)
        row_bias[pl.ds(2 * older, 1), :] = bias_row(full0)
        att.norm(4)
        att.norm(5)
        att.hand_on(6)
        row_bias[pl.ds(2 * older + 1, 1), :] = bias_row(full1)
        att.norm(3)
        att.hand_on(7)
        att.gate(1)

    send_first(pairs - 2, 1)
    res = [out_dot(sub, wo_s) for sub in range(2)]
    made = [start_resid(pairs - 1, sub, res[sub]) for sub in range(2)]
    store_h(pairs - 1, made[0], made[1])
    ends = [(pair, sub) for pair in (pairs - 2, pairs - 1) for sub in range(2)]
    send_h_view(LAST, group_view(0, pairs - 1, 1))
    full = [dot(wb_e[...], end_normed(pair, sub), 1, 1) for pair, sub in ends]
    for (pair, sub), val in zip(ends, full):
        row_bias[2 * pair + sub:2 * pair + sub + 1, :] = bias_row(val)
    publish_bias(1, chunks - 1)
    for peer in peers:
        drain(send_bias.at[0], bias_send_sem.at[0, peer])
    send_bias_part(1, chunks - 1, 1, peers, 2)
    for idx in range(1, groups):
        send_h_view(LAST + idx, group_view(idx, held, pairs - held))

    def spread(idx, first, count):
        @pl.loop(0, group)
        def _(src):
            for pair in range(first, first + count):
                block = got_h[src, idx, pair].astype(F32)
                for sub in range(2):
                    start = pl.multiple_of(((src * pairs + pair) * 2 + sub) * rows + early * idx, 8)
                    flat[pl.ds(start, early), :] = block[early * sub:early * sub + early]

    def column(col):
        return flat[pl.ds(col, seq_len, stride=rows), :]

    wait_h(WIDE)
    wait_h(FIRST)
    spread(0, 0, pairs - 1)
    wait_h(LAST)
    spread(0, pairs - 1, 1)
    forward_bias()

    for sub in range(2):
        stage(project(sub, duplicate_tail(layer_norm(column(sub))), wt_e, wp_e))

    opening = open_scores()
    for src in [partner] + others:
        drain(got_bias.at[1, src, most], bias_recv_sem.at[1, src])
    for src in peers:
        drain(got_bias.at[1, src, final], bias_recv_sem.at[2, src])
    for src in range(group):
        bias_t[rows * src:rows * src + rows] = bias_of(1, src) * (1 / SHRINK)

    for unit in range(2):
        opening.hand_on(unit)

    def end_mid(pair, sub, res):
        upd = merge_tail(res)
        return upd, layer_norm(column(2 * pair + sub) + upd)

    def widen(mid):
        return jnp.maximum(dot(mid[1], w1_ref[...]).astype(BF16), jnp.asarray(0, BF16))

    def end_tail(pair):
        res = [out_dot(sub, wo_e) for sub in range(2)]
        mids = [end_mid(pair, sub, res[sub]) for sub in range(2)]
        hidden = [widen(mid) for mid in mids]
        delta = [mids[sub][0] + dot(hidden[sub], w2_ref[...]) for sub in range(2)]
        store_block(send_d, got_d, pair, delta[0], delta[1], 0, rows)

    @pl.loop(0, pairs)
    def _(pair):
        for idx in range(1, groups):
            @pl.when(pair == early // 2 * idx - 1)
            def _():
                wait_h(LAST + idx)
                spread(idx, 0, pairs)

        @pl.when(pair == 2)
        def _():
            send_delta(0, 1)

        @pl.when(jnp.logical_and(pair > 2, lax.rem(pair, 2) == 0))
        def _():
            send_delta(pair - 3, 2)

        @pl.when(pair == pairs - 1)
        def _():
            send_delta(pairs - 3, 1)

        last = jnp.maximum(pair - 1, 0)
        ahead = jnp.minimum(pair + 1, pairs - 1)
        here = 2 * lax.rem(pair, 2)
        there = 2 - here
        att = Attention([here, here + 1, there])
        normed1 = duplicate_tail(layer_norm(column(2 * ahead + 1)))
        att.qk(2)
        att.qk(3)
        att.soften(0)
        res0 = out_dot(0, wo_e)
        res1 = out_dot(1, wo_e)
        att.soften(1)
        normed0 = duplicate_tail(layer_norm(column(2 * ahead)))
        att.mix(1)
        next0 = project(there, normed0, wt_e, wp_e)
        mid0 = end_mid(last, 0, res0)
        att.norm(1)
        att.soften(2)
        att.mix(0)
        att.qk(4)
        att.mix(2)
        stage(next0)
        att.norm(0)
        att.soften(3)
        att.qk(5)
        att.norm(2)
        hidden0 = widen(mid0)
        mid1 = end_mid(last, 1, res1)
        att.soften(4)
        att.qk(6)
        att.mix(3)
        delta0 = mid0[0] + dot(hidden0, w2_ref[...])
        hidden1 = widen(mid1)
        att.gate(0)
        att.qk(7)
        next1 = project(there + 1, normed1, wt_e, wp_e)
        delta1 = mid1[0] + dot(hidden1, w2_ref[...])
        att.hand_on(6)
        att.hand_on(7)
        att.norm(3)
        store_block(send_d, got_d, last, delta0, delta1, 0, rows)
        att.soften(5)
        att.mix(4)
        att.mix(5)
        att.norm(5)
        stage(next1)
        att.norm(4)
        att.gate(1)

    send_delta(pairs - 2, 1)
    end_tail(pairs - 1)
    send_delta(pairs - 1, 1)

    def finish(part, first, count):
        span = pl.ds(first, count)
        for peer in peers:
            pltpu.make_async_copy(got_d.at[peer, span], got_d.at[peer, span], d_recv_sem.at[part, peer]).wait()

        @pl.loop(0, group)
        def _(src):
            for pair in range(first, first + count):
                start = pl.multiple_of((src * pairs + pair) * 2 * rows, 2 * rows)
                flat[pl.ds(start, 2 * rows), :] = got_d[src, pair].astype(F32)

        @pl.loop(0, rows)
        def _(row):
            for src in range(group):
                low_col = rows * src + 2 * first
                y_ref[row, low_col:low_col + 2 * count] += flat[pl.ds(low_col * rows + row, 2 * count, stride=rows), :]

    finish(0, 0, late)
    finish(1, late, pairs - late)

    for peer in alike + [partner]:
        drain(send_bias.at[1, most], bias_send_sem.at[1, peer])
    for src in alike:
        drain(got_bias.at[1, src, most], pass_send_sem.at[src])
    for peer in peers:
        drain(send_bias.at[1, final], bias_send_sem.at[2, peer])
        for sem, view in enumerate(whole_views):
            drain(view(send_h, peer), h_send_sem.at[sem, peer])
        drain(send_d.at[peer], d_send_sem.at[peer])


def solution(mesh):
    row_spec = P(('dp', 'sp'), None, None)
    group = mesh.shape['sp']

    def local_fn(pair_loc, *weights):
        rows, seq_len, channels = pair_loc.shape
        heads = weights[1].shape[0]
        pairs = rows // 2
        wide = heads * seq_len
        early = 8
        chunk = 8
        hbm = pl.BlockSpec(memory_space=pltpu.HBM)

        groups = rows // early
        columns = pltpu.VMEM((group, groups, pairs, 2 * early, channels), BF16)
        deltas = pltpu.VMEM((group, pairs, 2 * rows, channels), BF16)

        def sems(*shape):
            return pltpu.SemaphoreType.DMA(shape)

        return pl.pallas_call(
            functools.partial(kernel, 'sp', group, early),
            out_shape=jax.ShapeDtypeStruct(pair_loc.shape, F32),
            in_specs=[hbm] * 9,
            out_specs=pl.BlockSpec(memory_space=pltpu.VMEM),
            scratch_shapes=[pltpu.VMEM(pair_loc.shape, F32)] + [pltpu.VMEM(val.shape, BF16) for val in weights] + [
                pltpu.VMEM((3 * channels, channels), BF16),
                pltpu.VMEM((3 * channels, channels), BF16),
                pltpu.VMEM((rows, wide), F32),
                pltpu.VMEM((2, rows // chunk, chunk, wide), BF16),
                pltpu.VMEM((2, group, rows // chunk, chunk, wide), BF16),
                pltpu.VMEM((seq_len, wide), F32),
                pltpu.VMEM((rows, seq_len, channels), BF16),
                pltpu.VMEM((rows, channels, DOUBLE), BF16),
                pltpu.VMEM((rows, seq_len, channels), BF16),
                pltpu.VMEM((rows, channels, seq_len), BF16),
                pltpu.VMEM((rows, channels, DOUBLE), F32),
                pltpu.VMEM((2, channels, DOUBLE), BF16),
                pltpu.VMEM((2, 2, seq_len, LANES), F32),
                pltpu.VMEM((2, 2, 1, LANES), F32),
                columns, columns, deltas, deltas,
                pltpu.VMEM((rows * seq_len, channels), F32),
                sems(rows // chunk), sems(len(weights)), sems(3, group), sems(3, group), sems(group),
                sems(groups + 2, group), sems(groups + 2, group), sems(group), sems(2, group),
            ],
            compiler_params=pltpu.CompilerParams(collective_id=0, has_side_effects=True, vmem_limit_bytes=34 * 1024 * 1024),
        )(*[pltpu.with_memory_space_constraint(val, pltpu.HBM) for val in (pair_loc, *weights)])

    return jax.shard_map(local_fn, mesh=mesh, in_specs=(row_spec, P(), P(), P(), P(), P(), P(), P(), P()), out_specs=row_spec, check_vma=False)
```

```python
import functools

import jax
import jax.numpy as jnp
from jax import lax
from jax.experimental import pallas as pl
from jax.experimental.pallas import tpu as pltpu
from jax.sharding import PartitionSpec as P

LN_EPS = 1e-5
LANES = 128
DOUBLE = 256
HALF = 64
HEAD = 32
Q_SHRINK = 0.125
SHRINK = 32 ** -0.5 / Q_SHRINK
LOG2_E = 1.4426950408889634
MESH = pl.DeviceIdType.MESH
F32 = jnp.float32
BF16 = jnp.bfloat16


def layer_norm(vals):
    mean_c = jnp.mean(vals, axis=-1, keepdims=True)
    centered = vals - mean_c
    variance = jnp.mean(centered * centered, axis=-1, keepdims=True)
    return (centered * lax.rsqrt(variance + LN_EPS)).astype(BF16)


def dot(lhs, rhs, lhs_dim=1, rhs_dim=0):
    return lax.dot_general(lhs, rhs, (((lhs_dim,), (rhs_dim,)), ((), ())), preferred_element_type=F32)


def duplicate_tail(normed):
    return jnp.concatenate([normed, normed[LANES:]], axis=0)


def low_half(shape):
    return lax.broadcasted_iota(jnp.int32, shape, len(shape) - 1) < HALF


def bias_row(full):
    low = low_half((1, LANES))
    tiles = []
    for first in (0, 2):
        head_a, head_b = full[first:first + 1], full[first + 1:first + 2]
        tiles += [head_a[:, :LANES], jnp.where(low, head_a[:, LANES:], head_b[:, LANES:]), head_b[:, :LANES]]
    return jnp.concatenate(tiles, axis=1)


def keep_low(val):
    return jnp.where(low_half(val.shape), val, jnp.zeros_like(val))


def keep_high(val):
    return jnp.where(low_half(val.shape), jnp.zeros_like(val), val)


def stack(rows):
    return jnp.concatenate([jnp.concatenate(row, axis=1) for row in rows], axis=0)


def score_block(q_t, tile):
    zero = jnp.zeros((HEAD, LANES), BF16)
    none = [zero, zero]

    def head(idx):
        return q_t[HEAD * idx:HEAD * idx + HEAD, :LANES], q_t[HEAD * idx:HEAD * idx + HEAD, LANES:]

    first, second = head(tile), head(tile + 1)
    if tile == 0:
        return stack([[first[0], keep_low(first[1])], [zero, keep_high(second[1])], none, none])
    if tile == 1:
        return stack([none, [first[0], zero], [zero, second[0]], none])
    return stack([none, none, [keep_low(first[1]), zero], [keep_high(second[1]), second[0]]])


def gather_heads(outs, g_t):
    main = jnp.concatenate([outs[0][:HEAD, :LANES], outs[1][:HEAD, :LANES], outs[1][HEAD:, LANES:], outs[2][HEAD:, LANES:]], axis=0)
    tail = jnp.concatenate([keep_low(outs[0][:HEAD, LANES:]), keep_high(outs[0][HEAD:, LANES:]),
                            keep_low(outs[2][:HEAD, :LANES]), keep_high(outs[2][HEAD:, :LANES])], axis=0)
    return (jnp.concatenate([main, tail], axis=1) * g_t).astype(BF16)


def merge_tail(res):
    return jnp.concatenate([res[:LANES], res[LANES:192] + res[192:]], axis=0)


def kernel(axis, group, early, z_hbm, wp_s_hbm, wb_s_hbm, wo_s_hbm, wp_e_hbm, wb_e_hbm, wo_e_hbm, w1_hbm, w2_hbm, y_ref,
           z_ref, wp_s, wb_s, wo_s, wp_e, wb_e, wo_e, w1_ref, w2_ref,
           wt_s, wt_e, row_bias, send_bias, got_bias, bias_t, normed_sc, q_sc, k_sc, v_sc, g_sc, gated_sc, part_sc, top_sc,
           send_h, got_h, send_d, got_d, flat,
           z_sem, w_sem, bias_send_sem, bias_recv_sem, pass_send_sem, h_send_sem, h_recv_sem, d_send_sem, d_recv_sem):
    rows, seq_len, channels = z_hbm.shape
    pairs = rows // 2
    chunk = 8
    chunks = rows // chunk
    late = pairs - 2
    groups = rows // early
    held = pairs - 9
    me = lax.axis_index(axis)
    half = group // 2
    order = sorted(range(1, group), key=lambda step: abs(step - half))
    peers = [lax.rem(me + step, group) for step in order]
    partner = me + 1 - 2 * lax.rem(me, 2)
    alike = [lax.rem(me + step, group) for step in order if step % 2 == 0]
    others = [lax.rem(partner + step, group) for step in order if step % 2 == 0]

    def load_z(idx):
        span = pl.ds(idx * chunk, chunk)
        return pltpu.make_async_copy(z_hbm.at[span], z_ref.at[span], z_sem.at[idx])

    loads = [pltpu.make_async_copy(src, dst, w_sem.at[idx]) for idx, (src, dst) in enumerate(
        ((wb_s_hbm, wb_s), (wp_s_hbm, wp_s), (wp_e_hbm, wp_e), (wo_s_hbm, wo_s), (wb_e_hbm, wb_e),
         (wo_e_hbm, wo_e), (w1_hbm, w1_ref), (w2_hbm, w2_ref)))]
    loads[0].start()
    for idx in range(chunks):
        load_z(idx).start()
    for load in loads[1:]:
        load.start()

    barrier = pltpu.get_barrier_semaphore()
    for peer in peers:
        pl.semaphore_signal(barrier, inc=1, device_id={axis: peer}, device_id_type=MESH)

    def send_bias_part(phase, part, count, to, sem):
        span = pl.ds(part, count)
        for peer in to:
            pltpu.make_async_remote_copy(
                src_ref=send_bias.at[phase, span], dst_ref=got_bias.at[phase, me, span],
                send_sem=bias_send_sem.at[sem, peer], recv_sem=bias_recv_sem.at[sem, me],
                device_id={axis: peer}, device_id_type=MESH).start()

    def drain(ref, sem):
        pltpu.make_async_copy(ref, ref, sem).wait()

    most, final = pl.ds(0, chunks - 1), pl.ds(chunks - 1, 1)

    def forward_bias():
        for src in alike:
            view = got_bias.at[1, src, most]
            drain(view, bias_recv_sem.at[1, src])
            pltpu.make_async_remote_copy(
                src_ref=view, dst_ref=view,
                send_sem=pass_send_sem.at[src], recv_sem=bias_recv_sem.at[1, src],
                device_id={axis: partner}, device_id_type=MESH).start()

    def publish_bias(phase, part):
        rounded = row_bias[chunk * part:chunk * part + chunk].astype(BF16)
        send_bias[phase, part] = rounded
        got_bias[phase, me, part] = rounded

    def send_blocks(send, got, send_sem, recv_sem, start, count):
        span = pl.ds(start, count)
        for peer in peers:
            pltpu.make_async_remote_copy(
                src_ref=send.at[peer, span], dst_ref=got.at[me, span],
                send_sem=send_sem.at[peer], recv_sem=recv_sem.at[me],
                device_id={axis: peer}, device_id_type=MESH).start()

    def send_h_view(sem, view):
        for peer in peers:
            pltpu.make_async_remote_copy(
                src_ref=view(send_h, peer), dst_ref=view(got_h, me),
                send_sem=h_send_sem.at[sem, peer], recv_sem=h_recv_sem.at[sem, me],
                device_id={axis: peer}, device_id_type=MESH).start()

    def wide_view(start, count):
        return lambda ref, who: ref.at[who, :, pl.ds(start, count)]

    def group_view(idx, start, count):
        return lambda ref, who: ref.at[who, idx, pl.ds(start, count)]

    WIDE, FIRST, LAST = range(3)
    whole_views = [wide_view(0, held), group_view(0, held, pairs - 1 - held), group_view(0, pairs - 1, 1)]
    whole_views += [group_view(idx, held, pairs - held) for idx in range(1, groups)]

    def wait_h(sem):
        for peer in peers:
            view = whole_views[sem](got_h, peer)
            pltpu.make_async_copy(view, view, h_recv_sem.at[sem, peer]).wait()

    def send_first(start, count):
        send_h_view(FIRST, group_view(0, start, count))

    def send_delta(start, count):
        send_blocks(send_d, got_d, d_send_sem, d_recv_sem.at[start // late], start, count)

    def store_block(send, got, pair, first, second, low, high):
        for dest in range(group):
            span = slice(rows * dest + low, rows * dest + high)
            send[dest, pair] = jnp.concatenate([first[span], second[span]], axis=0).astype(BF16)
        got[me, pair] = send[me, pair]

    def project(slot, normed_dup, wt, wp):
        cols = dot(wt[...], normed_dup, 1, 1)
        keys = dot(normed_dup[:seq_len], wp[:, channels:2 * channels])
        return slot, cols, keys

    def stage(projected):
        slot, cols, keys = projected
        q_sc[slot] = cols[:channels].astype(BF16)
        v_sc[slot] = cols[channels:2 * channels, :seq_len].astype(BF16)
        g_sc[slot] = jax.nn.sigmoid(cols[2 * channels:])
        k_sc[slot] = keys.astype(BF16)

    def transpose_weights(wp, wt):
        wt[0:channels] = wp[:, 0:channels].T * jnp.asarray(Q_SHRINK, BF16)
        wt[channels:2 * channels] = wp[:, 2 * channels:3 * channels].T
        wt[2 * channels:3 * channels] = wp[:, 3 * channels:].T

    class Attention:
        def __init__(self, slots):
            self.slots = slots
            self.score, self.prob, self.mixed, self.done = {}, {}, {}, {}

        def qk(self, unit):
            slot, tile = self.slots[unit // 3], unit % 3
            self.score[unit] = dot(k_sc[slot], score_block(q_sc[slot], tile))

        def biased(self, unit, half):
            at = DOUBLE * (unit % 3) + LANES * half
            return self.score[unit][:, LANES * half:LANES * half + LANES] + bias_t[:, at:at + LANES]

        def hand_on(self, unit):
            for half in range(2):
                part = self.biased(unit, half)
                part_sc[unit % 3, half] = part
                top_sc[unit % 3, half] = jnp.max(part, axis=0, keepdims=True)

        def soften(self, unit):
            probs, totals = [], []
            for half in range(2):
                if unit in self.score:
                    part = self.biased(unit, half)
                    top = jnp.max(part, axis=0, keepdims=True)
                else:
                    part, top = part_sc[unit, half], top_sc[unit, half]
                prob = jnp.exp2((part - top) * (SHRINK * LOG2_E))
                totals.append(jnp.sum(prob, axis=0, keepdims=True))
                probs.append(prob.astype(BF16))
            self.prob[unit] = jnp.concatenate(probs, axis=1), jnp.concatenate(totals, axis=1)

        def mix(self, unit):
            slot, tile = self.slots[unit // 3], unit % 3
            prob, total = self.prob.pop(unit)
            self.mixed[unit] = dot(v_sc[slot, HEAD * tile:HEAD * tile + HALF], prob), total

        def norm(self, unit):
            mixed, total = self.mixed.pop(unit)
            self.done[unit] = mixed / total

        def gate(self, sub):
            outs = [self.done.pop(3 * sub + tile) for tile in range(3)]
            gated_sc[sub] = gather_heads(outs, g_sc[self.slots[sub]])

    def out_dot(sub, wo):
        return dot(gated_sc[sub].T, wo[...])

    loads[0].wait()
    for part in range(chunks):
        load_z(part).wait()
        base = chunk * part
        normed = [layer_norm(z_ref[base + sub]) for sub in range(chunk)]
        full = [dot(wb_s[...], duplicate_tail(val), 1, 1) for val in normed]
        for sub in range(chunk):
            normed_sc[base + sub] = normed[sub]
        for sub in range(chunk):
            row_bias[base + sub:base + sub + 1, :] = bias_row(full[sub])
        publish_bias(0, part)
        if part == chunks - 2:
            pl.semaphore_wait(barrier, group - 1)
            send_bias_part(0, 0, chunks - 1, peers, 0)

    for load in loads[1:]:
        load.wait()
    send_bias_part(0, chunks - 1, 1, peers, 0)
    transpose_weights(wp_s, wt_s)

    @pl.loop(0, pairs)
    def _(step):
        made = [project(2 * step + sub, duplicate_tail(normed_sc[2 * step + sub]), wt_s, wp_s) for sub in range(2)]
        for val in made:
            stage(val)

    def bias_of(phase, src):
        return jnp.concatenate([got_bias[phase, src, part].astype(F32) for part in range(chunks)], axis=0)

    def open_scores():
        att = Attention([0])
        for unit in range(2):
            att.qk(unit)
        return att

    transpose_weights(wp_e, wt_e)
    opening = open_scores()
    for src in peers:
        drain(got_bias.at[0, src], bias_recv_sem.at[0, src])
    low = low_half((HALF, LANES))
    by_query = jnp.concatenate([bias_of(0, src) for src in range(group)], axis=0) * (1 / SHRINK)
    by_query = jnp.concatenate([by_query, by_query[LANES:]], axis=0)
    for first in (0, 1):
        base = 384 * first
        head_a = by_query[:, base:base + LANES].T
        mixed = by_query[:, base + LANES:base + DOUBLE].T
        head_b = by_query[:, base + DOUBLE:base + 384].T
        bias_t[0:LANES, base:base + LANES] = head_a[:, :LANES]
        bias_t[LANES:192, base:base + LANES] = mixed[:HALF, :LANES]
        low_a = low_half((LANES, LANES))
        bias_t[0:LANES, base + LANES:base + DOUBLE] = jnp.where(low_a, head_a[:, LANES:], head_b[:, LANES:])
        bias_t[LANES:192, base + LANES:base + DOUBLE] = jnp.where(low, mixed[:HALF, LANES:], mixed[HALF:, LANES:])
        bias_t[0:LANES, base + DOUBLE:base + 384] = head_b[:, :LANES]
        bias_t[LANES:192, base + DOUBLE:base + 384] = mixed[HALF:, :LANES]

    def start_resid(pair, sub, res):
        row = 2 * pair + sub
        value = z_ref[row] + merge_tail(res)
        y_ref[row] = value
        return value

    def store_h(pair, first, second):
        for idx in range(groups):
            for dest in range(group):
                low = rows * dest + early * idx
                span = slice(low, low + early)
                send_h[dest, idx, pair] = jnp.concatenate([first[span], second[span]], axis=0).astype(BF16)
            got_h[me, idx, pair] = send_h[me, idx, pair]

    def end_normed(pair, sub):
        return duplicate_tail(layer_norm(y_ref[2 * pair + sub].astype(BF16).astype(F32)))

    for unit in range(2):
        opening.hand_on(unit)

    @pl.loop(0, pairs)
    def _(pair):
        even = lax.rem(pair, 2) == 0
        @pl.when(pair == pairs - 2)
        def _():
            for part in range(chunks - 1):
                publish_bias(1, part)

        @pl.when(pair == held + 1)
        def _():
            send_h_view(WIDE, wide_view(0, held))

        @pl.when(pair == pairs - 4)
        def _():
            send_first(held, pairs - 5 - held)

        @pl.when(pair == pairs - 2)
        def _():
            send_first(pairs - 5, 2)

        @pl.when(pair == pairs - 1)
        def _():
            send_first(pairs - 3, 1)

        @pl.when(pair == pairs - 2)
        def _():
            send_bias_part(1, 0, chunks - 1, alike + [partner], 1)

        last = jnp.maximum(pair - 1, 0)
        older = jnp.maximum(pair - 2, 0)
        att = Attention([2 * pair, 2 * pair + 1, 2 * jnp.minimum(pair + 1, pairs - 1)])
        normed0 = end_normed(older, 0)
        att.qk(3)
        normed1 = end_normed(older, 1)
        att.soften(0)
        res1 = out_dot(1, wo_s)
        att.qk(2)
        att.mix(0)
        att.soften(1)
        att.soften(2)
        res0 = out_dot(0, wo_s)
        att.mix(1)
        made0 = start_resid(last, 0, res0)
        full1 = dot(wb_e[...], normed1, 1, 1)
        att.qk(4)
        full0 = dot(wb_e[...], normed0, 1, 1)
        att.norm(1)
        att.soften(3)
        att.mix(2)
        att.norm(0)
        att.qk(5)
        made1 = start_resid(last, 1, res1)
        att.soften(5)
        att.soften(4)
        att.qk(6)
        att.norm(2)
        att.gate(0)
        att.qk(7)
        att.mix(3)
        att.mix(4)
        att.mix(5)
        store_h(last, made0, made1)
        row_bias[pl.ds(2 * older, 1), :] = bias_row(full0)
        att.norm(4)
        att.norm(5)
        att.hand_on(6)
        row_bias[pl.ds(2 * older + 1, 1), :] = bias_row(full1)
        att.norm(3)
        att.hand_on(7)
        att.gate(1)

    send_first(pairs - 2, 1)
    res = [out_dot(sub, wo_s) for sub in range(2)]
    made = [start_resid(pairs - 1, sub, res[sub]) for sub in range(2)]
    store_h(pairs - 1, made[0], made[1])
    ends = [(pair, sub) for pair in (pairs - 2, pairs - 1) for sub in range(2)]
    send_h_view(LAST, group_view(0, pairs - 1, 1))
    full = [dot(wb_e[...], end_normed(pair, sub), 1, 1) for pair, sub in ends]
    for (pair, sub), val in zip(ends, full):
        row_bias[2 * pair + sub:2 * pair + sub + 1, :] = bias_row(val)
    publish_bias(1, chunks - 1)
    for peer in peers:
        drain(send_bias.at[0], bias_send_sem.at[0, peer])
    send_bias_part(1, chunks - 1, 1, peers, 2)
    for idx in range(1, groups):
        send_h_view(LAST + idx, group_view(idx, held, pairs - held))

    def spread(idx, first, count):
        @pl.loop(0, group)
        def _(src):
            for pair in range(first, first + count):
                block = got_h[src, idx, pair].astype(F32)
                for sub in range(2):
                    start = pl.multiple_of(((src * pairs + pair) * 2 + sub) * rows + early * idx, 8)
                    flat[pl.ds(start, early), :] = block[early * sub:early * sub + early]

    def column(col):
        return flat[pl.ds(col, seq_len, stride=rows), :]

    wait_h(WIDE)
    wait_h(FIRST)
    spread(0, 0, pairs - 1)
    wait_h(LAST)
    spread(0, pairs - 1, 1)
    forward_bias()

    for sub in range(2):
        stage(project(sub, duplicate_tail(layer_norm(column(sub))), wt_e, wp_e))

    opening = open_scores()
    for src in [partner] + others:
        drain(got_bias.at[1, src, most], bias_recv_sem.at[1, src])
    for src in peers:
        drain(got_bias.at[1, src, final], bias_recv_sem.at[2, src])
    for src in range(group):
        bias_t[rows * src:rows * src + rows] = bias_of(1, src) * (1 / SHRINK)

    for unit in range(2):
        opening.hand_on(unit)

    def end_mid(pair, sub, res):
        upd = merge_tail(res)
        return upd, layer_norm(column(2 * pair + sub) + upd)

    def widen(mid):
        return jnp.maximum(dot(mid[1], w1_ref[...]).astype(BF16), jnp.asarray(0, BF16))

    def end_tail(pair):
        res = [out_dot(sub, wo_e) for sub in range(2)]
        mids = [end_mid(pair, sub, res[sub]) for sub in range(2)]
        hidden = [widen(mid) for mid in mids]
        delta = [mids[sub][0] + dot(hidden[sub], w2_ref[...]) for sub in range(2)]
        store_block(send_d, got_d, pair, delta[0], delta[1], 0, rows)

    @pl.loop(0, pairs)
    def _(pair):
        for idx in range(1, groups):
            @pl.when(pair == early // 2 * idx - 1)
            def _():
                wait_h(LAST + idx)
                spread(idx, 0, pairs)

        @pl.when(pair > 1)
        def _():
            send_delta(pair - 2, 1)

        last = jnp.maximum(pair - 1, 0)
        ahead = jnp.minimum(pair + 1, pairs - 1)
        here = 2 * lax.rem(pair, 2)
        there = 2 - here
        att = Attention([here, here + 1, there])
        normed1 = duplicate_tail(layer_norm(column(2 * ahead + 1)))
        att.qk(2)
        att.qk(3)
        att.soften(0)
        res0 = out_dot(0, wo_e)
        res1 = out_dot(1, wo_e)
        att.soften(1)
        normed0 = duplicate_tail(layer_norm(column(2 * ahead)))
        att.mix(1)
        next0 = project(there, normed0, wt_e, wp_e)
        mid0 = end_mid(last, 0, res0)
        att.norm(1)
        att.soften(2)
        att.mix(0)
        att.qk(4)
        att.mix(2)
        stage(next0)
        att.norm(0)
        att.soften(3)
        att.qk(5)
        att.norm(2)
        hidden0 = widen(mid0)
        mid1 = end_mid(last, 1, res1)
        att.soften(4)
        att.qk(6)
        att.mix(3)
        delta0 = mid0[0] + dot(hidden0, w2_ref[...])
        hidden1 = widen(mid1)
        att.gate(0)
        att.qk(7)
        next1 = project(there + 1, normed1, wt_e, wp_e)
        delta1 = mid1[0] + dot(hidden1, w2_ref[...])
        att.hand_on(6)
        att.hand_on(7)
        att.norm(3)
        store_block(send_d, got_d, last, delta0, delta1, 0, rows)
        att.soften(5)
        att.mix(4)
        att.mix(5)
        att.norm(5)
        stage(next1)
        att.norm(4)
        att.gate(1)

    send_delta(pairs - 2, 1)
    end_tail(pairs - 1)
    send_delta(pairs - 1, 1)

    def finish(part, first, count):
        span = pl.ds(first, count)
        for peer in peers:
            pltpu.make_async_copy(got_d.at[peer, span], got_d.at[peer, span], d_recv_sem.at[part, peer]).wait()

        @pl.loop(0, group)
        def _(src):
            for pair in range(first, first + count):
                start = pl.multiple_of((src * pairs + pair) * 2 * rows, 2 * rows)
                flat[pl.ds(start, 2 * rows), :] = got_d[src, pair].astype(F32)

        @pl.loop(0, rows)
        def _(row):
            for src in range(group):
                low_col = rows * src + 2 * first
                y_ref[row, low_col:low_col + 2 * count] += flat[pl.ds(low_col * rows + row, 2 * count, stride=rows), :]

    finish(0, 0, late)
    finish(1, late, pairs - late)

    for peer in alike + [partner]:
        drain(send_bias.at[1, most], bias_send_sem.at[1, peer])
    for src in alike:
        drain(got_bias.at[1, src, most], pass_send_sem.at[src])
    for peer in peers:
        drain(send_bias.at[1, final], bias_send_sem.at[2, peer])
        for sem, view in enumerate(whole_views):
            drain(view(send_h, peer), h_send_sem.at[sem, peer])
        drain(send_d.at[peer], d_send_sem.at[peer])


def solution(mesh):
    row_spec = P(('dp', 'sp'), None, None)
    group = mesh.shape['sp']

    def local_fn(pair_loc, *weights):
        rows, seq_len, channels = pair_loc.shape
        heads = weights[1].shape[0]
        pairs = rows // 2
        wide = heads * seq_len
        early = 8
        chunk = 8
        hbm = pl.BlockSpec(memory_space=pltpu.HBM)

        groups = rows // early
        columns = pltpu.VMEM((group, groups, pairs, 2 * early, channels), BF16)
        deltas = pltpu.VMEM((group, pairs, 2 * rows, channels), BF16)

        def sems(*shape):
            return pltpu.SemaphoreType.DMA(shape)

        return pl.pallas_call(
            functools.partial(kernel, 'sp', group, early),
            out_shape=jax.ShapeDtypeStruct(pair_loc.shape, F32),
            in_specs=[hbm] * 9,
            out_specs=pl.BlockSpec(memory_space=pltpu.VMEM),
            scratch_shapes=[pltpu.VMEM(pair_loc.shape, F32)] + [pltpu.VMEM(val.shape, BF16) for val in weights] + [
                pltpu.VMEM((3 * channels, channels), BF16),
                pltpu.VMEM((3 * channels, channels), BF16),
                pltpu.VMEM((rows, wide), F32),
                pltpu.VMEM((2, rows // chunk, chunk, wide), BF16),
                pltpu.VMEM((2, group, rows // chunk, chunk, wide), BF16),
                pltpu.VMEM((seq_len, wide), F32),
                pltpu.VMEM((rows, seq_len, channels), BF16),
                pltpu.VMEM((rows, channels, DOUBLE), BF16),
                pltpu.VMEM((rows, seq_len, channels), BF16),
                pltpu.VMEM((rows, channels, seq_len), BF16),
                pltpu.VMEM((rows, channels, DOUBLE), F32),
                pltpu.VMEM((2, channels, DOUBLE), BF16),
                pltpu.VMEM((2, 2, seq_len, LANES), F32),
                pltpu.VMEM((2, 2, 1, LANES), F32),
                columns, columns, deltas, deltas,
                pltpu.VMEM((rows * seq_len, channels), F32),
                sems(rows // chunk), sems(len(weights)), sems(3, group), sems(3, group), sems(group),
                sems(groups + 2, group), sems(groups + 2, group), sems(group), sems(2, group),
            ],
            compiler_params=pltpu.CompilerParams(collective_id=0, has_side_effects=True, vmem_limit_bytes=34 * 1024 * 1024),
        )(*[pltpu.with_memory_space_constraint(val, pltpu.HBM) for val in (pair_loc, *weights)])

    return jax.shard_map(local_fn, mesh=mesh, in_specs=(row_spec, P(), P(), P(), P(), P(), P(), P(), P()), out_specs=row_spec, check_vma=False)
```

```python
import functools

import jax
import jax.numpy as jnp
from jax import lax
from jax.experimental import pallas as pl
from jax.experimental.pallas import tpu as pltpu
from jax.sharding import PartitionSpec as P

LN_EPS = 1e-5
LANES = 128
DOUBLE = 256
HALF = 64
HEAD = 32
Q_SHRINK = 0.125
SHRINK = 32 ** -0.5 / Q_SHRINK
LOG2_E = 1.4426950408889634
MESH = pl.DeviceIdType.MESH
F32 = jnp.float32
BF16 = jnp.bfloat16


def layer_norm(vals):
    mean_c = jnp.mean(vals, axis=-1, keepdims=True)
    centered = vals - mean_c
    variance = jnp.mean(centered * centered, axis=-1, keepdims=True)
    return (centered * lax.rsqrt(variance + LN_EPS)).astype(BF16)


def dot(lhs, rhs, lhs_dim=1, rhs_dim=0):
    return lax.dot_general(lhs, rhs, (((lhs_dim,), (rhs_dim,)), ((), ())), preferred_element_type=F32)


def duplicate_tail(normed):
    return jnp.concatenate([normed, normed[LANES:]], axis=0)


def low_half(shape):
    return lax.broadcasted_iota(jnp.int32, shape, len(shape) - 1) < HALF


def bias_row(full):
    low = low_half((1, LANES))
    tiles = []
    for first in (0, 2):
        head_a, head_b = full[first:first + 1], full[first + 1:first + 2]
        tiles += [head_a[:, :LANES], jnp.where(low, head_a[:, LANES:], head_b[:, LANES:]), head_b[:, :LANES]]
    return jnp.concatenate(tiles, axis=1)


def keep_low(val):
    return jnp.where(low_half(val.shape), val, jnp.zeros_like(val))


def keep_high(val):
    return jnp.where(low_half(val.shape), jnp.zeros_like(val), val)


def stack(rows):
    return jnp.concatenate([jnp.concatenate(row, axis=1) for row in rows], axis=0)


def score_block(q_t, tile):
    zero = jnp.zeros((HEAD, LANES), BF16)
    none = [zero, zero]

    def head(idx):
        return q_t[HEAD * idx:HEAD * idx + HEAD, :LANES], q_t[HEAD * idx:HEAD * idx + HEAD, LANES:]

    first, second = head(tile), head(tile + 1)
    if tile == 0:
        return stack([[first[0], keep_low(first[1])], [zero, keep_high(second[1])], none, none])
    if tile == 1:
        return stack([none, [first[0], zero], [zero, second[0]], none])
    return stack([none, none, [keep_low(first[1]), zero], [keep_high(second[1]), second[0]]])


def gather_heads(outs, g_t):
    main = jnp.concatenate([outs[0][:HEAD, :LANES], outs[1][:HEAD, :LANES], outs[1][HEAD:, LANES:], outs[2][HEAD:, LANES:]], axis=0)
    tail = jnp.concatenate([keep_low(outs[0][:HEAD, LANES:]), keep_high(outs[0][HEAD:, LANES:]),
                            keep_low(outs[2][:HEAD, :LANES]), keep_high(outs[2][HEAD:, :LANES])], axis=0)
    return (jnp.concatenate([main, tail], axis=1) * g_t).astype(BF16)


def merge_tail(res):
    return jnp.concatenate([res[:LANES], res[LANES:192] + res[192:]], axis=0)


def kernel(axis, group, early, z_hbm, wp_s_hbm, wb_s_hbm, wo_s_hbm, wp_e_hbm, wb_e_hbm, wo_e_hbm, w1_hbm, w2_hbm, y_ref,
           z_ref, wp_s, wb_s, wo_s, wp_e, wb_e, wo_e, w1_ref, w2_ref,
           wt_s, wt_e, row_bias, send_bias, got_bias, bias_t, normed_sc, q_sc, k_sc, v_sc, g_sc, gated_sc, part_sc, top_sc,
           send_h, got_h, send_d, got_d, flat,
           z_sem, w_sem, bias_send_sem, bias_recv_sem, pass_send_sem, h_send_sem, h_recv_sem, d_send_sem, d_recv_sem):
    rows, seq_len, channels = z_hbm.shape
    pairs = rows // 2
    chunk = 8
    chunks = rows // chunk
    late = pairs - 2
    groups = rows // early
    held = pairs - 9
    me = lax.axis_index(axis)
    half = group // 2
    order = sorted(range(1, group), key=lambda step: abs(step - half))
    peers = [lax.rem(me + step, group) for step in order]
    partner = me + 1 - 2 * lax.rem(me, 2)
    alike = [lax.rem(me + step, group) for step in order if step % 2 == 0]
    others = [lax.rem(partner + step, group) for step in order if step % 2 == 0]

    def load_z(idx):
        span = pl.ds(idx * chunk, chunk)
        return pltpu.make_async_copy(z_hbm.at[span], z_ref.at[span], z_sem.at[idx])

    loads = [pltpu.make_async_copy(src, dst, w_sem.at[idx]) for idx, (src, dst) in enumerate(
        ((wb_s_hbm, wb_s), (wp_s_hbm, wp_s), (wp_e_hbm, wp_e), (wo_s_hbm, wo_s), (wb_e_hbm, wb_e),
         (wo_e_hbm, wo_e), (w1_hbm, w1_ref), (w2_hbm, w2_ref)))]
    loads[0].start()
    for idx in range(chunks):
        load_z(idx).start()
    for load in loads[1:]:
        load.start()

    barrier = pltpu.get_barrier_semaphore()
    for peer in peers:
        pl.semaphore_signal(barrier, inc=1, device_id={axis: peer}, device_id_type=MESH)

    def send_bias_part(phase, part, count, to, sem):
        span = pl.ds(part, count)
        for peer in to:
            pltpu.make_async_remote_copy(
                src_ref=send_bias.at[phase, span], dst_ref=got_bias.at[phase, me, span],
                send_sem=bias_send_sem.at[sem, peer], recv_sem=bias_recv_sem.at[sem, me],
                device_id={axis: peer}, device_id_type=MESH).start()

    def drain(ref, sem):
        pltpu.make_async_copy(ref, ref, sem).wait()

    most, final = pl.ds(0, chunks - 1), pl.ds(chunks - 1, 1)

    def forward_bias():
        for src in alike:
            view = got_bias.at[1, src, most]
            drain(view, bias_recv_sem.at[1, src])
            pltpu.make_async_remote_copy(
                src_ref=view, dst_ref=view,
                send_sem=pass_send_sem.at[src], recv_sem=bias_recv_sem.at[1, src],
                device_id={axis: partner}, device_id_type=MESH).start()

    def publish_bias(phase, part):
        rounded = row_bias[chunk * part:chunk * part + chunk].astype(BF16)
        send_bias[phase, part] = rounded
        got_bias[phase, me, part] = rounded

    def send_blocks(send, got, send_sem, recv_sem, start, count):
        span = pl.ds(start, count)
        for peer in peers:
            pltpu.make_async_remote_copy(
                src_ref=send.at[peer, span], dst_ref=got.at[me, span],
                send_sem=send_sem.at[peer], recv_sem=recv_sem.at[me],
                device_id={axis: peer}, device_id_type=MESH).start()

    def send_h_view(sem, view):
        for peer in peers:
            pltpu.make_async_remote_copy(
                src_ref=view(send_h, peer), dst_ref=view(got_h, me),
                send_sem=h_send_sem.at[sem, peer], recv_sem=h_recv_sem.at[sem, me],
                device_id={axis: peer}, device_id_type=MESH).start()

    def wide_view(start, count):
        return lambda ref, who: ref.at[who, :, pl.ds(start, count)]

    def group_view(idx, start, count):
        return lambda ref, who: ref.at[who, idx, pl.ds(start, count)]

    WIDE, FIRST, LAST = range(3)
    whole_views = [wide_view(0, held), group_view(0, held, pairs - 1 - held), group_view(0, pairs - 1, 1)]
    whole_views += [group_view(idx, held, pairs - held) for idx in range(1, groups)]

    def wait_h(sem):
        for peer in peers:
            view = whole_views[sem](got_h, peer)
            pltpu.make_async_copy(view, view, h_recv_sem.at[sem, peer]).wait()

    def send_first(start, count):
        send_h_view(FIRST, group_view(0, start, count))

    def send_delta(start, count):
        send_blocks(send_d, got_d, d_send_sem, d_recv_sem.at[start // late], start, count)

    def store_block(send, got, pair, first, second, low, high):
        for dest in range(group):
            span = slice(rows * dest + low, rows * dest + high)
            send[dest, pair] = jnp.concatenate([first[span], second[span]], axis=0).astype(BF16)
        got[me, pair] = send[me, pair]

    def project(slot, normed_dup, wt, wp):
        cols = dot(wt[...], normed_dup, 1, 1)
        keys = dot(normed_dup[:seq_len], wp[:, channels:2 * channels])
        return slot, cols, keys

    def stage(projected):
        slot, cols, keys = projected
        q_sc[slot] = cols[:channels].astype(BF16)
        v_sc[slot] = cols[channels:2 * channels, :seq_len].astype(BF16)
        g_sc[slot] = jax.nn.sigmoid(cols[2 * channels:])
        k_sc[slot] = keys.astype(BF16)

    def transpose_weights(wp, wt):
        wt[0:channels] = wp[:, 0:channels].T * jnp.asarray(Q_SHRINK, BF16)
        wt[channels:2 * channels] = wp[:, 2 * channels:3 * channels].T
        wt[2 * channels:3 * channels] = wp[:, 3 * channels:].T

    class Attention:
        def __init__(self, slots):
            self.slots = slots
            self.score, self.prob, self.mixed, self.done = {}, {}, {}, {}

        def qk(self, unit):
            slot, tile = self.slots[unit // 3], unit % 3
            self.score[unit] = dot(k_sc[slot], score_block(q_sc[slot], tile))

        def biased(self, unit, half):
            at = DOUBLE * (unit % 3) + LANES * half
            return self.score[unit][:, LANES * half:LANES * half + LANES] + bias_t[:, at:at + LANES]

        def hand_on(self, unit):
            for half in range(2):
                part = self.biased(unit, half)
                part_sc[unit % 3, half] = part
                top_sc[unit % 3, half] = jnp.max(part, axis=0, keepdims=True)

        def soften(self, unit):
            probs, totals = [], []
            for half in range(2):
                if unit in self.score:
                    part = self.biased(unit, half)
                    top = jnp.max(part, axis=0, keepdims=True)
                else:
                    part, top = part_sc[unit, half], top_sc[unit, half]
                prob = jnp.exp2((part - top) * (SHRINK * LOG2_E))
                totals.append(jnp.sum(prob, axis=0, keepdims=True))
                probs.append(prob.astype(BF16))
            self.prob[unit] = jnp.concatenate(probs, axis=1), jnp.concatenate(totals, axis=1)

        def mix(self, unit):
            slot, tile = self.slots[unit // 3], unit % 3
            prob, total = self.prob.pop(unit)
            self.mixed[unit] = dot(v_sc[slot, HEAD * tile:HEAD * tile + HALF], prob), total

        def norm(self, unit):
            mixed, total = self.mixed.pop(unit)
            self.done[unit] = mixed / total

        def gate(self, sub):
            outs = [self.done.pop(3 * sub + tile) for tile in range(3)]
            gated_sc[sub] = gather_heads(outs, g_sc[self.slots[sub]])

    def out_dot(sub, wo):
        return dot(gated_sc[sub].T, wo[...])

    loads[0].wait()
    for part in range(chunks):
        load_z(part).wait()
        base = chunk * part
        normed = [layer_norm(z_ref[base + sub]) for sub in range(chunk)]
        full = [dot(wb_s[...], duplicate_tail(val), 1, 1) for val in normed]
        for sub in range(chunk):
            normed_sc[base + sub] = normed[sub]
        for sub in range(chunk):
            row_bias[base + sub:base + sub + 1, :] = bias_row(full[sub])
        publish_bias(0, part)
        if part == chunks - 2:
            pl.semaphore_wait(barrier, group - 1)
            send_bias_part(0, 0, chunks - 1, peers, 0)

    for load in loads[1:]:
        load.wait()
    send_bias_part(0, chunks - 1, 1, peers, 0)
    transpose_weights(wp_s, wt_s)

    @pl.loop(0, pairs)
    def _(step):
        made = [project(2 * step + sub, duplicate_tail(normed_sc[2 * step + sub]), wt_s, wp_s) for sub in range(2)]
        for val in made:
            stage(val)

    def bias_of(phase, src):
        return jnp.concatenate([got_bias[phase, src, part].astype(F32) for part in range(chunks)], axis=0)

    def open_scores():
        att = Attention([0])
        for unit in range(2):
            att.qk(unit)
        return att

    transpose_weights(wp_e, wt_e)
    opening = open_scores()
    for src in peers:
        drain(got_bias.at[0, src], bias_recv_sem.at[0, src])
    low = low_half((HALF, LANES))
    by_query = jnp.concatenate([bias_of(0, src) for src in range(group)], axis=0) * (1 / SHRINK)
    by_query = jnp.concatenate([by_query, by_query[LANES:]], axis=0)
    for first in (0, 1):
        base = 384 * first
        head_a = by_query[:, base:base + LANES].T
        mixed = by_query[:, base + LANES:base + DOUBLE].T
        head_b = by_query[:, base + DOUBLE:base + 384].T
        bias_t[0:LANES, base:base + LANES] = head_a[:, :LANES]
        bias_t[LANES:192, base:base + LANES] = mixed[:HALF, :LANES]
        low_a = low_half((LANES, LANES))
        bias_t[0:LANES, base + LANES:base + DOUBLE] = jnp.where(low_a, head_a[:, LANES:], head_b[:, LANES:])
        bias_t[LANES:192, base + LANES:base + DOUBLE] = jnp.where(low, mixed[:HALF, LANES:], mixed[HALF:, LANES:])
        bias_t[0:LANES, base + DOUBLE:base + 384] = head_b[:, :LANES]
        bias_t[LANES:192, base + DOUBLE:base + 384] = mixed[HALF:, :LANES]

    def start_resid(pair, sub, res):
        row = 2 * pair + sub
        value = z_ref[row] + merge_tail(res)
        y_ref[row] = value
        return value

    def store_h(pair, first, second):
        for idx in range(groups):
            for dest in range(group):
                low = rows * dest + early * idx
                span = slice(low, low + early)
                send_h[dest, idx, pair] = jnp.concatenate([first[span], second[span]], axis=0).astype(BF16)
            got_h[me, idx, pair] = send_h[me, idx, pair]

    def end_normed(pair, sub):
        return duplicate_tail(layer_norm(y_ref[2 * pair + sub].astype(BF16).astype(F32)))

    for unit in range(2):
        opening.hand_on(unit)

    @pl.loop(0, pairs)
    def _(pair):
        even = lax.rem(pair, 2) == 0
        @pl.when(pair == pairs - 2)
        def _():
            for part in range(chunks - 1):
                publish_bias(1, part)

        @pl.when(pair == held + 1)
        def _():
            send_h_view(WIDE, wide_view(0, held))

        @pl.when(pair == pairs - 4)
        def _():
            send_first(held, pairs - 5 - held)

        @pl.when(pair == pairs - 2)
        def _():
            send_first(pairs - 5, 2)

        @pl.when(pair == pairs - 1)
        def _():
            send_first(pairs - 3, 1)

        @pl.when(pair == pairs - 2)
        def _():
            send_bias_part(1, 0, chunks - 1, alike + [partner], 1)

        last = jnp.maximum(pair - 1, 0)
        older = jnp.maximum(pair - 2, 0)
        att = Attention([2 * pair, 2 * pair + 1, 2 * jnp.minimum(pair + 1, pairs - 1)])
        normed0 = end_normed(older, 0)
        att.qk(3)
        normed1 = end_normed(older, 1)
        att.soften(0)
        res1 = out_dot(1, wo_s)
        att.qk(2)
        att.mix(0)
        att.soften(1)
        att.soften(2)
        res0 = out_dot(0, wo_s)
        att.mix(1)
        made0 = start_resid(last, 0, res0)
        full1 = dot(wb_e[...], normed1, 1, 1)
        att.qk(4)
        full0 = dot(wb_e[...], normed0, 1, 1)
        att.norm(1)
        att.soften(3)
        att.mix(2)
        att.norm(0)
        att.qk(5)
        made1 = start_resid(last, 1, res1)
        att.soften(5)
        att.soften(4)
        att.qk(6)
        att.norm(2)
        att.gate(0)
        att.qk(7)
        att.mix(3)
        att.mix(4)
        att.mix(5)
        store_h(last, made0, made1)
        row_bias[pl.ds(2 * older, 1), :] = bias_row(full0)
        att.norm(4)
        att.norm(5)
        att.hand_on(6)
        row_bias[pl.ds(2 * older + 1, 1), :] = bias_row(full1)
        att.norm(3)
        att.hand_on(7)
        att.gate(1)

    send_first(pairs - 2, 1)
    res = [out_dot(sub, wo_s) for sub in range(2)]
    made = [start_resid(pairs - 1, sub, res[sub]) for sub in range(2)]
    store_h(pairs - 1, made[0], made[1])
    ends = [(pair, sub) for pair in (pairs - 2, pairs - 1) for sub in range(2)]
    send_h_view(LAST, group_view(0, pairs - 1, 1))
    full = [dot(wb_e[...], end_normed(pair, sub), 1, 1) for pair, sub in ends]
    for (pair, sub), val in zip(ends, full):
        row_bias[2 * pair + sub:2 * pair + sub + 1, :] = bias_row(val)
    publish_bias(1, chunks - 1)
    for peer in peers:
        drain(send_bias.at[0], bias_send_sem.at[0, peer])
    send_bias_part(1, chunks - 1, 1, peers, 2)
    for idx in range(1, groups):
        send_h_view(LAST + idx, group_view(idx, held, pairs - held))

    def spread(idx, first, count):
        @pl.loop(0, group)
        def _(src):
            for pair in range(first, first + count):
                block = got_h[src, idx, pair].astype(F32)
                for sub in range(2):
                    start = pl.multiple_of(((src * pairs + pair) * 2 + sub) * rows + early * idx, 8)
                    flat[pl.ds(start, early), :] = block[early * sub:early * sub + early]

    def column(col):
        return flat[pl.ds(col, seq_len, stride=rows), :]

    wait_h(WIDE)
    wait_h(FIRST)
    spread(0, 0, pairs - 1)
    wait_h(LAST)
    spread(0, pairs - 1, 1)
    forward_bias()

    for sub in range(2):
        stage(project(sub, duplicate_tail(layer_norm(column(sub))), wt_e, wp_e))

    opening = open_scores()
    for src in [partner] + others:
        drain(got_bias.at[1, src, most], bias_recv_sem.at[1, src])
    for src in peers:
        drain(got_bias.at[1, src, final], bias_recv_sem.at[2, src])
    for src in range(group):
        bias_t[rows * src:rows * src + rows] = bias_of(1, src) * (1 / SHRINK)

    for unit in range(2):
        opening.hand_on(unit)

    def end_mid(pair, sub, res):
        upd = merge_tail(res)
        return upd, layer_norm(column(2 * pair + sub) + upd)

    def widen(mid):
        return jnp.maximum(dot(mid[1], w1_ref[...]).astype(BF16), jnp.asarray(0, BF16))

    def end_tail(pair):
        res = [out_dot(sub, wo_e) for sub in range(2)]
        mids = [end_mid(pair, sub, res[sub]) for sub in range(2)]
        hidden = [widen(mid) for mid in mids]
        delta = [mids[sub][0] + dot(hidden[sub], w2_ref[...]) for sub in range(2)]
        store_block(send_d, got_d, pair, delta[0], delta[1], 0, rows)

    @pl.loop(0, pairs)
    def _(pair):
        for idx in range(1, groups):
            @pl.when(pair == early // 2 * idx - 1)
            def _():
                wait_h(LAST + idx)
                spread(idx, 0, pairs)

        @pl.when(pair > 1)
        def _():
            send_delta(pair - 2, 1)

        last = jnp.maximum(pair - 1, 0)
        ahead = jnp.minimum(pair + 1, pairs - 1)
        here = 2 * lax.rem(pair, 2)
        there = 2 - here
        att = Attention([here, here + 1, there])
        normed1 = duplicate_tail(layer_norm(column(2 * ahead + 1)))
        att.qk(2)
        att.qk(3)
        att.soften(0)
        res0 = out_dot(0, wo_e)
        res1 = out_dot(1, wo_e)
        att.soften(1)
        normed0 = duplicate_tail(layer_norm(column(2 * ahead)))
        att.mix(1)
        next0 = project(there, normed0, wt_e, wp_e)
        mid0 = end_mid(last, 0, res0)
        att.norm(1)
        att.soften(2)
        att.mix(0)
        att.qk(4)
        att.mix(2)
        stage(next0)
        att.norm(0)
        att.soften(3)
        att.qk(5)
        att.norm(2)
        hidden0 = widen(mid0)
        mid1 = end_mid(last, 1, res1)
        att.soften(4)
        att.qk(6)
        att.mix(3)
        delta0 = mid0[0] + dot(hidden0, w2_ref[...])
        hidden1 = widen(mid1)
        att.gate(0)
        att.qk(7)
        next1 = project(there + 1, normed1, wt_e, wp_e)
        delta1 = mid1[0] + dot(hidden1, w2_ref[...])
        att.hand_on(6)
        att.hand_on(7)
        att.norm(3)
        store_block(send_d, got_d, last, delta0, delta1, 0, rows)
        att.soften(5)
        att.mix(4)
        att.mix(5)
        att.norm(5)
        stage(next1)
        att.norm(4)
        att.gate(1)

    send_delta(pairs - 2, 1)
    end_tail(pairs - 1)
    send_delta(pairs - 1, 1)

    def finish(part, first, count):
        span = pl.ds(first, count)
        for peer in peers:
            pltpu.make_async_copy(got_d.at[peer, span], got_d.at[peer, span], d_recv_sem.at[part, peer]).wait()

        @pl.loop(0, group)
        def _(src):
            for pair in range(first, first + count):
                start = pl.multiple_of((src * pairs + pair) * 2 * rows, 2 * rows)
                flat[pl.ds(start, 2 * rows), :] = got_d[src, pair].astype(F32)

        @pl.loop(0, rows)
        def _(row):
            for src in range(group):
                low_col = rows * src + 2 * first
                y_ref[row, low_col:low_col + 2 * count] += flat[pl.ds(low_col * rows + row, 2 * count, stride=rows), :]

    finish(0, 0, late)
    for peer in alike + [partner]:
        drain(send_bias.at[1, most], bias_send_sem.at[1, peer])
    for src in alike:
        drain(got_bias.at[1, src, most], pass_send_sem.at[src])
    for peer in peers:
        drain(send_bias.at[1, final], bias_send_sem.at[2, peer])
        for sem, view in enumerate(whole_views):
            drain(view(send_h, peer), h_send_sem.at[sem, peer])
        drain(send_d.at[peer], d_send_sem.at[peer])
    finish(1, late, pairs - late)


def solution(mesh):
    row_spec = P(('dp', 'sp'), None, None)
    group = mesh.shape['sp']

    def local_fn(pair_loc, *weights):
        rows, seq_len, channels = pair_loc.shape
        heads = weights[1].shape[0]
        pairs = rows // 2
        wide = heads * seq_len
        early = 8
        chunk = 8
        hbm = pl.BlockSpec(memory_space=pltpu.HBM)

        groups = rows // early
        columns = pltpu.VMEM((group, groups, pairs, 2 * early, channels), BF16)
        deltas = pltpu.VMEM((group, pairs, 2 * rows, channels), BF16)

        def sems(*shape):
            return pltpu.SemaphoreType.DMA(shape)

        return pl.pallas_call(
            functools.partial(kernel, 'sp', group, early),
            out_shape=jax.ShapeDtypeStruct(pair_loc.shape, F32),
            in_specs=[hbm] * 9,
            out_specs=pl.BlockSpec(memory_space=pltpu.VMEM),
            scratch_shapes=[pltpu.VMEM(pair_loc.shape, F32)] + [pltpu.VMEM(val.shape, BF16) for val in weights] + [
                pltpu.VMEM((3 * channels, channels), BF16),
                pltpu.VMEM((3 * channels, channels), BF16),
                pltpu.VMEM((rows, wide), F32),
                pltpu.VMEM((2, rows // chunk, chunk, wide), BF16),
                pltpu.VMEM((2, group, rows // chunk, chunk, wide), BF16),
                pltpu.VMEM((seq_len, wide), F32),
                pltpu.VMEM((rows, seq_len, channels), BF16),
                pltpu.VMEM((rows, channels, DOUBLE), BF16),
                pltpu.VMEM((rows, seq_len, channels), BF16),
                pltpu.VMEM((rows, channels, seq_len), BF16),
                pltpu.VMEM((rows, channels, DOUBLE), F32),
                pltpu.VMEM((2, channels, DOUBLE), BF16),
                pltpu.VMEM((2, 2, seq_len, LANES), F32),
                pltpu.VMEM((2, 2, 1, LANES), F32),
                columns, columns, deltas, deltas,
                pltpu.VMEM((rows * seq_len, channels), F32),
                sems(rows // chunk), sems(len(weights)), sems(3, group), sems(3, group), sems(group),
                sems(groups + 2, group), sems(groups + 2, group), sems(group), sems(2, group),
            ],
            compiler_params=pltpu.CompilerParams(collective_id=0, has_side_effects=True, vmem_limit_bytes=34 * 1024 * 1024),
        )(*[pltpu.with_memory_space_constraint(val, pltpu.HBM) for val in (pair_loc, *weights)])

    return jax.shard_map(local_fn, mesh=mesh, in_specs=(row_spec, P(), P(), P(), P(), P(), P(), P(), P()), out_specs=row_spec, check_vma=False)
```
